32 devices in a mesh: dp: 2 (over x), tp: 4 (over z), sq: 4 (over y, core).
Axes of the slice: x: 2, y: 2, z: 4, core: 2. Of those that a mesh axis runs over, the one named last changes fastest.
Arguments:
- hidden: bfloat16 [512, 2048], P('dp'), parts along dimension 0
- cache_lens: int32 [512], P('dp'), parts along dimension 0
- k_cache: bfloat16 [512, 1024, 128], P('dp', 'sq'), parts along dimension 0
- v_cache: bfloat16 [512, 1024, 128], P('dp', 'sq'), parts along dimension 0
- ln_gain: float32 [2048], replicated
- ln_bias: float32 [2048], replicated
- w_query: bfloat16 [2048, 2048], P(None, 'tp')
- b_query: float32 [2048], P('tp')
- w_kv: bfloat16 [2048, 256], replicated
- b_kv: float32 [256], replicated
- w_out: bfloat16 [2048, 2048], P('tp')
- b_out: float32 [2048], replicated
Outputs:
- output 1: bfloat16 [512, 2048], P('dp'), parts along dimension 0
- output 2: bfloat16 [512, 1024, 128], P('dp', 'sq'), parts along dimension 0
- output 3: bfloat16 [512, 1024, 128], P('dp', 'sq'), parts along dimension 0
There are 2 independent parts. The reference program is written for one: setup_inputs(seed, part) draws one part's arguments, and reference() takes and returns one part's arrays. A program takes and returns all parts, laid end to end along the dimension named above; an argument that names none is the same for every part.
All inputs are finite; a program needn't handle non-finite values.
Results may differ from the reference program's by a relative error of at most 0.00347619.
Values sent between devices are 32-bit elements.
A program may use at most 1 GiB of HBM per device.

```python
import math
import jax
import jax.numpy as jnp
from jax import lax

BATCH = 256
CACHE_LEN = 1024
D_MODEL = 2048
HEADS = 16
HEAD_DIM = 128


def layer_norm(x_rows, ln_gain, ln_bias):
    x_wide = x_rows.astype(jnp.float32)
    mean_val = jnp.mean(x_wide, axis=-1, keepdims=True)
    centered = x_wide - mean_val
    variance = jnp.mean(centered * centered, axis=-1, keepdims=True)
    normed = centered * lax.rsqrt(variance + 1e-5)
    return (normed * ln_gain + ln_bias).astype(jnp.bfloat16)


def setup_inputs(seed: int = 0, part: int = 0) -> dict:
    own_keys = jax.random.split(jax.random.fold_in(jax.random.key(seed), part), 5)
    shared_keys = jax.random.split(jax.random.key(seed + 1), 10)
    q_width = HEADS * HEAD_DIM
    score_var = max(1.0, math.log(CACHE_LEN / 32.0))
    key_scale = math.sqrt(score_var / 2.0)
    self_bias = (math.log(0.6 * CACHE_LEN) + 0.5 * score_var) / math.sqrt(HEAD_DIM)
    hidden = jax.random.normal(own_keys[0], (BATCH, D_MODEL), jnp.float32).astype(jnp.bfloat16)
    drawn = CACHE_LEN - 1 - jax.random.randint(own_keys[1], (BATCH,), 0, CACHE_LEN // 2)
    order = jax.random.permutation(own_keys[2], BATCH)
    seq_ids = jnp.arange(BATCH)
    cache_lens = jnp.where(seq_ids == order[0], CACHE_LEN - 1, jnp.where(seq_ids == order[1], 1, drawn)).astype(jnp.int32)
    k_cache = (key_scale * jax.random.normal(own_keys[3], (BATCH, CACHE_LEN, HEAD_DIM), jnp.float32)).astype(jnp.bfloat16)
    v_cache = jax.random.normal(own_keys[4], (BATCH, CACHE_LEN, HEAD_DIM), jnp.float32).astype(jnp.bfloat16)
    ln_gain = 1.0 + 0.3 * jax.random.normal(shared_keys[0], (D_MODEL,), jnp.float32)
    ln_bias = 0.3 * jax.random.normal(shared_keys[1], (D_MODEL,), jnp.float32)
    w_query = (jax.random.normal(shared_keys[2], (D_MODEL, q_width), jnp.float32) * D_MODEL ** -0.5).astype(jnp.bfloat16)
    shared_dir = jax.random.normal(shared_keys[3], (HEAD_DIM,), jnp.float32)
    b_query = jnp.tile(shared_dir, HEADS) + 0.2 * jax.random.normal(shared_keys[4], (q_width,), jnp.float32)
    w_kv = (jax.random.normal(shared_keys[5], (D_MODEL, 2 * HEAD_DIM), jnp.float32) * D_MODEL ** -0.5).astype(jnp.bfloat16)
    key_bias = self_bias * shared_dir + 0.2 * jax.random.normal(shared_keys[6], (HEAD_DIM,), jnp.float32)
    val_bias = 0.5 * jax.random.normal(shared_keys[7], (HEAD_DIM,), jnp.float32)
    b_kv = jnp.concatenate([key_bias, val_bias])
    w_out = (jax.random.normal(shared_keys[8], (q_width, D_MODEL), jnp.float32) * q_width ** -0.5).astype(jnp.bfloat16)
    b_out = 0.3 * jax.random.normal(shared_keys[9], (D_MODEL,), jnp.float32)
    return {"hidden": hidden, "cache_lens": cache_lens, "k_cache": k_cache, "v_cache": v_cache, "ln_gain": ln_gain, "ln_bias": ln_bias, "w_query": w_query, "b_query": b_query, "w_kv": w_kv, "b_kv": b_kv, "w_out": w_out, "b_out": b_out}


def reference(hidden, cache_lens, k_cache, v_cache, ln_gain, ln_bias, w_query, b_query, w_kv, b_kv, w_out, b_out):
    normed = layer_norm(hidden, ln_gain, ln_bias)
    query = (jnp.dot(normed, w_query, preferred_element_type=jnp.float32) + b_query).astype(jnp.bfloat16)
    query = query.reshape(BATCH, HEADS, HEAD_DIM)
    key_val = (jnp.dot(normed, w_kv, preferred_element_type=jnp.float32) + b_kv).astype(jnp.bfloat16)
    positions = jnp.arange(CACHE_LEN, dtype=jnp.int32)
    at_slot = (positions[None, :] == cache_lens[:, None])[:, :, None]
    key_new = jnp.where(at_slot, key_val[:, None, :HEAD_DIM], k_cache)
    val_new = jnp.where(at_slot, key_val[:, None, HEAD_DIM:], v_cache)

    def one_sequence(packed):
        query_row, key_rows, val_rows, length = packed
        scores = jnp.einsum("nd,td->nt", query_row.astype(jnp.float32), key_rows.astype(jnp.float32)) * (HEAD_DIM ** -0.5)
        valid = positions <= length
        scores = jnp.where(valid[None, :], scores, -jnp.inf)
        weights = jax.nn.softmax(scores, axis=-1)
        return jnp.einsum("nt,td->nd", weights, val_rows.astype(jnp.float32)).astype(jnp.bfloat16)

    attended = lax.map(one_sequence, (query, key_new, val_new, cache_lens))
    projected = jnp.dot(attended.reshape(BATCH, HEADS * HEAD_DIM), w_out, preferred_element_type=jnp.float32)
    out_hidden = (hidden.astype(jnp.float32) + projected + b_out).astype(jnp.bfloat16)
    return (out_hidden, key_new, val_new)
```

```python
import functools

import jax
import jax.numpy as jnp
from jax import lax
from jax.experimental import pallas as pl
from jax.experimental.pallas import tpu as pltpu
from jax.sharding import PartitionSpec as P

F32 = jnp.float32
BF16 = jnp.bfloat16
NEG = -1e30


def attend_kernel(
    pairs, lens_ref, x_hbm, gain_ref, bias_ref, wq_hbm, bq_ref, wkv_hbm, bkv_ref, k_hbm, v_hbm,
    k_out, v_out, acc_ref, ml_ref,
    x_buf, h_buf, wq_buf, wkv_buf, q_buf, kv_buf, s_buf, k_buf, v_buf, in_sem, k_sem, v_sem, ko_sem, vo_sem,
):
    batch, pos_local, dim = k_buf.shape
    heads = wq_buf.shape[1] // dim
    per = 2 * pairs
    chunks = batch // per
    rows = 2 * heads
    first_pos = lax.axis_index("sq") * pos_local
    scale = dim ** -0.5

    x_copy = pltpu.make_async_copy(x_hbm, x_buf, in_sem.at[0])
    kv_copy = pltpu.make_async_copy(wkv_hbm, wkv_buf, in_sem.at[1])
    q_copy = pltpu.make_async_copy(wq_hbm, wq_buf, in_sem.at[2])
    x_copy.start()
    kv_copy.start()
    q_copy.start()

    def span(ref, c):
        return ref.at[pl.ds(c * per, per)]

    def k_load(c):
        return pltpu.make_async_copy(span(k_hbm, c), span(k_buf, c), k_sem.at[c])

    def v_load(c):
        return pltpu.make_async_copy(span(v_hbm, c), span(v_buf, c), v_sem.at[c])

    def k_store(c):
        return pltpu.make_async_copy(span(k_buf, c), span(k_out, c), ko_sem.at[c])

    def v_store(c):
        return pltpu.make_async_copy(span(v_buf, c), span(v_out, c), vo_sem.at[c])

    @pl.loop(0, chunks)
    def _(c):
        k_load(c).start()
        v_load(c).start()

    x_copy.wait()
    block = 32

    @pl.loop(0, batch // block)
    def _(i):
        x = x_buf[pl.ds(i * block, block), :].astype(F32)
        mean = jnp.mean(x, axis=-1, keepdims=True)
        cen = x - mean
        var = jnp.mean(cen * cen, axis=-1, keepdims=True)
        h = cen * lax.rsqrt(var + 1e-5) * gain_ref[...] + bias_ref[...]
        h_buf[pl.ds(i * block, block), :] = h.astype(BF16)

    kv_copy.wait()
    kv = jnp.dot(h_buf[...], wkv_buf[...], preferred_element_type=F32) + bkv_ref[...]
    kv_buf[...] = kv.astype(BF16).astype(F32)
    q_copy.wait()
    for n0 in range(0, heads, 2):
        cols = slice(n0 * dim, (n0 + 2) * dim)
        q = jnp.dot(h_buf[...], wq_buf[:, cols], preferred_element_type=F32) + bq_ref[:, cols]
        q = q.astype(BF16).astype(F32)
        q_buf[pl.ds(n0, batch, stride=heads), :] = q[:, :dim]
        q_buf[pl.ds(n0 + 1, batch, stride=heads), :] = q[:, dim:]

    top = lax.broadcasted_iota(jnp.int32, (rows, dim), 0) < heads
    top2 = lax.broadcasted_iota(jnp.int32, (rows, pos_local), 0) < heads
    lane = lax.broadcasted_iota(jnp.int32, (rows, dim), 1)
    place = first_pos + lax.broadcasted_iota(jnp.int32, (rows, pos_local), 1)
    sub = lax.broadcasted_iota(jnp.int32, (16, dim), 0)

    def update_rows(c):
        fresh = kv_buf[pl.ds(pl.multiple_of(c * per, per), per), :]
        for j in range(per):
            b = c * per + j
            at = lens_ref[b] - first_pos
            base = pl.multiple_of(jnp.clip(at, 0, pos_local - 1) // 16 * 16, 16)
            hit = sub == at - base
            for buf, lo in ((k_buf, 0), (v_buf, dim)):
                new = jnp.broadcast_to(fresh[j:j + 1, lo:lo + dim], (16, dim))
                old = buf[b, pl.ds(base, 16), :].astype(F32)
                buf[b, pl.ds(base, 16), :] = jnp.where(hit, new, old).astype(BF16)

    def score(c):
        out = []
        for j in range(pairs):
            p = c * pairs + j
            q = q_buf[pl.ds(pl.multiple_of(p * rows, rows), rows), :]
            lhs = jnp.concatenate([jnp.where(top, q, 0.0), jnp.where(top, 0.0, q)], axis=1).astype(BF16)
            keys = jnp.concatenate([k_buf[2 * p], k_buf[2 * p + 1]], axis=1)
            s = lax.dot_general(lhs, keys, (((1,), (1,)), ((), ())), preferred_element_type=F32)
            out.append(s)
        return out

    def weigh(c, m_all, l_all):
        for j in range(pairs):
            p = c * pairs + j
            s = s_buf[j * rows:(j + 1) * rows, :] * scale
            last = jnp.where(top2, lens_ref[2 * p], lens_ref[2 * p + 1])
            valid = place <= last
            s = jnp.where(valid, s, NEG)
            m = jnp.max(s, axis=-1, keepdims=True)
            w = jnp.where(valid, jnp.exp(s - m), 0.0)
            total = jnp.sum(w, axis=-1, keepdims=True)
            vals = jnp.concatenate([v_buf[2 * p], v_buf[2 * p + 1]], axis=1)
            o = jnp.dot(w.astype(BF16), vals, preferred_element_type=F32)
            acc_ref[pl.ds(pl.multiple_of(p * rows, rows), rows), :] = jnp.where(top, o[:, :dim], o[:, dim:])
            m_all = jnp.where(lane == p, m, m_all)
            l_all = jnp.where(lane == p, total, l_all)
        return m_all, l_all

    def put_scores(out):
        for j, s in enumerate(out):
            s_buf[j * rows:(j + 1) * rows, :] = s

    def arrive(c):
        k_load(c).wait()
        v_load(c).wait()
        update_rows(c)

    def leave(c):
        k_store(c).start()
        v_store(c).start()

    arrive(0)
    put_scores(score(0))
    leave(0)
    zero = jnp.zeros((rows, dim), F32)

    def body(c, carry):
        arrive(c + 1)
        carry = weigh(c, *carry)
        put_scores(score(c + 1))
        leave(c + 1)
        return carry

    carry = lax.fori_loop(0, chunks - 1, body, (zero, zero))
    m_all, l_all = weigh(chunks - 1, *carry)
    ml_ref[:rows, :] = m_all
    ml_ref[rows:, :] = l_all

    @pl.loop(0, chunks)
    def _(c):
        k_store(c).wait()
        v_store(c).wait()


def attend(lens, x, gain, bias, wq, bq, wkv, bkv, k, v, pairs=8):
    batch, pos_local, dim = k.shape
    width = x.shape[1]
    heads = wq.shape[1] // dim
    chunks = batch // (2 * pairs)
    hbm = pl.BlockSpec(memory_space=pl.ANY)
    vmem = pl.BlockSpec(memory_space=pltpu.VMEM)
    dma = pltpu.SemaphoreType.DMA
    return pl.pallas_call(
        functools.partial(attend_kernel, pairs),
        out_shape=(
            jax.ShapeDtypeStruct(k.shape, k.dtype),
            jax.ShapeDtypeStruct(v.shape, v.dtype),
            jax.ShapeDtypeStruct((batch * heads, dim), F32),
            jax.ShapeDtypeStruct((4 * heads, dim), F32),
        ),
        in_specs=[pl.BlockSpec(memory_space=pltpu.SMEM), hbm, vmem, vmem, hbm, vmem, hbm, vmem, hbm, hbm],
        out_specs=(hbm, hbm, vmem, vmem),
        scratch_shapes=[
            pltpu.VMEM(x.shape, BF16),
            pltpu.VMEM(x.shape, BF16),
            pltpu.VMEM(wq.shape, BF16),
            pltpu.VMEM(wkv.shape, BF16),
            pltpu.VMEM((batch * heads, dim), F32),
            pltpu.VMEM((batch, 2 * dim), F32),
            pltpu.VMEM((pairs * 2 * heads, pos_local), F32),
            pltpu.VMEM(k.shape, BF16),
            pltpu.VMEM(v.shape, BF16),
            dma((3,)), dma((chunks,)), dma((chunks,)), dma((chunks,)), dma((chunks,)),
        ],
        compiler_params=pltpu.CompilerParams(vmem_limit_bytes=56 * 1024 * 1024),
        cost_estimate=pl.CostEstimate(flops=2 * 2**30, bytes_accessed=72 * 2**20, transcendentals=0),
        name="attend",
    )(lens, x, gain.reshape(1, width), bias.reshape(1, width), wq, bq.reshape(1, -1), wkv, bkv.reshape(1, -1), k, v)


def solution(mesh):
    def local_step(hidden, cache_lens, k_cache, v_cache, ln_gain, ln_bias, w_query, b_query, w_kv, b_kv, w_out, b_out):
        batch, pos_local, dim = k_cache.shape
        heads = w_query.shape[1] // dim
        key_new, val_new, acc, ml = attend(
            cache_lens, hidden, ln_gain, ln_bias, w_query, b_query, w_kv, b_kv, k_cache, v_cache)
        m = ml[:2 * heads, :batch // 2].reshape(2, heads, batch // 2).transpose(2, 0, 1).reshape(batch, heads, 1)
        l = ml[2 * heads:, :batch // 2].reshape(2, heads, batch // 2).transpose(2, 0, 1).reshape(batch, heads, 1)
        top = lax.pmax(m, "sq")
        f = jnp.exp(m - top)
        num, den = lax.psum((acc.reshape(batch, heads, dim) * f, l * f), "sq")
        attended = (num / den).astype(BF16).reshape(batch, heads * dim)
        rows = batch // mesh.shape["sq"]
        mine = lax.dynamic_slice_in_dim(attended, lax.axis_index("sq") * rows, rows, 0)
        part = jnp.dot(mine, w_out, preferred_element_type=F32)
        total = lax.psum(part, "tp")
        gathered = lax.all_gather(total, "sq", axis=0, tiled=True)
        out_hidden = (hidden.astype(F32) + gathered + b_out).astype(BF16)
        return out_hidden, key_new, val_new

    cache_spec = P("dp", "sq", None)
    row_spec = P("dp", None)
    in_specs = (row_spec, P("dp"), cache_spec, cache_spec, P(None), P(None), P(None, "tp"), P("tp"), P(None, None), P(None), P("tp", None), P(None))
    out_specs = (row_spec, cache_spec, cache_spec)
    return jax.shard_map(local_step, mesh=mesh, in_specs=in_specs, out_specs=out_specs, check_vma=False)
```

```python
import functools

import jax
import jax.numpy as jnp
from jax import lax
from jax.experimental import pallas as pl
from jax.experimental.pallas import tpu as pltpu
from jax.sharding import PartitionSpec as P

F32 = jnp.float32
BF16 = jnp.bfloat16
NEG = -1e30


def attend_kernel(
    pairs, lens_ref, x_hbm, gain_ref, bias_ref, wq_hbm, bq_ref, wkv_hbm, bkv_ref, k_hbm, v_hbm,
    k_out, v_out, acc_ref, ml_ref,
    x_buf, h_buf, wq_buf, wkv_buf, q_buf, kv_buf, s_buf, k_buf, v_buf, in_sem, k_sem, v_sem, ko_sem, vo_sem,
):
    batch, pos_local, dim = k_buf.shape
    heads = wq_buf.shape[1] // dim
    per = 2 * pairs
    chunks = batch // per
    rows = 2 * heads
    first_pos = lax.axis_index("sq") * pos_local
    scale = dim ** -0.5

    x_copy = pltpu.make_async_copy(x_hbm, x_buf, in_sem.at[0])
    kv_copy = pltpu.make_async_copy(wkv_hbm, wkv_buf, in_sem.at[1])
    q_copy = pltpu.make_async_copy(wq_hbm, wq_buf, in_sem.at[2])
    x_copy.start()
    kv_copy.start()
    q_copy.start()

    def span(ref, c):
        return ref.at[pl.ds(c * per, per)]

    def k_load(c):
        return pltpu.make_async_copy(span(k_hbm, c), span(k_buf, c), k_sem.at[c])

    def v_load(c):
        return pltpu.make_async_copy(span(v_hbm, c), span(v_buf, c), v_sem.at[c])

    def k_store(c):
        return pltpu.make_async_copy(span(k_buf, c), span(k_out, c), ko_sem.at[c])

    def v_store(c):
        return pltpu.make_async_copy(span(v_buf, c), span(v_out, c), vo_sem.at[c])

    @pl.loop(0, chunks)
    def _(c):
        k_load(c).start()
        v_load(c).start()

    x_copy.wait()
    block = 32

    @pl.loop(0, batch // block)
    def _(i):
        x = x_buf[pl.ds(i * block, block), :].astype(F32)
        mean = jnp.mean(x, axis=-1, keepdims=True)
        cen = x - mean
        var = jnp.mean(cen * cen, axis=-1, keepdims=True)
        h = cen * lax.rsqrt(var + 1e-5) * gain_ref[...] + bias_ref[...]
        h_buf[pl.ds(i * block, block), :] = h.astype(BF16)

    kv_copy.wait()
    kv = jnp.dot(h_buf[...], wkv_buf[...], preferred_element_type=F32) + bkv_ref[...]
    kv_buf[...] = kv.astype(BF16).astype(F32)
    q_copy.wait()
    for n0 in range(0, heads, 2):
        cols = slice(n0 * dim, (n0 + 2) * dim)
        q = jnp.dot(h_buf[...], wq_buf[:, cols], preferred_element_type=F32) + bq_ref[:, cols]
        q = q.astype(BF16).astype(F32)
        q_buf[pl.ds(n0, batch, stride=heads), :] = q[:, :dim]
        q_buf[pl.ds(n0 + 1, batch, stride=heads), :] = q[:, dim:]

    top = lax.broadcasted_iota(jnp.int32, (rows, dim), 0) < heads
    top2 = lax.broadcasted_iota(jnp.int32, (rows, pos_local), 0) < heads
    lane = lax.broadcasted_iota(jnp.int32, (rows, dim), 1)
    place = first_pos + lax.broadcasted_iota(jnp.int32, (rows, pos_local), 1)
    sub = lax.broadcasted_iota(jnp.int32, (16, dim), 0)

    def update_rows(c):
        fresh = kv_buf[pl.ds(pl.multiple_of(c * per, per), per), :]
        for j in range(per):
            b = c * per + j
            at = lens_ref[b] - first_pos
            base = pl.multiple_of(jnp.clip(at, 0, pos_local - 1) // 16 * 16, 16)
            hit = sub == at - base
            for buf, lo in ((k_buf, 0), (v_buf, dim)):
                new = jnp.broadcast_to(fresh[j:j + 1, lo:lo + dim], (16, dim))
                old = buf[b, pl.ds(base, 16), :].astype(F32)
                buf[b, pl.ds(base, 16), :] = jnp.where(hit, new, old).astype(BF16)

    def score(c):
        out = []
        for j in range(pairs):
            p = c * pairs + j
            q = q_buf[pl.ds(pl.multiple_of(p * rows, rows), rows), :]
            lhs = jnp.concatenate([jnp.where(top, q, 0.0), jnp.where(top, 0.0, q)], axis=1).astype(BF16)
            keys = jnp.concatenate([k_buf[2 * p], k_buf[2 * p + 1]], axis=1)
            s = lax.dot_general(lhs, keys, (((1,), (1,)), ((), ())), preferred_element_type=F32)
            out.append(s)
        return out

    def weigh(c, m_all, l_all):
        for j in range(pairs):
            p = c * pairs + j
            s = s_buf[j * rows:(j + 1) * rows, :] * scale
            last = jnp.where(top2, lens_ref[2 * p], lens_ref[2 * p + 1])
            valid = place <= last
            s = jnp.where(valid, s, NEG)
            m = jnp.max(s, axis=-1, keepdims=True)
            w = jnp.where(valid, jnp.exp(s - m), 0.0)
            total = jnp.sum(w, axis=-1, keepdims=True)
            vals = jnp.concatenate([v_buf[2 * p], v_buf[2 * p + 1]], axis=1)
            o = jnp.dot(w.astype(BF16), vals, preferred_element_type=F32)
            acc_ref[pl.ds(pl.multiple_of(p * rows, rows), rows), :] = jnp.where(top, o[:, :dim], o[:, dim:])
            m_all = jnp.where(lane == p, m, m_all)
            l_all = jnp.where(lane == p, total, l_all)
        return m_all, l_all

    def put_scores(out):
        for j, s in enumerate(out):
            s_buf[j * rows:(j + 1) * rows, :] = s

    def arrive(c):
        k_load(c).wait()
        v_load(c).wait()
        update_rows(c)

    def leave(c):
        k_store(c).start()
        v_store(c).start()

    arrive(0)
    put_scores(score(0))
    leave(0)
    zero = jnp.zeros((rows, dim), F32)

    def body(c, carry):
        arrive(c + 1)
        carry = weigh(c, *carry)
        put_scores(score(c + 1))
        leave(c + 1)
        return carry

    carry = lax.fori_loop(0, chunks - 1, body, (zero, zero))
    m_all, l_all = weigh(chunks - 1, *carry)
    ml_ref[:rows, :] = m_all
    ml_ref[rows:, :] = l_all

    @pl.loop(0, chunks)
    def _(c):
        k_store(c).wait()
        v_store(c).wait()


def attend(lens, x, gain, bias, wq, bq, wkv, bkv, k, v, pairs=8):
    batch, pos_local, dim = k.shape
    width = x.shape[1]
    heads = wq.shape[1] // dim
    chunks = batch // (2 * pairs)
    hbm = pl.BlockSpec(memory_space=pl.ANY)
    vmem = pl.BlockSpec(memory_space=pltpu.VMEM)
    dma = pltpu.SemaphoreType.DMA
    return pl.pallas_call(
        functools.partial(attend_kernel, pairs),
        out_shape=(
            jax.ShapeDtypeStruct(k.shape, k.dtype),
            jax.ShapeDtypeStruct(v.shape, v.dtype),
            jax.ShapeDtypeStruct((batch * heads, dim), F32),
            jax.ShapeDtypeStruct((4 * heads, dim), F32),
        ),
        in_specs=[pl.BlockSpec(memory_space=pltpu.SMEM), hbm, vmem, vmem, hbm, vmem, hbm, vmem, hbm, hbm],
        out_specs=(hbm, hbm, vmem, vmem),
        scratch_shapes=[
            pltpu.VMEM(x.shape, BF16),
            pltpu.VMEM(x.shape, BF16),
            pltpu.VMEM(wq.shape, BF16),
            pltpu.VMEM(wkv.shape, BF16),
            pltpu.VMEM((batch * heads, dim), F32),
            pltpu.VMEM((batch, 2 * dim), F32),
            pltpu.VMEM((pairs * 2 * heads, pos_local), F32),
            pltpu.VMEM(k.shape, BF16),
            pltpu.VMEM(v.shape, BF16),
            dma((3,)), dma((chunks,)), dma((chunks,)), dma((chunks,)), dma((chunks,)),
        ],
        compiler_params=pltpu.CompilerParams(vmem_limit_bytes=56 * 1024 * 1024),
        cost_estimate=pl.CostEstimate(flops=2 * 2**30, bytes_accessed=72 * 2**20, transcendentals=0),
        name="attend",
    )(lens, x, gain.reshape(1, width), bias.reshape(1, width), wq, bq.reshape(1, -1), wkv, bkv.reshape(1, -1), k, v)


def meet_kernel(
    parts, acc_ref, ml_ref, x_hbm, wo_ref, bo_ref, out_ref,
    x_buf, sq_buf, ml_buf, a_buf, z_out, z_in, y_buf, x_sem,
    ml_send, ml_recv, sq_send, sq_recv, z_send, z_recv, g_send, g_recv, y_send, y_recv, c_send, c_recv, f_send, f_recv,
):
    n_sq, n_tp = sq_buf.shape[0] + 1, z_in.shape[0] + 1
    width = y_buf.shape[1]
    dim = acc_ref.shape[1]
    sq, tp = lax.axis_index("sq"), lax.axis_index("tp")
    own = y_buf.shape[0] // n_sq
    step = own // parts
    cols = width // n_tp
    heads = wo_ref.shape[0] // dim
    rows = 2 * heads
    pairs = step // 2
    fold = step * heads
    mesh_id = pl.DeviceIdType.MESH

    def at_sq(d):
        return {"sq": lax.rem(sq + d, n_sq)}

    def at_tp(d):
        return {"tp": lax.rem(tp + d, n_tp)}

    core = {"sq": sq + 1 - 2 * lax.rem(sq, 2)}
    across = {"sq": lax.rem(sq + 2, n_sq)}
    core_sq = sq + 1 - 2 * lax.rem(sq, 2)
    across_sq = lax.rem(sq + 2, n_sq)

    x_copy = pltpu.make_async_copy(x_hbm.at[pl.ds(pl.multiple_of(sq * own, own), own), pl.ds(pl.multiple_of(tp * cols, cols), cols)], x_buf, x_sem)
    x_copy.start()

    barrier = pltpu.get_barrier_semaphore()
    for d in range(1, n_sq):
        pl.semaphore_signal(barrier, inc=1, device_id=at_sq(d), device_id_type=mesh_id)
    for d in range(1, n_tp):
        pl.semaphore_signal(barrier, inc=1, device_id=at_tp(d), device_id_type=mesh_id)
    pl.semaphore_wait(barrier, n_sq - 1 + n_tp - 1)

    def remote(src, dst, send, recv, to):
        return pltpu.make_async_remote_copy(src_ref=src, dst_ref=dst, send_sem=send, recv_sem=recv, device_id=to, device_id_type=mesh_id)

    def ml_copy(d):
        return remote(ml_ref, ml_buf.at[d - 1], ml_send.at[d - 1], ml_recv.at[d - 1], at_sq(d))

    def sq_copy(d, c):
        start = pl.multiple_of(lax.rem(sq + d, n_sq) * (own * heads) + c * fold, fold)
        return remote(acc_ref.at[pl.ds(start, fold)], sq_buf.at[d - 1, pl.ds(c * fold, fold)], sq_send.at[d - 1, c], sq_recv.at[d - 1, c], at_sq(d))

    def z_copy(d, c):
        return remote(z_out.at[d - 1, c], z_in.at[d - 1, c], z_send.at[d - 1, c], z_recv.at[d - 1, c], at_tp(d))

    def rows_of(s, c):
        return pl.ds(pl.multiple_of(s * own + c * step, step), step)

    my_cols = pl.ds(pl.multiple_of(tp * cols, cols), cols)

    def g_copy(d, c):
        block = y_buf.at[rows_of(sq, c), my_cols]
        return remote(block, block, g_send.at[d - 1, c], g_recv.at[d - 1, c], at_tp(d))

    def y_copy(c):
        block = y_buf.at[rows_of(sq, c)]
        return remote(block, block, y_send.at[c], y_recv.at[c], across)

    def c_copy(c):
        block = y_buf.at[rows_of(sq, c)]
        return remote(block, block, c_send.at[c], c_recv.at[c], core)

    def f_copy(c):
        block = y_buf.at[rows_of(across_sq, c)]
        return remote(block, block, f_send.at[c], f_recv.at[c], core)

    for d in range(1, n_sq):
        ml_copy(d).start()
    for c in range(parts):
        for d in range(1, n_sq):
            sq_copy(d, c).start()
    x_copy.wait()

    for d in range(1, n_sq):
        ml_copy(d).wait()
    maxima = [ml_ref[:rows, :]] + [ml_buf[d, :rows, :] for d in range(n_sq - 1)]
    sums = [ml_ref[rows:, :]] + [ml_buf[d, rows:, :] for d in range(n_sq - 1)]
    top = functools.reduce(jnp.maximum, maxima)
    scales = [jnp.exp(m - top) for m in maxima]
    den = sum(e * s for e, s in zip(scales, sums))
    scales = [e / den for e in scales]
    lane = lax.broadcasted_iota(jnp.int32, (rows, dim), 1)

    def project(c):
        for d in range(1, n_sq):
            sq_copy(d, c).wait()
        for j in range(pairs):
            p = sq * (own // 2) + c * pairs + j
            pick = lane == p
            mine = pl.multiple_of(sq * (own * heads) + c * fold + j * rows, rows)
            terms = [acc_ref[pl.ds(mine, rows), :]]
            terms += [sq_buf[d, c * fold + j * rows:c * fold + (j + 1) * rows, :] for d in range(n_sq - 1)]
            total = sum(jnp.sum(jnp.where(pick, e, 0.0), axis=1, keepdims=True) * t for e, t in zip(scales, terms))
            a_buf[j * rows:(j + 1) * rows, :] = total
        lhs = jnp.concatenate([a_buf[pl.ds(n, step, stride=heads), :].astype(BF16) for n in range(heads)], axis=1)
        for d in list(range(1, n_tp)) + [0]:
            to = lax.rem(tp + d, n_tp)
            w = wo_ref[:, pl.ds(pl.multiple_of(to * cols, cols), cols)]
            z_out[(d - 1) % n_tp, c] = jnp.dot(lhs, w, preferred_element_type=F32)
            if d:
                z_copy(d, c).start()

    def finish(c):
        for d in range(1, n_tp):
            z_copy(d, c).wait()
        total = z_out[n_tp - 1, c] + sum(z_in[d, c] for d in range(n_tp - 1))
        total = total + x_buf[c * step:(c + 1) * step, :].astype(F32) + bo_ref[:, my_cols]
        y_buf[rows_of(sq, c), my_cols] = total
        for d in range(1, n_tp):
            g_copy(d, c).start()

    def spread(c):
        for d in range(1, n_tp):
            g_copy(d, c).wait()
        y_copy(c).start()
        c_copy(c).start()

    def forward(c):
        y_copy(c).wait()
        f_copy(c).start()

    def emit(s, c):
        out_ref[rows_of(s, c), :] = y_buf[rows_of(s, c), :].astype(BF16)

    def collect(c):
        emit(sq, c)
        emit(across_sq, c)
        c_copy(c).wait()
        emit(core_sq, c)
        f_copy(c).wait()
        emit(lax.rem(core_sq + 2, n_sq), c)

    stages = (project, finish, spread, forward, collect)
    for tick in range(parts + len(stages) - 1):
        for k, stage in enumerate(stages):
            if 0 <= tick - k < parts:
                stage(tick - k)


def meet(acc, ml, x, wo, bo, n_sq, n_tp, parts=4):
    batch, width = x.shape
    own = batch // n_sq
    cols = width // n_tp
    step = own // parts
    heads = wo.shape[0] // acc.shape[1]
    dim = acc.shape[1]
    hbm = pl.BlockSpec(memory_space=pl.ANY)
    vmem = pl.BlockSpec(memory_space=pltpu.VMEM)
    dma = pltpu.SemaphoreType.DMA
    return pl.pallas_call(
        functools.partial(meet_kernel, parts),
        out_shape=jax.ShapeDtypeStruct((batch, width), BF16),
        in_specs=[vmem, vmem, hbm, vmem, vmem],
        out_specs=vmem,
        scratch_shapes=[
            pltpu.VMEM((own, cols), BF16),
            pltpu.VMEM((n_sq - 1, own * heads, dim), F32),
            pltpu.VMEM((n_sq - 1,) + ml.shape, F32),
            pltpu.VMEM((step * heads, dim), F32),
            pltpu.VMEM((n_tp, parts, step, cols), F32),
            pltpu.VMEM((n_tp - 1, parts, step, cols), F32),
            pltpu.VMEM((batch, width), F32),
            dma,
            dma((n_sq - 1,)), dma((n_sq - 1,)),
            dma((n_sq - 1, parts)), dma((n_sq - 1, parts)),
            dma((n_tp - 1, parts)), dma((n_tp - 1, parts)),
            dma((n_tp - 1, parts)), dma((n_tp - 1, parts)),
            dma((parts,)), dma((parts,)), dma((parts,)), dma((parts,)), dma((parts,)), dma((parts,)),
        ],
        compiler_params=pltpu.CompilerParams(collective_id=0, has_side_effects=True, vmem_limit_bytes=24 * 1024 * 1024),
        cost_estimate=pl.CostEstimate(flops=2**28, bytes_accessed=8 * 2**20, transcendentals=0),
        name="meet",
    )(acc, ml, x, wo, bo.reshape(1, width))


def solution(mesh):
    def local_step(hidden, cache_lens, k_cache, v_cache, ln_gain, ln_bias, w_query, b_query, w_kv, b_kv, w_out, b_out):
        key_new, val_new, acc, ml = attend(
            cache_lens, hidden, ln_gain, ln_bias, w_query, b_query, w_kv, b_kv, k_cache, v_cache)
        out_hidden = meet(acc, ml, hidden, w_out, b_out, mesh.shape["sq"], mesh.shape["tp"])
        return out_hidden, key_new, val_new

    cache_spec = P("dp", "sq", None)
    row_spec = P("dp", None)
    in_specs = (row_spec, P("dp"), cache_spec, cache_spec, P(None), P(None), P(None, "tp"), P("tp"), P(None, None), P(None), P("tp", None), P(None))
    out_specs = (row_spec, cache_spec, cache_spec)
    return jax.shard_map(local_step, mesh=mesh, in_specs=in_specs, out_specs=out_specs, check_vma=False)
```

```python
import functools

import jax
import jax.numpy as jnp
from jax import lax
from jax.experimental import pallas as pl
from jax.experimental.pallas import tpu as pltpu
from jax.sharding import PartitionSpec as P

F32 = jnp.float32
BF16 = jnp.bfloat16
NEG = -1e30


def attend_kernel(
    pairs, held, lens_ref, x_hbm, gain_ref, bias_ref, wq_hbm, bq_ref, wkv_hbm, bkv_ref, k_hbm, v_hbm,
    k_out, v_out, acc_out, ml_out,
    x_buf, h_buf, wq_buf, wkv_buf, q_buf, kv_buf, s_buf, acc_ref, ml_ref, k_buf, v_buf,
    in_sem, k_sem, v_sem, ko_sem, vo_sem, acc_sem, ml_sem,
):
    batch, pos_local, dim = k_buf.shape
    heads = wq_buf.shape[1] // dim
    per = 2 * pairs
    chunks = batch // per
    rows = 2 * heads
    first_pos = lax.axis_index("sq") * pos_local
    scale = dim ** -0.5

    x_copy = pltpu.make_async_copy(x_hbm, x_buf, in_sem.at[0])
    kv_copy = pltpu.make_async_copy(wkv_hbm, wkv_buf, in_sem.at[1])
    q_copy = pltpu.make_async_copy(wq_hbm, wq_buf, in_sem.at[2])
    x_copy.start()
    kv_copy.start()
    q_copy.start()

    def span(ref, c):
        return ref.at[pl.ds(c * per, per)]

    def k_load(c):
        return pltpu.make_async_copy(span(k_hbm, c), span(k_buf, c), k_sem.at[c])

    def v_load(c):
        return pltpu.make_async_copy(span(v_hbm, c), span(v_buf, c), v_sem.at[c])

    def k_store(c):
        return pltpu.make_async_copy(span(k_buf, c), span(k_out, c), ko_sem.at[c])

    def v_store(c):
        return pltpu.make_async_copy(span(v_buf, c), span(v_out, c), vo_sem.at[c])

    @pl.loop(0, chunks)
    def _(c):
        k_load(c).start()
        v_load(c).start()

    x_copy.wait()
    block = 32

    @pl.loop(0, batch // block)
    def _(i):
        x = x_buf[pl.ds(i * block, block), :].astype(F32)
        mean = jnp.mean(x, axis=-1, keepdims=True)
        cen = x - mean
        var = jnp.mean(cen * cen, axis=-1, keepdims=True)
        h = cen * lax.rsqrt(var + 1e-5) * gain_ref[...] + bias_ref[...]
        h_buf[pl.ds(i * block, block), :] = h.astype(BF16)

    kv_copy.wait()
    kv = jnp.dot(h_buf[...], wkv_buf[...], preferred_element_type=F32) + bkv_ref[...]
    kv_buf[...] = kv.astype(BF16).astype(F32)
    q_copy.wait()
    for n0 in range(0, heads, 2):
        cols = slice(n0 * dim, (n0 + 2) * dim)
        q = jnp.dot(h_buf[...], wq_buf[:, cols], preferred_element_type=F32) + bq_ref[:, cols]
        q = q.astype(BF16).astype(F32)
        q_buf[pl.ds(n0, batch, stride=heads), :] = q[:, :dim]
        q_buf[pl.ds(n0 + 1, batch, stride=heads), :] = q[:, dim:]

    top = lax.broadcasted_iota(jnp.int32, (rows, dim), 0) < heads
    top2 = lax.broadcasted_iota(jnp.int32, (rows, pos_local), 0) < heads
    lane = lax.broadcasted_iota(jnp.int32, (rows, dim), 1)
    place = first_pos + lax.broadcasted_iota(jnp.int32, (rows, pos_local), 1)
    sub = lax.broadcasted_iota(jnp.int32, (16, dim), 0)

    def update_rows(c):
        fresh = kv_buf[pl.ds(pl.multiple_of(c * per, per), per), :]
        for j in range(per):
            b = c * per + j
            at = lens_ref[b] - first_pos
            base = pl.multiple_of(jnp.clip(at, 0, pos_local - 1) // 16 * 16, 16)
            hit = sub == at - base
            for buf, lo in ((k_buf, 0), (v_buf, dim)):
                new = jnp.broadcast_to(fresh[j:j + 1, lo:lo + dim], (16, dim))
                old = buf[b, pl.ds(base, 16), :].astype(F32)
                buf[b, pl.ds(base, 16), :] = jnp.where(hit, new, old).astype(BF16)

    def score(c):
        out = []
        for j in range(pairs):
            p = c * pairs + j
            q = q_buf[pl.ds(pl.multiple_of(p * rows, rows), rows), :]
            lhs = jnp.concatenate([jnp.where(top, q, 0.0), jnp.where(top, 0.0, q)], axis=1).astype(BF16)
            keys = jnp.concatenate([k_buf[2 * p], k_buf[2 * p + 1]], axis=1)
            s = lax.dot_general(lhs, keys, (((1,), (1,)), ((), ())), preferred_element_type=F32)
            out.append(s)
        return out

    def weigh(c, m_all, l_all):
        for j in range(pairs):
            p = c * pairs + j
            s = s_buf[j * rows:(j + 1) * rows, :] * scale
            last = jnp.where(top2, lens_ref[2 * p], lens_ref[2 * p + 1])
            valid = place <= last
            s = jnp.where(valid, s, NEG)
            m = jnp.max(s, axis=-1, keepdims=True)
            w = jnp.where(valid, jnp.exp(s - m), 0.0)
            total = jnp.sum(w, axis=-1, keepdims=True)
            vals = jnp.concatenate([v_buf[2 * p], v_buf[2 * p + 1]], axis=1)
            o = jnp.dot(w.astype(BF16), vals, preferred_element_type=F32)
            acc_ref[pl.ds(pl.multiple_of(p * rows, rows), rows), :] = jnp.where(top, o[:, :dim], o[:, dim:])
            m_all = jnp.where(lane == p, m, m_all)
            l_all = jnp.where(lane == p, total, l_all)
        return m_all, l_all

    def put_scores(out):
        for j, s in enumerate(out):
            s_buf[j * rows:(j + 1) * rows, :] = s

    def acc_store(c):
        part = pl.ds(pl.multiple_of(c * (pairs * rows), pairs * rows), pairs * rows)
        return pltpu.make_async_copy(acc_ref.at[part], acc_out.at[part], acc_sem.at[c])

    def loaded(c):
        k_load(c).wait()
        v_load(c).wait()

    def leave(c):
        k_store(c).start()
        v_store(c).start()

    loaded(0)
    update_rows(0)
    put_scores(score(0))
    zero = jnp.zeros((rows, dim), F32)

    def early(c, carry):
        loaded(c + 1)
        update_rows(c + 1)
        carry = weigh(c, *carry)
        put_scores(score(c + 1))
        acc_store(c).start()
        return carry

    carry = lax.fori_loop(0, held, early, (zero, zero))

    @pl.loop(held + 1, chunks)
    def _(c):
        loaded(c)

    @pl.loop(0, held + 1)
    def _(c):
        leave(c)

    def late(c, carry):
        update_rows(c + 1)
        carry = weigh(c, *carry)
        put_scores(score(c + 1))
        acc_store(c).start()
        leave(c + 1)
        return carry

    carry = lax.fori_loop(held, chunks - 1, late, carry)
    m_all, l_all = weigh(chunks - 1, *carry)
    ml_ref[:rows, :] = m_all
    ml_ref[rows:, :] = l_all
    acc_store(chunks - 1).start()

    @pl.loop(0, chunks - 1)
    def _(c):
        k_store(c).wait()
        v_store(c).wait()
        acc_store(c).wait()

    ml_store = pltpu.make_async_copy(ml_ref, ml_out, ml_sem)
    ml_store.start()
    k_store(chunks - 1).wait()
    v_store(chunks - 1).wait()
    acc_store(chunks - 1).wait()
    ml_store.wait()


def attend(lens, x, gain, bias, wq, bq, wkv, bkv, k, v, pairs=8, held=8):
    batch, pos_local, dim = k.shape
    width = x.shape[1]
    heads = wq.shape[1] // dim
    chunks = batch // (2 * pairs)
    hbm = pl.BlockSpec(memory_space=pltpu.HBM)
    vmem = pl.BlockSpec(memory_space=pltpu.VMEM)
    dma = pltpu.SemaphoreType.DMA
    return pl.pallas_call(
        functools.partial(attend_kernel, pairs, held),
        out_shape=(
            jax.ShapeDtypeStruct(k.shape, k.dtype),
            jax.ShapeDtypeStruct(v.shape, v.dtype),
            jax.ShapeDtypeStruct((batch * heads, dim), F32),
            jax.ShapeDtypeStruct((4 * heads, dim), F32),
        ),
        in_specs=[pl.BlockSpec(memory_space=pltpu.SMEM), hbm, vmem, vmem, hbm, vmem, hbm, vmem, hbm, hbm],
        out_specs=(hbm, hbm, hbm, hbm),
        scratch_shapes=[
            pltpu.VMEM(x.shape, BF16),
            pltpu.VMEM(x.shape, BF16),
            pltpu.VMEM(wq.shape, BF16),
            pltpu.VMEM(wkv.shape, BF16),
            pltpu.VMEM((batch * heads, dim), F32),
            pltpu.VMEM((batch, 2 * dim), F32),
            pltpu.VMEM((pairs * 2 * heads, pos_local), F32),
            pltpu.VMEM((batch * heads, dim), F32),
            pltpu.VMEM((4 * heads, dim), F32),
            pltpu.VMEM(k.shape, BF16),
            pltpu.VMEM(v.shape, BF16),
            dma((3,)), dma((chunks,)), dma((chunks,)), dma((chunks,)), dma((chunks,)), dma((chunks,)), dma,
        ],
        compiler_params=pltpu.CompilerParams(vmem_limit_bytes=60 * 1024 * 1024),
        cost_estimate=pl.CostEstimate(flops=2 * 2**30, bytes_accessed=72 * 2**20, transcendentals=0),
        name="attend",
    )(lens, x, gain.reshape(1, width), bias.reshape(1, width), wq, bq.reshape(1, -1), wkv, bkv.reshape(1, -1), k, v)


def meet_kernel(
    parts, timing, acc_hbm, ml_hbm, x_hbm, wo_hbm, bo_ref, out_ref,
    wo_ref, acc_buf, ml_own, x_buf, base_buf, sq_buf, ml_buf, a_buf, z_out, z_in, y_buf, in_sem,
    ml_send, ml_recv, sq_send, sq_recv, z_send, z_recv, l_send, l_recv, r_send, r_recv,
    y_send, y_recv, c_send, c_recv, f_send, f_recv,
):
    n_sq, n_tp = sq_buf.shape[0] + 1, z_in.shape[0] + 1
    width = y_buf.shape[1]
    dim = acc_buf.shape[1]
    sq, tp = lax.axis_index("sq"), lax.axis_index("tp")
    own = y_buf.shape[0] // n_sq
    step = own // parts
    cols = width // n_tp
    heads = wo_ref.shape[0] // dim
    rows = 2 * heads
    pairs = step // 2
    fold = step * heads
    mesh_id = pl.DeviceIdType.MESH

    def at_sq(d):
        return {"sq": lax.rem(sq + d, n_sq)}

    def at_tp(d):
        return {"tp": lax.rem(tp + d, n_tp)}

    core_sq = sq + 1 - 2 * lax.rem(sq, 2)
    across_sq = lax.rem(sq + 2, n_sq)
    core, across = {"sq": core_sq}, {"sq": across_sq}

    x_cols = pl.ds(pl.multiple_of(tp * cols, cols), cols)
    ml_in = pltpu.make_async_copy(ml_hbm, ml_own, in_sem.at[0])
    acc_in = pltpu.make_async_copy(acc_hbm, acc_buf, in_sem.at[1])
    x_in = pltpu.make_async_copy(x_hbm.at[pl.ds(pl.multiple_of(sq * own, own), own), x_cols], x_buf, in_sem.at[2])
    wo_in = pltpu.make_async_copy(wo_hbm, wo_ref, in_sem.at[3])
    ml_in.start()
    acc_in.start()
    x_in.start()
    wo_in.start()

    barrier = pltpu.get_barrier_semaphore()
    for d in range(1, n_sq):
        pl.semaphore_signal(barrier, inc=1, device_id=at_sq(d), device_id_type=mesh_id)
    for d in range(1, n_tp):
        pl.semaphore_signal(barrier, inc=1, device_id=at_tp(d), device_id_type=mesh_id)
    ml_in.wait()
    acc_in.wait()
    pl.semaphore_wait(barrier, n_sq - 1 + n_tp - 1)

    def remote(src, dst, send, recv, to):
        return pltpu.make_async_remote_copy(src_ref=src, dst_ref=dst, send_sem=send, recv_sem=recv, device_id=to, device_id_type=mesh_id)

    def ml_copy(d):
        return remote(ml_own, ml_buf.at[d - 1], ml_send.at[d - 1], ml_recv.at[d - 1], at_sq(d))

    def sq_copy(d, c):
        start = pl.multiple_of(lax.rem(sq + d, n_sq) * (own * heads) + c * fold, fold)
        return remote(acc_buf.at[pl.ds(start, fold)], sq_buf.at[d - 1, pl.ds(c * fold, fold)], sq_send.at[d - 1, c], sq_recv.at[d - 1, c], at_sq(d))

    def z_copy(d, c):
        return remote(z_out.at[d - 1, c], z_in.at[d - 1, c], z_send.at[d - 1, c], z_recv.at[d - 1, c], at_tp(d))

    def block(s, t, c):
        return y_buf.at[pl.ds(pl.multiple_of(s * own + c * step, step), step), pl.ds(pl.multiple_of(t * cols, cols), cols)]

    def source(tag):
        return tp - tag if tag < n_tp else tp + (tag - n_tp + 1)

    def right_copy(tag, c):
        b = block(sq, source(tag), c)
        return remote(b, b, l_send.at[tag, c], l_recv.at[tag + 1, c], {"tp": tp + 1})

    def left_copy(tag, c):
        b = block(sq, source(tag), c)
        hop = tag if tag == 0 else tag - n_tp + 1
        return remote(b, b, r_send.at[hop, c], r_recv.at[hop + 1, c], {"tp": tp - 1})

    def from_left(hop, c):
        b = block(sq, tp - hop, c)
        return remote(b, b, l_send.at[hop, c], l_recv.at[hop, c], {"tp": tp})

    def from_right(hop, c):
        b = block(sq, tp + hop, c)
        return remote(b, b, r_send.at[hop, c], r_recv.at[hop, c], {"tp": tp})

    def y_copy(tag, c):
        b = block(sq, source(tag), c)
        return remote(b, b, y_send.at[tag, c], y_recv.at[tag, c], across)

    def c_copy(tag, c):
        b = block(sq, source(tag), c)
        return remote(b, b, c_send.at[tag, c], c_recv.at[tag, c], core)

    def f_copy(tag, c):
        b = block(across_sq, source(tag), c)
        return remote(b, b, f_send.at[tag, c], f_recv.at[tag, c], core)

    for d in range(1, n_sq):
        ml_copy(d).start()
    for c in range(parts):
        for d in range(1, n_sq):
            sq_copy(d, c).start()
    x_in.wait()
    wo_in.wait()
    base_buf[...] = x_buf[...].astype(F32) + bo_ref[:, x_cols]

    for d in range(1, n_sq):
        ml_copy(d).wait()
    maxima = [ml_own[:rows, :]] + [ml_buf[d, :rows, :] for d in range(n_sq - 1)]
    sums = [ml_own[rows:, :]] + [ml_buf[d, rows:, :] for d in range(n_sq - 1)]
    top = functools.reduce(jnp.maximum, maxima)
    scales = [jnp.exp(m - top) for m in maxima]
    den = sum(e * s for e, s in zip(scales, sums))
    scales = [e / den for e in scales]
    lane = lax.broadcasted_iota(jnp.int32, (rows, dim), 1)

    def project(c):
        for d in range(1, n_sq):
            sq_copy(d, c).wait()
        for j in range(pairs):
            p = sq * (own // 2) + c * pairs + j
            pick = lane == p
            mine = pl.multiple_of(sq * (own * heads) + c * fold + j * rows, rows)
            terms = [acc_buf[pl.ds(mine, rows), :]]
            terms += [sq_buf[d, c * fold + j * rows:c * fold + (j + 1) * rows, :] for d in range(n_sq - 1)]
            total = sum(jnp.sum(jnp.where(pick, e, 0.0), axis=1, keepdims=True) * t for e, t in zip(scales, terms))
            a_buf[j * rows:(j + 1) * rows, :] = total
        lhs = jnp.concatenate([a_buf[pl.ds(n, step, stride=heads), :].astype(BF16) for n in range(heads)], axis=1)
        for d in list(range(1, n_tp)) + [0]:
            to = lax.rem(tp + d, n_tp)
            w = wo_ref[:, pl.ds(pl.multiple_of(to * cols, cols), cols)]
            z_out[(d - 1) % n_tp, c] = jnp.dot(lhs, w, preferred_element_type=F32)
            if d:
                z_copy(d, c).start()

    def share(tag, c):
        y_copy(tag, c).start()
        c_copy(tag, c).start()

    def when(cond):
        return pl.when(cond)

    def finish(c):
        for d in range(1, n_tp):
            z_copy(d, c).wait()
        total = z_out[n_tp - 1, c] + sum(z_in[d, c] for d in range(n_tp - 1))
        total = total + base_buf[c * step:(c + 1) * step, :]
        mine = block(sq, tp, c)
        mine[...] = total

        @when(tp < n_tp - 1)
        def _():
            right_copy(0, c).start()

        @when(tp > 0)
        def _():
            left_copy(0, c).start()

        share(0, c)

    def hop(h, c):
        @when(tp >= h)
        def _():
            from_left(h, c).wait_recv()

            @when(tp < n_tp - 1)
            def _():
                right_copy(h, c).start()

            share(h, c)

        @when(tp + h < n_tp)
        def _():
            from_right(h, c).wait_recv()

            @when(tp > 0)
            def _():
                left_copy(h + n_tp - 1, c).start()

            share(h + n_tp - 1, c)

    def crossed(h, c):
        def take(tag):
            y_copy(tag, c).wait_recv()
            f_copy(tag, c).start()

        if h == 0:
            take(0)
            return

        @when(tp >= h)
        def _():
            take(h)

        @when(tp + h < n_tp)
        def _():
            take(h + n_tp - 1)

    tau, lag, leg = timing
    events = []
    for c in range(parts):
        t = c * tau
        events.append((t, 0, functools.partial(project, c)))
        t += lag
        events.append((t, 1, functools.partial(finish, c)))
        events.append((t + leg, 3, functools.partial(crossed, 0, c)))
        for h in range(1, n_tp):
            events.append((t + h * leg, 2, functools.partial(hop, h, c)))
            events.append((t + (h + 1) * leg, 3, functools.partial(crossed, h, c)))
    for _, _, event in sorted(events, key=lambda e: e[:2]):
        event()

    def close(tag, c):
        y_copy(tag, c).wait_send()
        c_copy(tag, c).wait()
        f_copy(tag, c).wait()

    for c in range(parts):
        @when(tp < n_tp - 1)
        def _():
            right_copy(0, c).wait_send()

        @when(tp > 0)
        def _():
            left_copy(0, c).wait_send()

        close(0, c)
        for h in range(1, n_tp):
            @when(tp >= h)
            def _():
                @when(tp < n_tp - 1)
                def _():
                    right_copy(h, c).wait_send()

                close(h, c)

            @when(tp + h < n_tp)
            def _():
                @when(tp > 0)
                def _():
                    left_copy(h + n_tp - 1, c).wait_send()

                close(h + n_tp - 1, c)

    chunk = 32
    for i in range(y_buf.shape[0] // chunk):
        out_ref[i * chunk:(i + 1) * chunk, :] = y_buf[i * chunk:(i + 1) * chunk, :].astype(BF16)


def meet(acc, ml, x, wo, bo, n_sq, n_tp, parts=8, timing=(1.4, 4.0, 2.5)):
    batch, width = x.shape
    own = batch // n_sq
    cols = width // n_tp
    step = own // parts
    heads = wo.shape[0] // acc.shape[1]
    dim = acc.shape[1]
    hbm = pl.BlockSpec(memory_space=pltpu.HBM)
    vmem = pl.BlockSpec(memory_space=pltpu.VMEM)
    dma = pltpu.SemaphoreType.DMA
    tags = 2 * n_tp - 1
    return pl.pallas_call(
        functools.partial(meet_kernel, parts, timing),
        out_shape=jax.ShapeDtypeStruct((batch, width), BF16),
        in_specs=[hbm, hbm, hbm, hbm, vmem],
        out_specs=vmem,
        scratch_shapes=[
            pltpu.VMEM(wo.shape, BF16),
            pltpu.VMEM(acc.shape, F32),
            pltpu.VMEM(ml.shape, F32),
            pltpu.VMEM((own, cols), BF16),
            pltpu.VMEM((own, cols), F32),
            pltpu.VMEM((n_sq - 1, own * heads, dim), F32),
            pltpu.VMEM((n_sq - 1,) + ml.shape, F32),
            pltpu.VMEM((step * heads, dim), F32),
            pltpu.VMEM((n_tp, parts, step, cols), F32),
            pltpu.VMEM((n_tp - 1, parts, step, cols), F32),
            pltpu.VMEM((batch, width), F32),
            dma((4,)),
            dma((n_sq - 1,)), dma((n_sq - 1,)),
            dma((n_sq - 1, parts)), dma((n_sq - 1, parts)),
            dma((n_tp - 1, parts)), dma((n_tp - 1, parts)),
            dma((n_tp + 1, parts)), dma((n_tp + 1, parts)),
            dma((n_tp + 1, parts)), dma((n_tp + 1, parts)),
            dma((tags, parts)), dma((tags, parts)),
            dma((tags, parts)), dma((tags, parts)),
            dma((tags, parts)), dma((tags, parts)),
        ],
        compiler_params=pltpu.CompilerParams(collective_id=0, has_side_effects=True, vmem_limit_bytes=60 * 1024 * 1024),
        cost_estimate=pl.CostEstimate(flops=2**28, bytes_accessed=8 * 2**20, transcendentals=0),
        name="meet",
    )(acc, ml, x, wo, bo.reshape(1, width))


def solution(mesh):
    def local_step(hidden, cache_lens, k_cache, v_cache, ln_gain, ln_bias, w_query, b_query, w_kv, b_kv, w_out, b_out):
        key_new, val_new, acc, ml = attend(
            cache_lens, hidden, ln_gain, ln_bias, w_query, b_query, w_kv, b_kv, k_cache, v_cache)
        out_hidden = meet(acc, ml, hidden, w_out, b_out, mesh.shape["sq"], mesh.shape["tp"])
        return out_hidden, key_new, val_new

    cache_spec = P("dp", "sq", None)
    row_spec = P("dp", None)
    in_specs = (row_spec, P("dp"), cache_spec, cache_spec, P(None), P(None), P(None, "tp"), P("tp"), P(None, None), P(None), P("tp", None), P(None))
    out_specs = (row_spec, cache_spec, cache_spec)
    return jax.shard_map(local_step, mesh=mesh, in_specs=in_specs, out_specs=out_specs, check_vma=False)
```

```python
import functools

import jax
import jax.numpy as jnp
from jax import lax
from jax.experimental import pallas as pl
from jax.experimental.pallas import tpu as pltpu
from jax.sharding import PartitionSpec as P

F32 = jnp.float32
BF16 = jnp.bfloat16
NEG = -1e30


def attend_kernel(
    pairs, held, lens_ref, x_hbm, gain_ref, bias_ref, wq_hbm, bq_ref, wkv_hbm, bkv_ref, k_hbm, v_hbm,
    k_out, v_out, acc_out, ml_out,
    x_buf, h_buf, wq_buf, wkv_buf, q_buf, kv_buf, s_buf, acc_ref, ml_ref, k_buf, v_buf,
    in_sem, k_sem, v_sem, ko_sem, vo_sem, acc_sem, ml_sem,
):
    batch, pos_local, dim = k_buf.shape
    heads = wq_buf.shape[1] // dim
    per = 2 * pairs
    chunks = batch // per
    rows = 2 * heads
    first_pos = lax.axis_index("sq") * pos_local
    scale = dim ** -0.5

    x_copy = pltpu.make_async_copy(x_hbm, x_buf, in_sem.at[0])
    kv_copy = pltpu.make_async_copy(wkv_hbm, wkv_buf, in_sem.at[1])
    q_copy = pltpu.make_async_copy(wq_hbm, wq_buf, in_sem.at[2])
    x_copy.start()
    kv_copy.start()
    q_copy.start()

    def span(ref, c):
        return ref.at[pl.ds(c * per, per)]

    def k_load(c):
        return pltpu.make_async_copy(span(k_hbm, c), span(k_buf, c), k_sem.at[c])

    def v_load(c):
        return pltpu.make_async_copy(span(v_hbm, c), span(v_buf, c), v_sem.at[c])

    def k_store(c):
        return pltpu.make_async_copy(span(k_buf, c), span(k_out, c), ko_sem.at[c])

    def v_store(c):
        return pltpu.make_async_copy(span(v_buf, c), span(v_out, c), vo_sem.at[c])

    @pl.loop(0, chunks)
    def _(c):
        k_load(c).start()
        v_load(c).start()

    x_copy.wait()
    block = 32

    @pl.loop(0, batch // block)
    def _(i):
        x = x_buf[pl.ds(i * block, block), :].astype(F32)
        mean = jnp.mean(x, axis=-1, keepdims=True)
        cen = x - mean
        var = jnp.mean(cen * cen, axis=-1, keepdims=True)
        h = cen * lax.rsqrt(var + 1e-5) * gain_ref[...] + bias_ref[...]
        h_buf[pl.ds(i * block, block), :] = h.astype(BF16)

    kv_copy.wait()
    kv = jnp.dot(h_buf[...], wkv_buf[...], preferred_element_type=F32) + bkv_ref[...]
    kv_buf[...] = kv.astype(BF16).astype(F32)
    q_copy.wait()
    for n0 in range(0, heads, 2):
        cols = slice(n0 * dim, (n0 + 2) * dim)
        q = jnp.dot(h_buf[...], wq_buf[:, cols], preferred_element_type=F32) + bq_ref[:, cols]
        q = q.astype(BF16).astype(F32)
        q_buf[pl.ds(n0, batch, stride=heads), :] = q[:, :dim]
        q_buf[pl.ds(n0 + 1, batch, stride=heads), :] = q[:, dim:]

    top = lax.broadcasted_iota(jnp.int32, (rows, dim), 0) < heads
    top2 = lax.broadcasted_iota(jnp.int32, (rows, pos_local), 0) < heads
    lane = lax.broadcasted_iota(jnp.int32, (rows, dim), 1)
    place = first_pos + lax.broadcasted_iota(jnp.int32, (rows, pos_local), 1)
    sub = lax.broadcasted_iota(jnp.int32, (16, dim), 0)

    def update_rows(c):
        fresh = kv_buf[pl.ds(pl.multiple_of(c * per, per), per), :]
        for j in range(per):
            b = c * per + j
            at = lens_ref[b] - first_pos
            base = pl.multiple_of(jnp.clip(at, 0, pos_local - 1) // 16 * 16, 16)
            hit = sub == at - base
            for buf, lo in ((k_buf, 0), (v_buf, dim)):
                new = jnp.broadcast_to(fresh[j:j + 1, lo:lo + dim], (16, dim))
                old = buf[b, pl.ds(base, 16), :].astype(F32)
                buf[b, pl.ds(base, 16), :] = jnp.where(hit, new, old).astype(BF16)

    def score(c):
        out = []
        for j in range(pairs):
            p = c * pairs + j
            q = q_buf[pl.ds(pl.multiple_of(p * rows, rows), rows), :]
            lhs = jnp.concatenate([jnp.where(top, q, 0.0), jnp.where(top, 0.0, q)], axis=1).astype(BF16)
            keys = jnp.concatenate([k_buf[2 * p], k_buf[2 * p + 1]], axis=1)
            s = lax.dot_general(lhs, keys, (((1,), (1,)), ((), ())), preferred_element_type=F32)
            out.append(s)
        return out

    def weigh(c, m_all, l_all):
        for j in range(pairs):
            p = c * pairs + j
            s = s_buf[j * rows:(j + 1) * rows, :] * scale
            last = jnp.where(top2, lens_ref[2 * p], lens_ref[2 * p + 1])
            valid = place <= last
            s = jnp.where(valid, s, NEG)
            m = jnp.max(s, axis=-1, keepdims=True)
            w = jnp.where(valid, jnp.exp(s - m), 0.0)
            total = jnp.sum(w, axis=-1, keepdims=True)
            vals = jnp.concatenate([v_buf[2 * p], v_buf[2 * p + 1]], axis=1)
            o = jnp.dot(w.astype(BF16), vals, preferred_element_type=F32)
            acc_ref[pl.ds(pl.multiple_of(p * rows, rows), rows), :] = jnp.where(top, o[:, :dim], o[:, dim:])
            m_all = jnp.where(lane == p, m, m_all)
            l_all = jnp.where(lane == p, total, l_all)
        return m_all, l_all

    def put_scores(out):
        for j, s in enumerate(out):
            s_buf[j * rows:(j + 1) * rows, :] = s

    def acc_store(c):
        part = pl.ds(pl.multiple_of(c * (pairs * rows), pairs * rows), pairs * rows)
        return pltpu.make_async_copy(acc_ref.at[part], acc_out.at[part], acc_sem.at[c])

    def loaded(c):
        k_load(c).wait()
        v_load(c).wait()

    def leave(c):
        k_store(c).start()
        v_store(c).start()

    loaded(0)
    update_rows(0)
    put_scores(score(0))
    zero = jnp.zeros((rows, dim), F32)

    def early(c, carry):
        loaded(c + 1)
        update_rows(c + 1)
        carry = weigh(c, *carry)
        put_scores(score(c + 1))
        acc_store(c).start()
        return carry

    carry = lax.fori_loop(0, held, early, (zero, zero))

    @pl.loop(held + 1, chunks)
    def _(c):
        loaded(c)

    @pl.loop(0, held + 1)
    def _(c):
        leave(c)

    def late(c, carry):
        update_rows(c + 1)
        carry = weigh(c, *carry)
        put_scores(score(c + 1))
        acc_store(c).start()
        leave(c + 1)
        return carry

    carry = lax.fori_loop(held, chunks - 1, late, carry)
    m_all, l_all = weigh(chunks - 1, *carry)
    ml_ref[:rows, :] = m_all
    ml_ref[rows:, :] = l_all
    acc_store(chunks - 1).start()

    @pl.loop(0, chunks - 1)
    def _(c):
        k_store(c).wait()
        v_store(c).wait()
        acc_store(c).wait()

    ml_store = pltpu.make_async_copy(ml_ref, ml_out, ml_sem)
    ml_store.start()
    k_store(chunks - 1).wait()
    v_store(chunks - 1).wait()
    acc_store(chunks - 1).wait()
    ml_store.wait()


def attend(lens, x, gain, bias, wq, bq, wkv, bkv, k, v, pairs=8, held=8):
    batch, pos_local, dim = k.shape
    width = x.shape[1]
    heads = wq.shape[1] // dim
    chunks = batch // (2 * pairs)
    hbm = pl.BlockSpec(memory_space=pltpu.HBM)
    vmem = pl.BlockSpec(memory_space=pltpu.VMEM)
    dma = pltpu.SemaphoreType.DMA
    return pl.pallas_call(
        functools.partial(attend_kernel, pairs, held),
        out_shape=(
            jax.ShapeDtypeStruct(k.shape, k.dtype),
            jax.ShapeDtypeStruct(v.shape, v.dtype),
            jax.ShapeDtypeStruct((batch * heads, dim), F32),
            jax.ShapeDtypeStruct((4 * heads, dim), F32),
        ),
        in_specs=[pl.BlockSpec(memory_space=pltpu.SMEM), hbm, vmem, vmem, hbm, vmem, hbm, vmem, hbm, hbm],
        out_specs=(hbm, hbm, hbm, hbm),
        scratch_shapes=[
            pltpu.VMEM(x.shape, BF16),
            pltpu.VMEM(x.shape, BF16),
            pltpu.VMEM(wq.shape, BF16),
            pltpu.VMEM(wkv.shape, BF16),
            pltpu.VMEM((batch * heads, dim), F32),
            pltpu.VMEM((batch, 2 * dim), F32),
            pltpu.VMEM((pairs * 2 * heads, pos_local), F32),
            pltpu.VMEM((batch * heads, dim), F32),
            pltpu.VMEM((4 * heads, dim), F32),
            pltpu.VMEM(k.shape, BF16),
            pltpu.VMEM(v.shape, BF16),
            dma((3,)), dma((chunks,)), dma((chunks,)), dma((chunks,)), dma((chunks,)), dma((chunks,)), dma,
        ],
        compiler_params=pltpu.CompilerParams(vmem_limit_bytes=60 * 1024 * 1024),
        cost_estimate=pl.CostEstimate(flops=2 * 2**30, bytes_accessed=72 * 2**20, transcendentals=0),
        name="attend",
    )(lens, x, gain.reshape(1, width), bias.reshape(1, width), wq, bq.reshape(1, -1), wkv, bkv.reshape(1, -1), k, v)


def meet_kernel(
    parts, relayed, acc_hbm, ml_hbm, x_hbm, wo_hbm, bo_hbm, out_ref,
    wo_ref, bo_ref, acc_buf, ml_own, x_buf, base_buf, sq_buf, ml_buf, a_buf, z_out, z_in, y_buf, in_sem,
    ml_send, ml_recv, sq_send, sq_recv, z_send, z_recv, g_send, g_recv, l_send, l_recv, r_send, r_recv,
    y_send, y_recv, c_send, c_recv, f_send, f_recv,
):
    n_sq, n_tp = sq_buf.shape[0] + 1, z_in.shape[0] + 1
    width = y_buf.shape[1]
    dim = acc_buf.shape[1]
    sq, tp = lax.axis_index("sq"), lax.axis_index("tp")
    own = y_buf.shape[0] // n_sq
    step = own // parts
    cols = width // n_tp
    heads = wo_ref.shape[0] // dim
    rows = 2 * heads
    pairs = step // 2
    fold = step * heads
    mesh_id = pl.DeviceIdType.MESH

    def at_sq(d):
        return {"sq": lax.rem(sq + d, n_sq)}

    def at_tp(d):
        return {"tp": lax.rem(tp + d, n_tp)}

    core_sq = sq + 1 - 2 * lax.rem(sq, 2)
    across_sq = lax.rem(sq + 2, n_sq)
    core, across = {"sq": core_sq}, {"sq": across_sq}

    barrier = pltpu.get_barrier_semaphore()
    for d in range(1, n_sq):
        pl.semaphore_signal(barrier, inc=1, device_id=at_sq(d), device_id_type=mesh_id)
    for d in range(1, n_tp):
        pl.semaphore_signal(barrier, inc=1, device_id=at_tp(d), device_id_type=mesh_id)
    x_cols = pl.ds(pl.multiple_of(tp * cols, cols), cols)
    ml_in = pltpu.make_async_copy(ml_hbm, ml_own, in_sem.at[0])
    acc_in = pltpu.make_async_copy(acc_hbm, acc_buf, in_sem.at[1])
    x_in = pltpu.make_async_copy(x_hbm.at[pl.ds(pl.multiple_of(sq * own, own), own), x_cols], x_buf, in_sem.at[2])
    wo_in = pltpu.make_async_copy(wo_hbm, wo_ref, in_sem.at[3])
    bo_in = pltpu.make_async_copy(bo_hbm.at[:, x_cols], bo_ref, in_sem.at[4])
    ml_in.start()
    acc_in.start()
    x_in.start()
    bo_in.start()
    wo_in.start()

    ml_in.wait()
    acc_in.wait()
    pl.semaphore_wait(barrier, n_sq - 1 + n_tp - 1)

    def remote(src, dst, send, recv, to):
        return pltpu.make_async_remote_copy(src_ref=src, dst_ref=dst, send_sem=send, recv_sem=recv, device_id=to, device_id_type=mesh_id)

    def ml_copy(d):
        return remote(ml_own, ml_buf.at[d - 1], ml_send.at[d - 1], ml_recv.at[d - 1], at_sq(d))

    def sq_copy(d, c):
        start = pl.multiple_of(lax.rem(sq + d, n_sq) * (own * heads) + c * fold, fold)
        return remote(acc_buf.at[pl.ds(start, fold)], sq_buf.at[d - 1, pl.ds(c * fold, fold)], sq_send.at[d - 1, c], sq_recv.at[d - 1, c], at_sq(d))

    def z_copy(d, c):
        return remote(z_out.at[d - 1, c], z_in.at[d - 1, c], z_send.at[d - 1, c], z_recv.at[d - 1, c], at_tp(d))

    def block(s, t, c):
        return y_buf.at[pl.ds(pl.multiple_of(s * own + c * step, step), step), pl.ds(pl.multiple_of(t * cols, cols), cols)]

    def source(tag):
        return tp - tag if tag < n_tp else tp + (tag - n_tp + 1)

    def right_copy(tag, c):
        b = block(sq, source(tag), c)
        return remote(b, b, l_send.at[tag, c], l_recv.at[tag + 1, c], {"tp": tp + 1})

    def left_copy(tag, c):
        b = block(sq, source(tag), c)
        hop = tag if tag == 0 else tag - n_tp + 1
        return remote(b, b, r_send.at[hop, c], r_recv.at[hop + 1, c], {"tp": tp - 1})

    def from_left(hop, c):
        b = block(sq, tp - hop, c)
        return remote(b, b, l_send.at[hop, c], l_recv.at[hop, c], {"tp": tp})

    def from_right(hop, c):
        b = block(sq, tp + hop, c)
        return remote(b, b, r_send.at[hop, c], r_recv.at[hop, c], {"tp": tp})

    def source_of(tag, c):
        return source(tag) if c < relayed else lax.rem(tp - tag + n_tp, n_tp)

    def g_copy(d, c):
        b = block(sq, tp, c)
        return remote(b, b, g_send.at[d - 1, c], g_recv.at[d - 1, c], at_tp(d))

    def y_copy(tag, c):
        b = block(sq, source_of(tag, c), c)
        return remote(b, b, y_send.at[tag, c], y_recv.at[tag, c], across)

    def c_copy(tag, c):
        b = block(sq, source_of(tag, c), c)
        return remote(b, b, c_send.at[tag, c], c_recv.at[tag, c], core)

    def f_copy(tag, c):
        b = block(across_sq, source_of(tag, c), c)
        return remote(b, b, f_send.at[tag, c], f_recv.at[tag, c], core)

    for d in range(1, n_sq):
        ml_copy(d).start()
    for c in range(parts):
        for d in range(1, n_sq):
            sq_copy(d, c).start()
    x_in.wait()
    wo_in.wait()
    bo_in.wait()
    base_buf[...] = x_buf[...].astype(F32) + bo_ref[...]

    for d in range(1, n_sq):
        ml_copy(d).wait()
    maxima = [ml_own[:rows, :]] + [ml_buf[d, :rows, :] for d in range(n_sq - 1)]
    sums = [ml_own[rows:, :]] + [ml_buf[d, rows:, :] for d in range(n_sq - 1)]
    top = functools.reduce(jnp.maximum, maxima)
    scales = [jnp.exp(m - top) for m in maxima]
    den = sum(e * s for e, s in zip(scales, sums))
    scales = [e / den for e in scales]
    lane = lax.broadcasted_iota(jnp.int32, (rows, dim), 1)

    def project(c):
        for d in range(1, n_sq):
            sq_copy(d, c).wait()
        for j in range(pairs):
            p = sq * (own // 2) + c * pairs + j
            pick = lane == p
            mine = pl.multiple_of(sq * (own * heads) + c * fold + j * rows, rows)
            terms = [acc_buf[pl.ds(mine, rows), :]]
            terms += [sq_buf[d, c * fold + j * rows:c * fold + (j + 1) * rows, :] for d in range(n_sq - 1)]
            total = sum(jnp.sum(jnp.where(pick, e, 0.0), axis=1, keepdims=True) * t for e, t in zip(scales, terms))
            a_buf[j * rows:(j + 1) * rows, :] = total
        lhs = jnp.concatenate([a_buf[pl.ds(n, step, stride=heads), :].astype(BF16) for n in range(heads)], axis=1)
        for d in list(range(1, n_tp)) + [0]:
            to = lax.rem(tp + d, n_tp)
            w = wo_ref[:, pl.ds(pl.multiple_of(to * cols, cols), cols)]
            z_out[(d - 1) % n_tp, c] = jnp.dot(lhs, w, preferred_element_type=F32)
        for d in range(1, n_tp):
            z_copy(d, c).start()

    def share(tag, c):
        y_copy(tag, c).start()
        c_copy(tag, c).start()

    def when(cond):
        return pl.when(cond)

    def finish(c):
        for d in range(1, n_tp):
            z_copy(d, c).wait()
        total = z_out[n_tp - 1, c] + sum(z_in[d, c] for d in range(n_tp - 1))
        total = total + base_buf[c * step:(c + 1) * step, :]
        mine = block(sq, tp, c)
        mine[...] = total

        if c < relayed:
            @when(tp < n_tp - 1)
            def _():
                right_copy(0, c).start()

            @when(tp > 0)
            def _():
                left_copy(0, c).start()
        else:
            for d in range(1, n_tp):
                g_copy(d, c).start()

        share(0, c)

    def direct(d, c):
        g_copy(d, c).wait_recv()
        share(d, c)

    def hop(h, c):
        @when(tp >= h)
        def _():
            from_left(h, c).wait_recv()

            @when(tp < n_tp - 1)
            def _():
                right_copy(h, c).start()

            share(h, c)

        @when(tp + h < n_tp)
        def _():
            from_right(h, c).wait_recv()

            @when(tp > 0)
            def _():
                left_copy(h + n_tp - 1, c).start()

            share(h + n_tp - 1, c)

    def crossed(h, c):
        def take(tag):
            y_copy(tag, c).wait_recv()
            f_copy(tag, c).start()

        if h == 0 or c >= relayed:
            take(h)
            return

        @when(tp >= h)
        def _():
            take(h)

        @when(tp + h < n_tp)
        def _():
            take(h + n_tp - 1)

    slow = 11.2 / parts
    events = []
    for c in range(parts):
        events.append((6.3 + 5.6 / parts * c, 0, functools.partial(project, c)))
        t = 9.3 + slow * (c + 1)
        events.append((t, 1, functools.partial(finish, c)))
        events.append((t + 2.7, 3, functools.partial(crossed, 0, c)))
        for h in range(1, n_tp):
            if c < relayed:
                there = t + 3.0 * h
                events.append((there, 2, functools.partial(hop, h, c)))
            else:
                there = t + (4.0 if h == 2 else 3.0) + 0.5 * h
                events.append((there, 2, functools.partial(direct, h, c)))
            events.append((there + 2.7, 3, functools.partial(crossed, h, c)))
    for _, _, event in sorted(events, key=lambda e: e[:2]):
        event()

    def close(tag, c):
        y_copy(tag, c).wait_send()
        c_copy(tag, c).wait()
        f_copy(tag, c).wait()

    for c in range(parts):
        close(0, c)
        if c >= relayed:
            for d in range(1, n_tp):
                g_copy(d, c).wait_send()
                close(d, c)
            continue

        @when(tp < n_tp - 1)
        def _():
            right_copy(0, c).wait_send()

        @when(tp > 0)
        def _():
            left_copy(0, c).wait_send()

        for h in range(1, n_tp):
            @when(tp >= h)
            def _():
                @when(tp < n_tp - 1)
                def _():
                    right_copy(h, c).wait_send()

                close(h, c)

            @when(tp + h < n_tp)
            def _():
                @when(tp > 0)
                def _():
                    left_copy(h + n_tp - 1, c).wait_send()

                close(h + n_tp - 1, c)

    chunk = 32
    for i in range(y_buf.shape[0] // chunk):
        out_ref[i * chunk:(i + 1) * chunk, :] = y_buf[i * chunk:(i + 1) * chunk, :].astype(BF16)


def meet(acc, ml, x, wo, bo, n_sq, n_tp, parts=4, relayed=2):
    batch, width = x.shape
    own = batch // n_sq
    cols = width // n_tp
    step = own // parts
    heads = wo.shape[0] // acc.shape[1]
    dim = acc.shape[1]
    hbm = pl.BlockSpec(memory_space=pltpu.HBM)
    vmem = pl.BlockSpec(memory_space=pltpu.VMEM)
    dma = pltpu.SemaphoreType.DMA
    tags = 2 * n_tp - 1
    return pl.pallas_call(
        functools.partial(meet_kernel, parts, relayed),
        out_shape=jax.ShapeDtypeStruct((batch, width), BF16),
        in_specs=[hbm, hbm, hbm, hbm, hbm],
        out_specs=vmem,
        scratch_shapes=[
            pltpu.VMEM(wo.shape, BF16),
            pltpu.VMEM((1, cols), F32),
            pltpu.VMEM(acc.shape, F32),
            pltpu.VMEM(ml.shape, F32),
            pltpu.VMEM((own, cols), BF16),
            pltpu.VMEM((own, cols), F32),
            pltpu.VMEM((n_sq - 1, own * heads, dim), F32),
            pltpu.VMEM((n_sq - 1,) + ml.shape, F32),
            pltpu.VMEM((step * heads, dim), F32),
            pltpu.VMEM((n_tp, parts, step, cols), F32),
            pltpu.VMEM((n_tp - 1, parts, step, cols), F32),
            pltpu.VMEM((batch, width), F32),
            dma((5,)),
            dma((n_sq - 1,)), dma((n_sq - 1,)),
            dma((n_sq - 1, parts)), dma((n_sq - 1, parts)),
            dma((n_tp - 1, parts)), dma((n_tp - 1, parts)),
            dma((n_tp - 1, parts)), dma((n_tp - 1, parts)),
            dma((n_tp + 1, parts)), dma((n_tp + 1, parts)),
            dma((n_tp + 1, parts)), dma((n_tp + 1, parts)),
            dma((tags, parts)), dma((tags, parts)),
            dma((tags, parts)), dma((tags, parts)),
            dma((tags, parts)), dma((tags, parts)),
        ],
        compiler_params=pltpu.CompilerParams(collective_id=0, has_side_effects=True, vmem_limit_bytes=60 * 1024 * 1024),
        cost_estimate=pl.CostEstimate(flops=2**28, bytes_accessed=8 * 2**20, transcendentals=0),
        name="meet",
    )(acc, ml, x, wo, bo.reshape(1, width))


def solution(mesh):
    def local_step(hidden, cache_lens, k_cache, v_cache, ln_gain, ln_bias, w_query, b_query, w_kv, b_kv, w_out, b_out):
        key_new, val_new, acc, ml = attend(
            cache_lens, hidden, ln_gain, ln_bias, w_query, b_query, w_kv, b_kv, k_cache, v_cache)
        out_hidden = meet(acc, ml, hidden, w_out, b_out, mesh.shape["sq"], mesh.shape["tp"])
        return out_hidden, key_new, val_new

    cache_spec = P("dp", "sq", None)
    row_spec = P("dp", None)
    in_specs = (row_spec, P("dp"), cache_spec, cache_spec, P(None), P(None), P(None, "tp"), P("tp"), P(None, None), P(None), P("tp", None), P(None))
    out_specs = (row_spec, cache_spec, cache_spec)
    return jax.shard_map(local_step, mesh=mesh, in_specs=in_specs, out_specs=out_specs, check_vma=False)
```

```python
import functools

import jax
import jax.numpy as jnp
from jax import lax
from jax.experimental import pallas as pl
from jax.experimental.pallas import tpu as pltpu
from jax.sharding import PartitionSpec as P

F32 = jnp.float32
BF16 = jnp.bfloat16
NEG = -1e30


def attend_kernel(
    pairs, held, lens_ref, x_hbm, gain_ref, bias_ref, wq_hbm, bq_ref, wkv_hbm, bkv_ref, k_hbm, v_hbm,
    k_out, v_out, acc_out,
    x_buf, h_buf, wq_buf, wkv_buf, q_buf, kv_buf, s_buf, acc_ref, ml_ref, k_buf, v_buf,
    in_sem, k_sem, v_sem, ko_sem, vo_sem, acc_sem, ml_sem,
):
    batch, pos_local, dim = k_buf.shape
    heads = wq_buf.shape[1] // dim
    per = 2 * pairs
    chunks = batch // per
    rows = 2 * heads
    first_pos = lax.axis_index("sq") * pos_local
    scale = dim ** -0.5

    x_copy = pltpu.make_async_copy(x_hbm, x_buf, in_sem.at[0])
    kv_copy = pltpu.make_async_copy(wkv_hbm, wkv_buf, in_sem.at[1])
    q_copy = pltpu.make_async_copy(wq_hbm, wq_buf, in_sem.at[2])
    x_copy.start()
    kv_copy.start()
    q_copy.start()

    def span(ref, c):
        return ref.at[pl.ds(c * per, per)]

    def k_load(c):
        return pltpu.make_async_copy(span(k_hbm, c), span(k_buf, c), k_sem.at[c])

    def v_load(c):
        return pltpu.make_async_copy(span(v_hbm, c), span(v_buf, c), v_sem.at[c])

    def k_store(c):
        return pltpu.make_async_copy(span(k_buf, c), span(k_out, c), ko_sem.at[c])

    def v_store(c):
        return pltpu.make_async_copy(span(v_buf, c), span(v_out, c), vo_sem.at[c])

    @pl.loop(0, chunks)
    def _(c):
        k_load(c).start()
        v_load(c).start()

    x_copy.wait()
    block = 32

    @pl.loop(0, batch // block)
    def _(i):
        x = x_buf[pl.ds(i * block, block), :].astype(F32)
        mean = jnp.mean(x, axis=-1, keepdims=True)
        cen = x - mean
        var = jnp.mean(cen * cen, axis=-1, keepdims=True)
        h = cen * lax.rsqrt(var + 1e-5) * gain_ref[...] + bias_ref[...]
        h_buf[pl.ds(i * block, block), :] = h.astype(BF16)

    kv_copy.wait()
    kv = jnp.dot(h_buf[...], wkv_buf[...], preferred_element_type=F32) + bkv_ref[...]
    kv_buf[...] = kv.astype(BF16).astype(F32)
    q_copy.wait()
    for n0 in range(0, heads, 2):
        cols = slice(n0 * dim, (n0 + 2) * dim)
        q = jnp.dot(h_buf[...], wq_buf[:, cols], preferred_element_type=F32) + bq_ref[:, cols]
        q = q.astype(BF16).astype(F32)
        q_buf[pl.ds(n0, batch, stride=heads), :] = q[:, :dim]
        q_buf[pl.ds(n0 + 1, batch, stride=heads), :] = q[:, dim:]

    top = lax.broadcasted_iota(jnp.int32, (rows, dim), 0) < heads
    top2 = lax.broadcasted_iota(jnp.int32, (rows, pos_local), 0) < heads
    lane = lax.broadcasted_iota(jnp.int32, (rows, dim), 1)
    place = first_pos + lax.broadcasted_iota(jnp.int32, (rows, pos_local), 1)
    sub = lax.broadcasted_iota(jnp.int32, (16, dim), 0)

    def update_rows(c):
        fresh = kv_buf[pl.ds(pl.multiple_of(c * per, per), per), :]
        for j in range(per):
            b = c * per + j
            at = lens_ref[b] - first_pos
            base = pl.multiple_of(jnp.clip(at, 0, pos_local - 1) // 16 * 16, 16)
            hit = sub == at - base
            for buf, lo in ((k_buf, 0), (v_buf, dim)):
                new = jnp.broadcast_to(fresh[j:j + 1, lo:lo + dim], (16, dim))
                old = buf[b, pl.ds(base, 16), :].astype(F32)
                buf[b, pl.ds(base, 16), :] = jnp.where(hit, new, old).astype(BF16)

    def score(c):
        out = []
        for j in range(pairs):
            p = c * pairs + j
            q = q_buf[pl.ds(pl.multiple_of(p * rows, rows), rows), :]
            lhs = jnp.concatenate([jnp.where(top, q, 0.0), jnp.where(top, 0.0, q)], axis=1).astype(BF16)
            keys = jnp.concatenate([k_buf[2 * p], k_buf[2 * p + 1]], axis=1)
            s = lax.dot_general(lhs, keys, (((1,), (1,)), ((), ())), preferred_element_type=F32)
            out.append(s)
        return out

    def weigh(c, m_all, l_all):
        for j in range(pairs):
            p = c * pairs + j
            s = s_buf[j * rows:(j + 1) * rows, :] * scale
            last = jnp.where(top2, lens_ref[2 * p], lens_ref[2 * p + 1])
            valid = place <= last
            s = jnp.where(valid, s, NEG)
            m = jnp.max(s, axis=-1, keepdims=True)
            w = jnp.where(valid, jnp.exp(s - m), 0.0)
            total = jnp.sum(w, axis=-1, keepdims=True)
            vals = jnp.concatenate([v_buf[2 * p], v_buf[2 * p + 1]], axis=1)
            o = jnp.dot(w.astype(BF16), vals, preferred_element_type=F32)
            acc_ref[pl.ds(pl.multiple_of(p * rows, rows), rows), :] = jnp.where(top, o[:, :dim], o[:, dim:])
            m_all = jnp.where(lane == p, m, m_all)
            l_all = jnp.where(lane == p, total, l_all)
        return m_all, l_all

    def put_scores(out):
        for j, s in enumerate(out):
            s_buf[j * rows:(j + 1) * rows, :] = s

    def acc_store(c):
        part = pl.ds(pl.multiple_of(c * (pairs * rows), pairs * rows), pairs * rows)
        return pltpu.make_async_copy(acc_ref.at[part], acc_out.at[part], acc_sem.at[c])

    def loaded(c):
        k_load(c).wait()
        v_load(c).wait()

    def leave(c):
        k_store(c).start()
        v_store(c).start()

    loaded(0)
    update_rows(0)
    put_scores(score(0))
    zero = jnp.zeros((rows, dim), F32)

    def early(c, carry):
        loaded(c + 1)
        update_rows(c + 1)
        carry = weigh(c, *carry)
        put_scores(score(c + 1))
        acc_store(c).start()
        return carry

    carry = lax.fori_loop(0, held, early, (zero, zero))

    @pl.loop(held + 1, chunks)
    def _(c):
        loaded(c)

    @pl.loop(0, held + 1)
    def _(c):
        leave(c)

    def late(c, carry):
        update_rows(c + 1)
        carry = weigh(c, *carry)
        put_scores(score(c + 1))
        acc_store(c).start()
        leave(c + 1)
        return carry

    carry = lax.fori_loop(held, chunks - 1, late, carry)
    m_all, l_all = weigh(chunks - 1, *carry)
    ml_ref[:rows, :] = m_all
    ml_ref[rows:, :] = l_all
    acc_store(chunks - 1).start()

    @pl.loop(0, chunks - 1)
    def _(c):
        k_store(c).wait()
        v_store(c).wait()
        acc_store(c).wait()

    ml_store = pltpu.make_async_copy(ml_ref, acc_out.at[pl.ds(batch * heads, 2 * rows)], ml_sem)
    ml_store.start()
    k_store(chunks - 1).wait()
    v_store(chunks - 1).wait()
    acc_store(chunks - 1).wait()
    ml_store.wait()


def attend(lens, x, gain, bias, wq, bq, wkv, bkv, k, v, pairs=8, held=8):
    batch, pos_local, dim = k.shape
    width = x.shape[1]
    heads = wq.shape[1] // dim
    chunks = batch // (2 * pairs)
    hbm = pl.BlockSpec(memory_space=pltpu.HBM)
    vmem = pl.BlockSpec(memory_space=pltpu.VMEM)
    dma = pltpu.SemaphoreType.DMA
    return pl.pallas_call(
        functools.partial(attend_kernel, pairs, held),
        out_shape=(
            jax.ShapeDtypeStruct(k.shape, k.dtype),
            jax.ShapeDtypeStruct(v.shape, v.dtype),
            jax.ShapeDtypeStruct((batch * heads + 4 * heads, dim), F32),
        ),
        in_specs=[pl.BlockSpec(memory_space=pltpu.SMEM), hbm, vmem, vmem, hbm, vmem, hbm, vmem, hbm, hbm],
        out_specs=(hbm, hbm, hbm),
        scratch_shapes=[
            pltpu.VMEM(x.shape, BF16),
            pltpu.VMEM(x.shape, BF16),
            pltpu.VMEM(wq.shape, BF16),
            pltpu.VMEM(wkv.shape, BF16),
            pltpu.VMEM((batch * heads, dim), F32),
            pltpu.VMEM((batch, 2 * dim), F32),
            pltpu.VMEM((pairs * 2 * heads, pos_local), F32),
            pltpu.VMEM((batch * heads, dim), F32),
            pltpu.VMEM((4 * heads, dim), F32),
            pltpu.VMEM(k.shape, BF16),
            pltpu.VMEM(v.shape, BF16),
            dma((3,)), dma((chunks,)), dma((chunks,)), dma((chunks,)), dma((chunks,)), dma((chunks,)), dma,
        ],
        compiler_params=pltpu.CompilerParams(vmem_limit_bytes=60 * 1024 * 1024),
        cost_estimate=pl.CostEstimate(flops=2 * 2**30, bytes_accessed=72 * 2**20, transcendentals=0),
        name="attend",
    )(lens, x, gain.reshape(1, width), bias.reshape(1, width), wq, bq.reshape(1, -1), wkv, bkv.reshape(1, -1), k, v)


def meet_kernel(
    parts, relayed, acc_buf, x_ref, wo_ref, bo_ref, out_ref,
    base_buf, sq_buf, ml_buf, a_buf, z_out, z_in, y_buf,
    ml_send, ml_recv, sq_send, sq_recv, z_send, z_recv, g_send, g_recv, l_send, l_recv, r_send, r_recv,
    y_send, y_recv, c_send, c_recv, f_send, f_recv,
):
    n_sq, n_tp = sq_buf.shape[0] + 1, z_in.shape[0] + 1
    width = y_buf.shape[1]
    dim = acc_buf.shape[1]
    sq, tp = lax.axis_index("sq"), lax.axis_index("tp")
    own = y_buf.shape[0] // n_sq
    step = own // parts
    cols = width // n_tp
    heads = wo_ref.shape[0] // dim
    rows = 2 * heads
    pairs = step // 2
    fold = step * heads
    mesh_id = pl.DeviceIdType.MESH

    def at_sq(d):
        return {"sq": lax.rem(sq + d, n_sq)}

    def at_tp(d):
        return {"tp": lax.rem(tp + d, n_tp)}

    core_sq = sq + 1 - 2 * lax.rem(sq, 2)
    across_sq = lax.rem(sq + 2, n_sq)
    core, across = {"sq": core_sq}, {"sq": across_sq}

    barrier = pltpu.get_barrier_semaphore()
    for d in range(1, n_sq):
        pl.semaphore_signal(barrier, inc=1, device_id=at_sq(d), device_id_type=mesh_id)
    for d in range(1, n_tp):
        pl.semaphore_signal(barrier, inc=1, device_id=at_tp(d), device_id_type=mesh_id)
    x_cols = pl.ds(pl.multiple_of(tp * cols, cols), cols)
    base_buf[...] = x_ref[pl.ds(pl.multiple_of(sq * own, own), own), x_cols].astype(F32) + bo_ref[:, x_cols]
    ml_own = acc_buf.at[pl.ds(own * n_sq * heads, 2 * rows)]
    with jax.named_scope('barrier'):
        pl.semaphore_wait(barrier, n_sq - 1 + n_tp - 1)

    def remote(src, dst, send, recv, to):
        return pltpu.make_async_remote_copy(src_ref=src, dst_ref=dst, send_sem=send, recv_sem=recv, device_id=to, device_id_type=mesh_id)

    def ml_copy(d):
        return remote(ml_own, ml_buf.at[d - 1], ml_send.at[d - 1], ml_recv.at[d - 1], at_sq(d))

    def sq_copy(d, c):
        start = pl.multiple_of(lax.rem(sq + d, n_sq) * (own * heads) + c * fold, fold)
        return remote(acc_buf.at[pl.ds(start, fold)], sq_buf.at[d - 1, pl.ds(c * fold, fold)], sq_send.at[d - 1, c], sq_recv.at[d - 1, c], at_sq(d))

    def z_copy(d, c):
        return remote(z_out.at[d - 1, c], z_in.at[d - 1, c], z_send.at[d - 1, c], z_recv.at[d - 1, c], at_tp(d))

    def block(s, t, c):
        return y_buf.at[pl.ds(pl.multiple_of(s * own + c * step, step), step), pl.ds(pl.multiple_of(t * cols, cols), cols)]

    def source(tag):
        return tp - tag if tag < n_tp else tp + (tag - n_tp + 1)

    def right_copy(tag, c):
        b = block(sq, source(tag), c)
        return remote(b, b, l_send.at[tag, c], l_recv.at[tag + 1, c], {"tp": tp + 1})

    def left_copy(tag, c):
        b = block(sq, source(tag), c)
        hop = tag if tag == 0 else tag - n_tp + 1
        return remote(b, b, r_send.at[hop, c], r_recv.at[hop + 1, c], {"tp": tp - 1})

    def from_left(hop, c):
        b = block(sq, tp - hop, c)
        return remote(b, b, l_send.at[hop, c], l_recv.at[hop, c], {"tp": tp})

    def from_right(hop, c):
        b = block(sq, tp + hop, c)
        return remote(b, b, r_send.at[hop, c], r_recv.at[hop, c], {"tp": tp})

    def source_of(tag, c):
        return source(tag) if c < relayed else lax.rem(tp - tag + n_tp, n_tp)

    def g_copy(d, c):
        b = block(sq, tp, c)
        return remote(b, b, g_send.at[d - 1, c], g_recv.at[d - 1, c], at_tp(d))

    def y_copy(tag, c):
        b = block(sq, source_of(tag, c), c)
        return remote(b, b, y_send.at[tag, c], y_recv.at[tag, c], across)

    def c_copy(tag, c):
        b = block(sq, source_of(tag, c), c)
        return remote(b, b, c_send.at[tag, c], c_recv.at[tag, c], core)

    def f_copy(tag, c):
        b = block(across_sq, source_of(tag, c), c)
        return remote(b, b, f_send.at[tag, c], f_recv.at[tag, c], core)

    for d in range(1, n_sq):
        ml_copy(d).start()
    for c in range(parts):
        for d in range(1, n_sq):
            sq_copy(d, c).start()

    with jax.named_scope('mlwait'):
        for d in range(1, n_sq):
            ml_copy(d).wait()
    maxima = [acc_buf[own * n_sq * heads:own * n_sq * heads + rows, :]] + [ml_buf[d, :rows, :] for d in range(n_sq - 1)]
    sums = [acc_buf[own * n_sq * heads + rows:, :]] + [ml_buf[d, rows:, :] for d in range(n_sq - 1)]
    top = functools.reduce(jnp.maximum, maxima)
    scales = [jnp.exp(m - top) for m in maxima]
    den = sum(e * s for e, s in zip(scales, sums))
    scales = [e / den for e in scales]
    lane = lax.broadcasted_iota(jnp.int32, (rows, dim), 1)

    def project(c):
        for d in range(1, n_sq):
            sq_copy(d, c).wait()
        for j in range(pairs):
            p = sq * (own // 2) + c * pairs + j
            pick = lane == p
            mine = pl.multiple_of(sq * (own * heads) + c * fold + j * rows, rows)
            terms = [acc_buf[pl.ds(mine, rows), :]]
            terms += [sq_buf[d, c * fold + j * rows:c * fold + (j + 1) * rows, :] for d in range(n_sq - 1)]
            total = sum(jnp.sum(jnp.where(pick, e, 0.0), axis=1, keepdims=True) * t for e, t in zip(scales, terms))
            a_buf[j * rows:(j + 1) * rows, :] = total
        lhs = jnp.concatenate([a_buf[pl.ds(n, step, stride=heads), :].astype(BF16) for n in range(heads)], axis=1)
        for d in list(range(1, n_tp)) + [0]:
            to = lax.rem(tp + d, n_tp)
            w = wo_ref[:, pl.ds(pl.multiple_of(to * cols, cols), cols)]
            z_out[(d - 1) % n_tp, c] = jnp.dot(lhs, w, preferred_element_type=F32)
        for d in range(1, n_tp):
            z_copy(d, c).start()

    def share(tag, c):
        y_copy(tag, c).start()
        c_copy(tag, c).start()

    def when(cond):
        return pl.when(cond)

    def finish(c):
        for d in range(1, n_tp):
            z_copy(d, c).wait()
        total = z_out[n_tp - 1, c] + sum(z_in[d, c] for d in range(n_tp - 1))
        total = total + base_buf[c * step:(c + 1) * step, :]
        mine = block(sq, tp, c)
        mine[...] = total

        if c < relayed:
            @when(tp < n_tp - 1)
            def _():
                right_copy(0, c).start()

            @when(tp > 0)
            def _():
                left_copy(0, c).start()
        else:
            for d in range(1, n_tp):
                g_copy(d, c).start()

        share(0, c)

    def direct(d, c):
        g_copy(d, c).wait_recv()
        share(d, c)

    def hop(h, c):
        @when(tp >= h)
        def _():
            from_left(h, c).wait_recv()

            @when(tp < n_tp - 1)
            def _():
                right_copy(h, c).start()

            share(h, c)

        @when(tp + h < n_tp)
        def _():
            from_right(h, c).wait_recv()

            @when(tp > 0)
            def _():
                left_copy(h + n_tp - 1, c).start()

            share(h + n_tp - 1, c)

    def crossed(h, c):
        def take(tag):
            y_copy(tag, c).wait_recv()
            f_copy(tag, c).start()

        if h == 0 or c >= relayed:
            take(h)
            return

        @when(tp >= h)
        def _():
            take(h)

        @when(tp + h < n_tp)
        def _():
            take(h + n_tp - 1)

    def named(name, fn, *args):
        def run():
            with jax.named_scope(name):
                fn(*args)
        return run

    slow = 11.2 / parts
    events = []
    for c in range(parts):
        events.append((6.3 + 5.6 / parts * c, 0, named(f"p{c}", project, c)))
        t = 9.3 + slow * (c + 1)
        events.append((t, 1, named(f"f{c}", finish, c)))
        events.append((t + 3, 3, named(f"y{c}_0", crossed, 0, c)))
        for h in range(1, n_tp):
            if c < relayed:
                there = t + 3.0 * h
                events.append((there, 2, named(f"h{c}_{h}", hop, h, c)))
            else:
                there = 21 + slow * c + 0.25 * slow * h
                events.append((there, 2, named(f"d{c}_{h}", direct, h, c)))
            events.append((there + 2.7, 3, named(f"y{c}_{h}", crossed, h, c)))
    for _, _, event in sorted(events, key=lambda e: e[:2]):
        event()

    def close(tag, c):
        y_copy(tag, c).wait_send()
        c_copy(tag, c).wait()
        f_copy(tag, c).wait()

    for c in range(parts):
        close(0, c)
        if c >= relayed:
            for d in range(1, n_tp):
                g_copy(d, c).wait_send()
                close(d, c)
            continue

        @when(tp < n_tp - 1)
        def _():
            right_copy(0, c).wait_send()

        @when(tp > 0)
        def _():
            left_copy(0, c).wait_send()

        for h in range(1, n_tp):
            @when(tp >= h)
            def _():
                @when(tp < n_tp - 1)
                def _():
                    right_copy(h, c).wait_send()

                close(h, c)

            @when(tp + h < n_tp)
            def _():
                @when(tp > 0)
                def _():
                    left_copy(h + n_tp - 1, c).wait_send()

                close(h + n_tp - 1, c)

    chunk = 32
    for i in range(y_buf.shape[0] // chunk):
      with jax.named_scope(f'emit{i}'):
        out_ref[i * chunk:(i + 1) * chunk, :] = y_buf[i * chunk:(i + 1) * chunk, :].astype(BF16)


def meet(acc, x, wo, bo, n_sq, n_tp, parts=4, relayed=0):
    batch, width = x.shape
    own = batch // n_sq
    cols = width // n_tp
    step = own // parts
    heads = wo.shape[0] // acc.shape[1]
    dim = acc.shape[1]
    vmem = pl.BlockSpec(memory_space=pltpu.VMEM)
    dma = pltpu.SemaphoreType.DMA
    tags = 2 * n_tp - 1
    return pl.pallas_call(
        functools.partial(meet_kernel, parts, relayed),
        out_shape=jax.ShapeDtypeStruct((batch, width), BF16),
        in_specs=[vmem] * 4,
        out_specs=vmem,
        scratch_shapes=[
            pltpu.VMEM((own, cols), F32),
            pltpu.VMEM((n_sq - 1, own * heads, dim), F32),
            pltpu.VMEM((n_sq - 1, 4 * heads, dim), F32),
            pltpu.VMEM((step * heads, dim), F32),
            pltpu.VMEM((n_tp, parts, step, cols), F32),
            pltpu.VMEM((n_tp - 1, parts, step, cols), F32),
            pltpu.VMEM((batch, width), F32),
            dma((n_sq - 1,)), dma((n_sq - 1,)),
            dma((n_sq - 1, parts)), dma((n_sq - 1, parts)),
            dma((n_tp - 1, parts)), dma((n_tp - 1, parts)),
            dma((n_tp - 1, parts)), dma((n_tp - 1, parts)),
            dma((n_tp + 1, parts)), dma((n_tp + 1, parts)),
            dma((n_tp + 1, parts)), dma((n_tp + 1, parts)),
            dma((tags, parts)), dma((tags, parts)),
            dma((tags, parts)), dma((tags, parts)),
            dma((tags, parts)), dma((tags, parts)),
        ],
        compiler_params=pltpu.CompilerParams(collective_id=0, has_side_effects=True, vmem_limit_bytes=32 * 1024 * 1024),
        cost_estimate=pl.CostEstimate(flops=2**28, bytes_accessed=8 * 2**20, transcendentals=0),
        name="meet",
    )(acc, x, wo, bo.reshape(1, width))


def solution(mesh):
    def local_step(hidden, cache_lens, k_cache, v_cache, ln_gain, ln_bias, w_query, b_query, w_kv, b_kv, w_out, b_out):
        key_new, val_new, acc = attend(
            cache_lens, hidden, ln_gain, ln_bias, w_query, b_query, w_kv, b_kv, k_cache, v_cache)
        out_hidden = meet(acc, hidden, w_out, b_out, mesh.shape["sq"], mesh.shape["tp"])
        return out_hidden, key_new, val_new

    cache_spec = P("dp", "sq", None)
    row_spec = P("dp", None)
    in_specs = (row_spec, P("dp"), cache_spec, cache_spec, P(None), P(None), P(None, "tp"), P("tp"), P(None, None), P(None), P("tp", None), P(None))
    out_specs = (row_spec, cache_spec, cache_spec)
    return jax.shard_map(local_step, mesh=mesh, in_specs=in_specs, out_specs=out_specs, check_vma=False)
```

```python
import functools

import jax
import jax.numpy as jnp
from jax import lax
from jax.experimental import pallas as pl
from jax.experimental.pallas import tpu as pltpu
from jax.sharding import PartitionSpec as P

F32 = jnp.float32
BF16 = jnp.bfloat16
NEG = -1e30


def attend_kernel(
    pairs, held, lens_ref, x_hbm, gain_ref, bias_ref, wq_hbm, bq_ref, wkv_hbm, bkv_ref, k_hbm, v_hbm,
    k_out, v_out, acc_out,
    x_buf, h_buf, wq_buf, wkv_buf, q_buf, kv_buf, s_buf, acc_ref, ml_ref, k_buf, v_buf,
    in_sem, k_sem, v_sem, ko_sem, vo_sem, acc_sem, ml_sem,
):
    batch, pos_local, dim = k_buf.shape
    heads = wq_buf.shape[1] // dim
    per = 2 * pairs
    chunks = batch // per
    rows = 2 * heads
    first_pos = lax.axis_index("sq") * pos_local
    scale = dim ** -0.5

    x_copy = pltpu.make_async_copy(x_hbm, x_buf, in_sem.at[0])
    kv_copy = pltpu.make_async_copy(wkv_hbm, wkv_buf, in_sem.at[1])
    q_copy = pltpu.make_async_copy(wq_hbm, wq_buf, in_sem.at[2])
    x_copy.start()
    kv_copy.start()
    q_copy.start()

    def span(ref, c):
        return ref.at[pl.ds(c * per, per)]

    def k_load(c):
        return pltpu.make_async_copy(span(k_hbm, c), span(k_buf, c), k_sem.at[c])

    def v_load(c):
        return pltpu.make_async_copy(span(v_hbm, c), span(v_buf, c), v_sem.at[c])

    def k_store(c):
        return pltpu.make_async_copy(span(k_buf, c), span(k_out, c), ko_sem.at[c])

    def v_store(c):
        return pltpu.make_async_copy(span(v_buf, c), span(v_out, c), vo_sem.at[c])

    @pl.loop(0, chunks)
    def _(c):
        k_load(c).start()
        v_load(c).start()

    x_copy.wait()
    block = 32

    @pl.loop(0, batch // block)
    def _(i):
        x = x_buf[pl.ds(i * block, block), :].astype(F32)
        mean = jnp.mean(x, axis=-1, keepdims=True)
        cen = x - mean
        var = jnp.mean(cen * cen, axis=-1, keepdims=True)
        h = cen * lax.rsqrt(var + 1e-5) * gain_ref[...] + bias_ref[...]
        h_buf[pl.ds(i * block, block), :] = h.astype(BF16)

    kv_copy.wait()
    kv = jnp.dot(h_buf[...], wkv_buf[...], preferred_element_type=F32) + bkv_ref[...]
    kv_buf[...] = kv.astype(BF16).astype(F32)
    q_copy.wait()
    for n0 in range(0, heads, 2):
        cols = slice(n0 * dim, (n0 + 2) * dim)
        q = jnp.dot(h_buf[...], wq_buf[:, cols], preferred_element_type=F32) + bq_ref[:, cols]
        q = q.astype(BF16).astype(F32)
        q_buf[pl.ds(n0, batch, stride=heads), :] = q[:, :dim]
        q_buf[pl.ds(n0 + 1, batch, stride=heads), :] = q[:, dim:]

    top = lax.broadcasted_iota(jnp.int32, (rows, dim), 0) < heads
    top2 = lax.broadcasted_iota(jnp.int32, (rows, pos_local), 0) < heads
    lane = lax.broadcasted_iota(jnp.int32, (rows, dim), 1)
    place = first_pos + lax.broadcasted_iota(jnp.int32, (rows, pos_local), 1)
    sub = lax.broadcasted_iota(jnp.int32, (16, dim), 0)

    def update_rows(c):
        fresh = kv_buf[pl.ds(pl.multiple_of(c * per, per), per), :]
        for j in range(per):
            b = c * per + j
            at = lens_ref[b] - first_pos
            base = pl.multiple_of(jnp.clip(at, 0, pos_local - 1) // 16 * 16, 16)
            hit = sub == at - base
            for buf, lo in ((k_buf, 0), (v_buf, dim)):
                new = jnp.broadcast_to(fresh[j:j + 1, lo:lo + dim], (16, dim))
                old = buf[b, pl.ds(base, 16), :].astype(F32)
                buf[b, pl.ds(base, 16), :] = jnp.where(hit, new, old).astype(BF16)

    def score(c):
        out = []
        for j in range(pairs):
            p = c * pairs + j
            q = q_buf[pl.ds(pl.multiple_of(p * rows, rows), rows), :]
            lhs = jnp.concatenate([jnp.where(top, q, 0.0), jnp.where(top, 0.0, q)], axis=1).astype(BF16)
            keys = jnp.concatenate([k_buf[2 * p], k_buf[2 * p + 1]], axis=1)
            s = lax.dot_general(lhs, keys, (((1,), (1,)), ((), ())), preferred_element_type=F32)
            out.append(s)
        return out

    def weigh(c, m_all, l_all):
        for j in range(pairs):
            p = c * pairs + j
            s = s_buf[j * rows:(j + 1) * rows, :] * scale
            last = jnp.where(top2, lens_ref[2 * p], lens_ref[2 * p + 1])
            valid = place <= last
            s = jnp.where(valid, s, NEG)
            m = jnp.max(s, axis=-1, keepdims=True)
            w = jnp.where(valid, jnp.exp(s - m), 0.0)
            total = jnp.sum(w, axis=-1, keepdims=True)
            vals = jnp.concatenate([v_buf[2 * p], v_buf[2 * p + 1]], axis=1)
            o = jnp.dot(w.astype(BF16), vals, preferred_element_type=F32)
            acc_ref[pl.ds(pl.multiple_of(p * rows, rows), rows), :] = jnp.where(top, o[:, :dim], o[:, dim:])
            m_all = jnp.where(lane == p, m, m_all)
            l_all = jnp.where(lane == p, total, l_all)
        return m_all, l_all

    def put_scores(out):
        for j, s in enumerate(out):
            s_buf[j * rows:(j + 1) * rows, :] = s

    def acc_store(c):
        part = pl.ds(pl.multiple_of(c * (pairs * rows), pairs * rows), pairs * rows)
        return pltpu.make_async_copy(acc_ref.at[part], acc_out.at[part], acc_sem.at[c])

    def loaded(c):
        k_load(c).wait()
        v_load(c).wait()

    def leave(c):
        k_store(c).start()
        v_store(c).start()

    loaded(0)
    update_rows(0)
    put_scores(score(0))
    zero = jnp.zeros((rows, dim), F32)

    def early(c, carry):
        loaded(c + 1)
        update_rows(c + 1)
        carry = weigh(c, *carry)
        put_scores(score(c + 1))
        acc_store(c).start()
        return carry

    carry = lax.fori_loop(0, held, early, (zero, zero))

    @pl.loop(held + 1, chunks)
    def _(c):
        loaded(c)

    @pl.loop(0, held + 1)
    def _(c):
        leave(c)

    def late(c, carry):
        update_rows(c + 1)
        carry = weigh(c, *carry)
        put_scores(score(c + 1))
        acc_store(c).start()
        leave(c + 1)
        return carry

    carry = lax.fori_loop(held, chunks - 1, late, carry)
    m_all, l_all = weigh(chunks - 1, *carry)
    ml_ref[:rows, :] = m_all
    ml_ref[rows:, :] = l_all
    acc_store(chunks - 1).start()

    @pl.loop(0, chunks - 1)
    def _(c):
        k_store(c).wait()
        v_store(c).wait()
        acc_store(c).wait()

    ml_store = pltpu.make_async_copy(ml_ref, acc_out.at[pl.ds(batch * heads, 2 * rows)], ml_sem)
    ml_store.start()
    k_store(chunks - 1).wait()
    v_store(chunks - 1).wait()
    acc_store(chunks - 1).wait()
    ml_store.wait()


def attend(lens, x, gain, bias, wq, bq, wkv, bkv, k, v, pairs=8, held=8):
    batch, pos_local, dim = k.shape
    width = x.shape[1]
    heads = wq.shape[1] // dim
    chunks = batch // (2 * pairs)
    hbm = pl.BlockSpec(memory_space=pltpu.HBM)
    vmem = pl.BlockSpec(memory_space=pltpu.VMEM)
    dma = pltpu.SemaphoreType.DMA
    return pl.pallas_call(
        functools.partial(attend_kernel, pairs, held),
        out_shape=(
            jax.ShapeDtypeStruct(k.shape, k.dtype),
            jax.ShapeDtypeStruct(v.shape, v.dtype),
            jax.ShapeDtypeStruct((batch * heads + 4 * heads, dim), F32),
        ),
        in_specs=[pl.BlockSpec(memory_space=pltpu.SMEM), hbm, vmem, vmem, hbm, vmem, hbm, vmem, hbm, hbm],
        out_specs=(hbm, hbm, hbm),
        scratch_shapes=[
            pltpu.VMEM(x.shape, BF16),
            pltpu.VMEM(x.shape, BF16),
            pltpu.VMEM(wq.shape, BF16),
            pltpu.VMEM(wkv.shape, BF16),
            pltpu.VMEM((batch * heads, dim), F32),
            pltpu.VMEM((batch, 2 * dim), F32),
            pltpu.VMEM((pairs * 2 * heads, pos_local), F32),
            pltpu.VMEM((batch * heads, dim), F32),
            pltpu.VMEM((4 * heads, dim), F32),
            pltpu.VMEM(k.shape, BF16),
            pltpu.VMEM(v.shape, BF16),
            dma((3,)), dma((chunks,)), dma((chunks,)), dma((chunks,)), dma((chunks,)), dma((chunks,)), dma,
        ],
        compiler_params=pltpu.CompilerParams(vmem_limit_bytes=60 * 1024 * 1024),
        cost_estimate=pl.CostEstimate(flops=2 * 2**30, bytes_accessed=72 * 2**20, transcendentals=0),
        name="attend",
    )(lens, x, gain.reshape(1, width), bias.reshape(1, width), wq, bq.reshape(1, -1), wkv, bkv.reshape(1, -1), k, v)


def meet_kernel(
    parts, relayed, acc_buf, x_ref, wo_ref, bo_ref, out_ref,
    base_buf, sq_buf, ml_buf, a_buf, z_out, far_in, near_buf, far_buf, y_buf,
    ml_send, ml_recv, sq_send, sq_recv, m_send, m_recv, n_send, n_recv, s_send, s_recv, g_send, g_recv, l_send, l_recv, r_send, r_recv,
    y_send, y_recv, c_send, c_recv, f_send, f_recv,
):
    n_sq, n_tp = sq_buf.shape[0] + 1, z_out.shape[1]
    width = y_buf.shape[1]
    dim = acc_buf.shape[1]
    sq, tp = lax.axis_index("sq"), lax.axis_index("tp")
    own = y_buf.shape[0] // n_sq
    step = own // parts
    cols = width // n_tp
    heads = wo_ref.shape[0] // dim
    rows = 2 * heads
    pairs = step // 2
    fold = step * heads
    mesh_id = pl.DeviceIdType.MESH

    def at_sq(d):
        return {"sq": lax.rem(sq + d, n_sq)}

    def at_tp(d):
        return {"tp": lax.rem(tp + d, n_tp)}

    core_sq = sq + 1 - 2 * lax.rem(sq, 2)
    across_sq = lax.rem(sq + 2, n_sq)
    core, across = {"sq": core_sq}, {"sq": across_sq}

    barrier = pltpu.get_barrier_semaphore()
    for d in range(1, n_sq):
        pl.semaphore_signal(barrier, inc=1, device_id=at_sq(d), device_id_type=mesh_id)
    for d in range(1, n_tp):
        pl.semaphore_signal(barrier, inc=1, device_id=at_tp(d), device_id_type=mesh_id)
    x_cols = pl.ds(pl.multiple_of(tp * cols, cols), cols)
    base_buf[...] = x_ref[pl.ds(pl.multiple_of(sq * own, own), own), x_cols].astype(F32) + bo_ref[:, x_cols]
    ml_own = acc_buf.at[pl.ds(own * n_sq * heads, 2 * rows)]
    with jax.named_scope('barrier'):
        pl.semaphore_wait(barrier, n_sq - 1 + n_tp - 1)

    def remote(src, dst, send, recv, to):
        return pltpu.make_async_remote_copy(src_ref=src, dst_ref=dst, send_sem=send, recv_sem=recv, device_id=to, device_id_type=mesh_id)

    def ml_copy(d):
        return remote(ml_own, ml_buf.at[d - 1], ml_send.at[d - 1], ml_recv.at[d - 1], at_sq(d))

    def sq_copy(d, c):
        start = pl.multiple_of(lax.rem(sq + d, n_sq) * (own * heads) + c * fold, fold)
        return remote(acc_buf.at[pl.ds(start, fold)], sq_buf.at[d - 1, pl.ds(c * fold, fold)], sq_send.at[d - 1, c], sq_recv.at[d - 1, c], at_sq(d))

    half = n_tp // 2
    middle = lax.div(tp + 1, 2) == 1
    partner = tp + 1 - 2 * lax.rem(tp, 2)
    far = half - half * lax.div(tp, half)

    def m_copy(c):
        return remote(z_out.at[c, pl.ds(far, half)], far_in.at[c], m_send.at[c], m_recv.at[c], {"tp": partner})

    def n_copy(c):
        return remote(z_out.at[c, partner], near_buf.at[c], n_send.at[c], n_recv.at[c], {"tp": partner})

    def s_copy(k, c):
        return remote(z_out.at[c, far + k], far_buf.at[c], s_send.at[k, c], s_recv.at[c], {"tp": far + k})

    def block(s, t, c):
        return y_buf.at[pl.ds(pl.multiple_of(s * own + c * step, step), step), pl.ds(pl.multiple_of(t * cols, cols), cols)]

    def source(tag):
        return tp - tag if tag < n_tp else tp + (tag - n_tp + 1)

    def right_copy(tag, c):
        b = block(sq, source(tag), c)
        return remote(b, b, l_send.at[tag, c], l_recv.at[tag + 1, c], {"tp": tp + 1})

    def left_copy(tag, c):
        b = block(sq, source(tag), c)
        hop = tag if tag == 0 else tag - n_tp + 1
        return remote(b, b, r_send.at[hop, c], r_recv.at[hop + 1, c], {"tp": tp - 1})

    def from_left(hop, c):
        b = block(sq, tp - hop, c)
        return remote(b, b, l_send.at[hop, c], l_recv.at[hop, c], {"tp": tp})

    def from_right(hop, c):
        b = block(sq, tp + hop, c)
        return remote(b, b, r_send.at[hop, c], r_recv.at[hop, c], {"tp": tp})

    def source_of(tag, c):
        return source(tag) if c < relayed else lax.rem(tp - tag + n_tp, n_tp)

    def g_copy(d, c):
        b = block(sq, tp, c)
        return remote(b, b, g_send.at[d - 1, c], g_recv.at[d - 1, c], at_tp(d))

    def y_copy(tag, c):
        b = block(sq, source_of(tag, c), c)
        return remote(b, b, y_send.at[tag, c], y_recv.at[tag, c], across)

    def c_copy(tag, c):
        b = block(sq, source_of(tag, c), c)
        return remote(b, b, c_send.at[tag, c], c_recv.at[tag, c], core)

    def f_copy(tag, c):
        b = block(across_sq, source_of(tag, c), c)
        return remote(b, b, f_send.at[tag, c], f_recv.at[tag, c], core)

    for d in range(1, n_sq):
        ml_copy(d).start()
    for c in range(parts):
        for d in range(1, n_sq):
            sq_copy(d, c).start()

    with jax.named_scope('mlwait'):
        for d in range(1, n_sq):
            ml_copy(d).wait()
    maxima = [acc_buf[own * n_sq * heads:own * n_sq * heads + rows, :]] + [ml_buf[d, :rows, :] for d in range(n_sq - 1)]
    sums = [acc_buf[own * n_sq * heads + rows:, :]] + [ml_buf[d, rows:, :] for d in range(n_sq - 1)]
    top = functools.reduce(jnp.maximum, maxima)
    scales = [jnp.exp(m - top) for m in maxima]
    den = sum(e * s for e, s in zip(scales, sums))
    scales = [e / den for e in scales]
    lane = lax.broadcasted_iota(jnp.int32, (rows, dim), 1)

    def when(cond):
        return pl.when(cond)

    def project(c):
        for d in range(1, n_sq):
            sq_copy(d, c).wait()
        for j in range(pairs):
            p = sq * (own // 2) + c * pairs + j
            pick = lane == p
            mine = pl.multiple_of(sq * (own * heads) + c * fold + j * rows, rows)
            terms = [acc_buf[pl.ds(mine, rows), :]]
            terms += [sq_buf[d, c * fold + j * rows:c * fold + (j + 1) * rows, :] for d in range(n_sq - 1)]
            total = sum(jnp.sum(jnp.where(pick, e, 0.0), axis=1, keepdims=True) * t for e, t in zip(scales, terms))
            a_buf[j * rows:(j + 1) * rows, :] = total
        lhs = jnp.concatenate([a_buf[pl.ds(n, step, stride=heads), :].astype(BF16) for n in range(heads)], axis=1)
        for t in range(n_tp):
            z_out[c, t] = jnp.dot(lhs, wo_ref[:, t * cols:(t + 1) * cols], preferred_element_type=F32)

        @when(jnp.logical_not(middle))
        def _():
            m_copy(c).start()

        n_copy(c).start()

    def add(c):
        @when(middle)
        def _():
            m_copy(c).wait_recv()
            for k in range(half):
                z_out[c, far + k] = z_out[c, far + k] + far_in[c, k]
            for k in range(half):
                s_copy(k, c).start()

    def share(tag, c):
        y_copy(tag, c).start()
        c_copy(tag, c).start()

    def finish(c):
        n_copy(c).wait_recv()
        s_copy(0, c).wait_recv()
        total = z_out[c, tp] + near_buf[c] + far_buf[c]
        total = total + base_buf[c * step:(c + 1) * step, :]
        mine = block(sq, tp, c)
        mine[...] = total

        if c < relayed:
            @when(tp < n_tp - 1)
            def _():
                right_copy(0, c).start()

            @when(tp > 0)
            def _():
                left_copy(0, c).start()
        else:
            for d in range(1, n_tp):
                g_copy(d, c).start()

        share(0, c)

    def direct(d, c):
        g_copy(d, c).wait_recv()
        share(d, c)

    def hop(h, c):
        @when(tp >= h)
        def _():
            from_left(h, c).wait_recv()

            @when(tp < n_tp - 1)
            def _():
                right_copy(h, c).start()

            share(h, c)

        @when(tp + h < n_tp)
        def _():
            from_right(h, c).wait_recv()

            @when(tp > 0)
            def _():
                left_copy(h + n_tp - 1, c).start()

            share(h + n_tp - 1, c)

    def crossed(h, c):
        def take(tag):
            y_copy(tag, c).wait_recv()
            f_copy(tag, c).start()

        if h == 0 or c >= relayed:
            take(h)
            return

        @when(tp >= h)
        def _():
            take(h)

        @when(tp + h < n_tp)
        def _():
            take(h + n_tp - 1)

    def named(name, fn, *args):
        def run():
            with jax.named_scope(name):
                fn(*args)
        return run

    events = []
    for c in range(parts):
        events.append((6.3 + 5.6 / parts * c, 0, named(f"p{c}", project, c)))
        events.append((8.1 + 8.4 / parts * (c + 1), 0, named(f"a{c}", add, c)))
        t = 11.7 + 8.4 / parts * (c + 1)
        events.append((t, 1, named(f"f{c}", finish, c)))
        events.append((t + 2.8, 3, named(f"y{c}_0", crossed, 0, c)))
        for h in range(1, n_tp):
            if c < relayed:
                there = t + 2.8 * h
                events.append((there, 2, named(f"h{c}_{h}", hop, h, c)))
            else:
                there = t + 2.8 + 0.8 * h
                events.append((there, 2, named(f"d{c}_{h}", direct, h, c)))
            events.append((there + 2.8, 3, named(f"y{c}_{h}", crossed, h, c)))
    for _, _, event in sorted(events, key=lambda e: e[:2]):
        event()

    def close(tag, c):
        y_copy(tag, c).wait_send()
        c_copy(tag, c).wait()
        f_copy(tag, c).wait()

    for c in range(parts):
        @when(jnp.logical_not(middle))
        def _():
            m_copy(c).wait_send()

        @when(middle)
        def _():
            for k in range(half):
                s_copy(k, c).wait_send()

        n_copy(c).wait_send()
        close(0, c)
        if c >= relayed:
            for d in range(1, n_tp):
                g_copy(d, c).wait_send()
                close(d, c)
            continue

        @when(tp < n_tp - 1)
        def _():
            right_copy(0, c).wait_send()

        @when(tp > 0)
        def _():
            left_copy(0, c).wait_send()

        for h in range(1, n_tp):
            @when(tp >= h)
            def _():
                @when(tp < n_tp - 1)
                def _():
                    right_copy(h, c).wait_send()

                close(h, c)

            @when(tp + h < n_tp)
            def _():
                @when(tp > 0)
                def _():
                    left_copy(h + n_tp - 1, c).wait_send()

                close(h + n_tp - 1, c)

    chunk = 32
    for i in range(y_buf.shape[0] // chunk):
      with jax.named_scope(f'emit{i}'):
        out_ref[i * chunk:(i + 1) * chunk, :] = y_buf[i * chunk:(i + 1) * chunk, :].astype(BF16)


def meet(acc, x, wo, bo, n_sq, n_tp, parts=4, relayed=2):
    batch, width = x.shape
    own = batch // n_sq
    cols = width // n_tp
    step = own // parts
    heads = wo.shape[0] // acc.shape[1]
    dim = acc.shape[1]
    vmem = pl.BlockSpec(memory_space=pltpu.VMEM)
    dma = pltpu.SemaphoreType.DMA
    tags = 2 * n_tp - 1
    return pl.pallas_call(
        functools.partial(meet_kernel, parts, relayed),
        out_shape=jax.ShapeDtypeStruct((batch, width), BF16),
        in_specs=[vmem] * 4,
        out_specs=vmem,
        scratch_shapes=[
            pltpu.VMEM((own, cols), F32),
            pltpu.VMEM((n_sq - 1, own * heads, dim), F32),
            pltpu.VMEM((n_sq - 1, 4 * heads, dim), F32),
            pltpu.VMEM((step * heads, dim), F32),
            pltpu.VMEM((parts, n_tp, step, cols), F32),
            pltpu.VMEM((parts, n_tp // 2, step, cols), F32),
            pltpu.VMEM((parts, step, cols), F32),
            pltpu.VMEM((parts, step, cols), F32),
            pltpu.VMEM((batch, width), F32),
            dma((n_sq - 1,)), dma((n_sq - 1,)),
            dma((n_sq - 1, parts)), dma((n_sq - 1, parts)),
            dma((parts,)), dma((parts,)),
            dma((parts,)), dma((parts,)),
            dma((n_tp // 2, parts)), dma((parts,)),
            dma((n_tp - 1, parts)), dma((n_tp - 1, parts)),
            dma((n_tp + 1, parts)), dma((n_tp + 1, parts)),
            dma((n_tp + 1, parts)), dma((n_tp + 1, parts)),
            dma((tags, parts)), dma((tags, parts)),
            dma((tags, parts)), dma((tags, parts)),
            dma((tags, parts)), dma((tags, parts)),
        ],
        compiler_params=pltpu.CompilerParams(collective_id=0, has_side_effects=True, vmem_limit_bytes=32 * 1024 * 1024),
        cost_estimate=pl.CostEstimate(flops=2**28, bytes_accessed=8 * 2**20, transcendentals=0),
        name="meet",
    )(acc, x, wo, bo.reshape(1, width))


def solution(mesh):
    def local_step(hidden, cache_lens, k_cache, v_cache, ln_gain, ln_bias, w_query, b_query, w_kv, b_kv, w_out, b_out):
        key_new, val_new, acc = attend(
            cache_lens, hidden, ln_gain, ln_bias, w_query, b_query, w_kv, b_kv, k_cache, v_cache)
        out_hidden = meet(acc, hidden, w_out, b_out, mesh.shape["sq"], mesh.shape["tp"])
        return out_hidden, key_new, val_new

    cache_spec = P("dp", "sq", None)
    row_spec = P("dp", None)
    in_specs = (row_spec, P("dp"), cache_spec, cache_spec, P(None), P(None), P(None, "tp"), P("tp"), P(None, None), P(None), P("tp", None), P(None))
    out_specs = (row_spec, cache_spec, cache_spec)
    return jax.shard_map(local_step, mesh=mesh, in_specs=in_specs, out_specs=out_specs, check_vma=False)
```

```python
import functools

import jax
import jax.numpy as jnp
from jax import lax
from jax.experimental import pallas as pl
from jax.experimental.pallas import tpu as pltpu
from jax.sharding import PartitionSpec as P

F32 = jnp.float32
BF16 = jnp.bfloat16
NEG = -1e30


def attend_kernel(
    pairs, held, lens_ref, x_hbm, gain_ref, bias_ref, wq_hbm, bq_ref, wkv_hbm, bkv_ref, k_hbm, v_hbm,
    k_out, v_out, acc_out,
    x_buf, h_buf, wq_buf, wkv_buf, q_buf, kv_buf, s_buf, acc_ref, ml_ref, k_buf, v_buf,
    in_sem, k_sem, v_sem, ko_sem, vo_sem, acc_sem, ml_sem,
):
    batch, pos_local, dim = k_buf.shape
    heads = wq_buf.shape[1] // dim
    per = 2 * pairs
    chunks = batch // per
    rows = 2 * heads
    first_pos = lax.axis_index("sq") * pos_local
    scale = dim ** -0.5

    x_copy = pltpu.make_async_copy(x_hbm, x_buf, in_sem.at[0])
    kv_copy = pltpu.make_async_copy(wkv_hbm, wkv_buf, in_sem.at[1])
    q_copy = pltpu.make_async_copy(wq_hbm, wq_buf, in_sem.at[2])
    x_copy.start()
    kv_copy.start()
    q_copy.start()

    def span(ref, c):
        return ref.at[pl.ds(c * per, per)]

    def k_load(c):
        return pltpu.make_async_copy(span(k_hbm, c), span(k_buf, c), k_sem.at[c])

    def v_load(c):
        return pltpu.make_async_copy(span(v_hbm, c), span(v_buf, c), v_sem.at[c])

    def k_store(c):
        return pltpu.make_async_copy(span(k_buf, c), span(k_out, c), ko_sem.at[c])

    def v_store(c):
        return pltpu.make_async_copy(span(v_buf, c), span(v_out, c), vo_sem.at[c])

    @pl.loop(0, chunks)
    def _(c):
        k_load(c).start()
        v_load(c).start()

    x_copy.wait()
    block = 32

    @pl.loop(0, batch // block)
    def _(i):
        x = x_buf[pl.ds(i * block, block), :].astype(F32)
        mean = jnp.mean(x, axis=-1, keepdims=True)
        cen = x - mean
        var = jnp.mean(cen * cen, axis=-1, keepdims=True)
        h = cen * lax.rsqrt(var + 1e-5) * gain_ref[...] + bias_ref[...]
        h_buf[pl.ds(i * block, block), :] = h.astype(BF16)

    kv_copy.wait()
    kv = jnp.dot(h_buf[...], wkv_buf[...], preferred_element_type=F32) + bkv_ref[...]
    kv_buf[...] = kv.astype(BF16).astype(F32)
    q_copy.wait()
    for n0 in range(0, heads, 2):
        cols = slice(n0 * dim, (n0 + 2) * dim)
        q = jnp.dot(h_buf[...], wq_buf[:, cols], preferred_element_type=F32) + bq_ref[:, cols]
        q = q.astype(BF16).astype(F32)
        q_buf[pl.ds(n0, batch, stride=heads), :] = q[:, :dim]
        q_buf[pl.ds(n0 + 1, batch, stride=heads), :] = q[:, dim:]

    top = lax.broadcasted_iota(jnp.int32, (rows, dim), 0) < heads
    top2 = lax.broadcasted_iota(jnp.int32, (rows, pos_local), 0) < heads
    lane = lax.broadcasted_iota(jnp.int32, (rows, dim), 1)
    place = first_pos + lax.broadcasted_iota(jnp.int32, (rows, pos_local), 1)
    sub = lax.broadcasted_iota(jnp.int32, (16, dim), 0)

    def update_rows(c):
        fresh = kv_buf[pl.ds(pl.multiple_of(c * per, per), per), :]
        for j in range(per):
            b = c * per + j
            at = lens_ref[b] - first_pos
            base = pl.multiple_of(jnp.clip(at, 0, pos_local - 1) // 16 * 16, 16)
            hit = sub == at - base
            for buf, lo in ((k_buf, 0), (v_buf, dim)):
                new = jnp.broadcast_to(fresh[j:j + 1, lo:lo + dim], (16, dim))
                old = buf[b, pl.ds(base, 16), :].astype(F32)
                buf[b, pl.ds(base, 16), :] = jnp.where(hit, new, old).astype(BF16)

    def score(c):
        out = []
        for j in range(pairs):
            p = c * pairs + j
            q = q_buf[pl.ds(pl.multiple_of(p * rows, rows), rows), :]
            lhs = jnp.concatenate([jnp.where(top, q, 0.0), jnp.where(top, 0.0, q)], axis=1).astype(BF16)
            keys = jnp.concatenate([k_buf[2 * p], k_buf[2 * p + 1]], axis=1)
            s = lax.dot_general(lhs, keys, (((1,), (1,)), ((), ())), preferred_element_type=F32)
            out.append(s)
        return out

    def weigh(c, m_all, l_all):
        for j in range(pairs):
            p = c * pairs + j
            s = s_buf[j * rows:(j + 1) * rows, :] * scale
            last = jnp.where(top2, lens_ref[2 * p], lens_ref[2 * p + 1])
            valid = place <= last
            s = jnp.where(valid, s, NEG)
            m = jnp.max(s, axis=-1, keepdims=True)
            w = jnp.where(valid, jnp.exp(s - m), 0.0)
            total = jnp.sum(w, axis=-1, keepdims=True)
            vals = jnp.concatenate([v_buf[2 * p], v_buf[2 * p + 1]], axis=1)
            o = jnp.dot(w.astype(BF16), vals, preferred_element_type=F32)
            acc_ref[pl.ds(pl.multiple_of(p * rows, rows), rows), :] = jnp.where(top, o[:, :dim], o[:, dim:])
            m_all = jnp.where(lane == p, m, m_all)
            l_all = jnp.where(lane == p, total, l_all)
        return m_all, l_all

    def put_scores(out):
        for j, s in enumerate(out):
            s_buf[j * rows:(j + 1) * rows, :] = s

    def acc_store(c):
        part = pl.ds(pl.multiple_of(c * (pairs * rows), pairs * rows), pairs * rows)
        return pltpu.make_async_copy(acc_ref.at[part], acc_out.at[part], acc_sem.at[c])

    def loaded(c):
        k_load(c).wait()
        v_load(c).wait()

    def leave(c):
        k_store(c).start()
        v_store(c).start()

    loaded(0)
    update_rows(0)
    put_scores(score(0))
    zero = jnp.zeros((rows, dim), F32)

    def early(c, carry):
        loaded(c + 1)
        update_rows(c + 1)
        carry = weigh(c, *carry)
        put_scores(score(c + 1))
        acc_store(c).start()
        return carry

    carry = lax.fori_loop(0, held, early, (zero, zero))

    @pl.loop(held + 1, chunks)
    def _(c):
        loaded(c)

    @pl.loop(0, held + 1)
    def _(c):
        leave(c)

    def late(c, carry):
        update_rows(c + 1)
        carry = weigh(c, *carry)
        put_scores(score(c + 1))
        acc_store(c).start()
        leave(c + 1)
        return carry

    carry = lax.fori_loop(held, chunks - 1, late, carry)
    m_all, l_all = weigh(chunks - 1, *carry)
    ml_ref[:rows, :] = m_all
    ml_ref[rows:, :] = l_all
    acc_store(chunks - 1).start()

    @pl.loop(0, chunks - 1)
    def _(c):
        k_store(c).wait()
        v_store(c).wait()
        acc_store(c).wait()

    ml_store = pltpu.make_async_copy(ml_ref, acc_out.at[pl.ds(batch * heads, 2 * rows)], ml_sem)
    ml_store.start()
    k_store(chunks - 1).wait()
    v_store(chunks - 1).wait()
    acc_store(chunks - 1).wait()
    ml_store.wait()


def attend(lens, x, gain, bias, wq, bq, wkv, bkv, k, v, pairs=8, held=8):
    batch, pos_local, dim = k.shape
    width = x.shape[1]
    heads = wq.shape[1] // dim
    chunks = batch // (2 * pairs)
    hbm = pl.BlockSpec(memory_space=pltpu.HBM)
    vmem = pl.BlockSpec(memory_space=pltpu.VMEM)
    dma = pltpu.SemaphoreType.DMA
    return pl.pallas_call(
        functools.partial(attend_kernel, pairs, held),
        out_shape=(
            jax.ShapeDtypeStruct(k.shape, k.dtype),
            jax.ShapeDtypeStruct(v.shape, v.dtype),
            jax.ShapeDtypeStruct((batch * heads + 4 * heads, dim), F32),
        ),
        in_specs=[pl.BlockSpec(memory_space=pltpu.SMEM), hbm, vmem, vmem, hbm, vmem, hbm, vmem, hbm, hbm],
        out_specs=(hbm, hbm, hbm),
        scratch_shapes=[
            pltpu.VMEM(x.shape, BF16),
            pltpu.VMEM(x.shape, BF16),
            pltpu.VMEM(wq.shape, BF16),
            pltpu.VMEM(wkv.shape, BF16),
            pltpu.VMEM((batch * heads, dim), F32),
            pltpu.VMEM((batch, 2 * dim), F32),
            pltpu.VMEM((pairs * 2 * heads, pos_local), F32),
            pltpu.VMEM((batch * heads, dim), F32),
            pltpu.VMEM((4 * heads, dim), F32),
            pltpu.VMEM(k.shape, BF16),
            pltpu.VMEM(v.shape, BF16),
            dma((3,)), dma((chunks,)), dma((chunks,)), dma((chunks,)), dma((chunks,)), dma((chunks,)), dma,
        ],
        compiler_params=pltpu.CompilerParams(vmem_limit_bytes=60 * 1024 * 1024),
        cost_estimate=pl.CostEstimate(flops=2 * 2**30, bytes_accessed=72 * 2**20, transcendentals=0),
        name="attend",
    )(lens, x, gain.reshape(1, width), bias.reshape(1, width), wq, bq.reshape(1, -1), wkv, bkv.reshape(1, -1), k, v)


def meet_kernel(
    parts, relayed, acc_buf, x_ref, wo_ref, bo_ref, out_ref,
    base_buf, sq_buf, ml_buf, a_buf, z_out, far_in, in_buf, y_buf,
    ml_send, ml_recv, sq_send, sq_recv, z_send, m_recv, s_recv, g_send, g_recv, y_send, y_recv, c_send, c_recv, f_send, f_recv,
):
    n_sq, n_tp = sq_buf.shape[1] + 1, z_out.shape[1]
    width = y_buf.shape[1]
    dim = acc_buf.shape[1]
    sq, tp = lax.axis_index("sq"), lax.axis_index("tp")
    own = y_buf.shape[0] // n_sq
    step = own // parts
    cols = width // n_tp
    heads = wo_ref.shape[0] // dim
    rows = 2 * heads
    pairs = step // 2
    fold = step * heads
    mesh_id = pl.DeviceIdType.MESH

    def at_sq(d):
        return {"sq": lax.rem(sq + d, n_sq)}

    def at_tp(d):
        return {"tp": lax.rem(tp + d, n_tp)}

    core_sq = sq + 1 - 2 * lax.rem(sq, 2)
    across_sq = lax.rem(sq + 2, n_sq)
    core, across = {"sq": core_sq}, {"sq": across_sq}

    barrier = pltpu.get_barrier_semaphore()
    for d in range(1, n_sq):
        pl.semaphore_signal(barrier, inc=1, device_id=at_sq(d), device_id_type=mesh_id)
    for d in range(1, n_tp):
        pl.semaphore_signal(barrier, inc=1, device_id=at_tp(d), device_id_type=mesh_id)
    x_cols = pl.ds(pl.multiple_of(tp * cols, cols), cols)
    base_buf[...] = x_ref[pl.ds(pl.multiple_of(sq * own, own), own), x_cols].astype(F32) + bo_ref[:, x_cols]
    ml_own = acc_buf.at[pl.ds(own * n_sq * heads, 2 * rows)]
    with jax.named_scope('barrier'):
        pl.semaphore_wait(barrier, n_sq - 1 + n_tp - 1)

    def remote(src, dst, send, recv, to):
        return pltpu.make_async_remote_copy(src_ref=src, dst_ref=dst, send_sem=send, recv_sem=recv, device_id=to, device_id_type=mesh_id)

    def ml_copy(d):
        return remote(ml_own, ml_buf.at[d - 1], ml_send, ml_recv, at_sq(d))

    def sq_copy(d, c):
        start = pl.multiple_of(lax.rem(sq + d, n_sq) * (own * heads) + c * fold, fold)
        return remote(acc_buf.at[pl.ds(start, fold)], sq_buf.at[c, d - 1], sq_send, sq_recv.at[c], at_sq(d))

    half = n_tp // 2
    middle = lax.div(tp + 1, 2) == 1
    partner = tp + 1 - 2 * lax.rem(tp, 2)
    far = half - half * lax.div(tp, half)

    def m_copy(c):
        return remote(z_out.at[c, pl.ds(far, half)], far_in.at[c], z_send, m_recv.at[c], {"tp": partner})

    def n_copy(c):
        return remote(z_out.at[c, partner], in_buf.at[c, 0], z_send, s_recv.at[c], {"tp": partner})

    def s_copy(k, c):
        return remote(z_out.at[c, far + k], in_buf.at[c, 1], z_send, s_recv.at[c], {"tp": far + k})

    def block(s, t, c):
        return y_buf.at[pl.ds(pl.multiple_of(s * own + c * step, step), step), pl.ds(pl.multiple_of(t * cols, cols), cols)]

    def source(tag):
        return tp - tag if tag < n_tp else tp + (tag - n_tp + 1)

    def source_of(tag, c):
        return source(tag) if c < relayed else lax.rem(tp - tag + n_tp, n_tp)

    def tp_copy(t, c, to):
        b = block(sq, t, c)
        return remote(b, b, g_send, g_recv.at[t, c], {"tp": to})

    def y_copy(tag, c):
        t = source_of(tag, c)
        b = block(sq, t, c)
        return remote(b, b, y_send, y_recv.at[t, c], across)

    def c_copy(tag, c):
        b = block(sq, source_of(tag, c), c)
        return remote(b, b, c_send, c_recv, core)

    def f_copy(tag, c):
        b = block(across_sq, source_of(tag, c), c)
        return remote(b, b, f_send, f_recv, core)

    def all_of(ref, send, recv):
        return remote(ref, ref, send, recv, {"tp": tp})

    for d in range(1, n_sq):
        ml_copy(d).start()
    for c in range(parts):
        for d in range(1, n_sq):
            sq_copy(d, c).start()

    with jax.named_scope('mlwait'):
        all_of(ml_buf, ml_send, ml_recv).wait()
    maxima = [acc_buf[own * n_sq * heads:own * n_sq * heads + rows, :]] + [ml_buf[d, :rows, :] for d in range(n_sq - 1)]
    sums = [acc_buf[own * n_sq * heads + rows:, :]] + [ml_buf[d, rows:, :] for d in range(n_sq - 1)]
    top = functools.reduce(jnp.maximum, maxima)
    scales = [jnp.exp(m - top) for m in maxima]
    den = sum(e * s for e, s in zip(scales, sums))
    scales = [e / den for e in scales]
    lane = lax.broadcasted_iota(jnp.int32, (rows, dim), 1)

    def when(cond):
        return pl.when(cond)

    def project(c):
        all_of(sq_buf.at[c], sq_send, sq_recv.at[c]).wait_recv()
        for j in range(pairs):
            p = sq * (own // 2) + c * pairs + j
            pick = lane == p
            mine = pl.multiple_of(sq * (own * heads) + c * fold + j * rows, rows)
            terms = [acc_buf[pl.ds(mine, rows), :]]
            terms += [sq_buf[c, d, j * rows:(j + 1) * rows, :] for d in range(n_sq - 1)]
            total = sum(jnp.sum(jnp.where(pick, e, 0.0), axis=1, keepdims=True) * t for e, t in zip(scales, terms))
            a_buf[j * rows:(j + 1) * rows, :] = total
        lhs = jnp.concatenate([a_buf[pl.ds(n, step, stride=heads), :].astype(BF16) for n in range(heads)], axis=1)
        for t in range(n_tp):
            z_out[c, t] = jnp.dot(lhs, wo_ref[:, t * cols:(t + 1) * cols], preferred_element_type=F32)

        @when(jnp.logical_not(middle))
        def _():
            m_copy(c).start()

        n_copy(c).start()

    def add(c):
        @when(middle)
        def _():
            m_copy(c).wait_recv()
            for k in range(half):
                z_out[c, far + k] = z_out[c, far + k] + far_in[c, k]
            for k in range(half):
                s_copy(k, c).start()

    def share(tag, c):
        y_copy(tag, c).start()
        c_copy(tag, c).start()

    def finish(c):
        all_of(in_buf.at[c], z_send, s_recv.at[c]).wait_recv()
        total = z_out[c, tp] + in_buf[c, 0] + in_buf[c, 1]
        total = total + base_buf[c * step:(c + 1) * step, :]
        mine = block(sq, tp, c)
        mine[...] = total

        if c < relayed:
            @when(tp < n_tp - 1)
            def _():
                tp_copy(tp, c, tp + 1).start()

            @when(tp > 0)
            def _():
                tp_copy(tp, c, tp - 1).start()
        else:
            for d in range(1, n_tp):
                tp_copy(tp, c, lax.rem(tp + d, n_tp)).start()

        share(0, c)

    def direct(d, c):
        tp_copy(source_of(d, c), c, tp).wait_recv()
        share(d, c)

    def hop(h, c):
        @when(tp >= h)
        def _():
            tp_copy(tp - h, c, tp).wait_recv()

            @when(tp < n_tp - 1)
            def _():
                tp_copy(tp - h, c, tp + 1).start()

            share(h, c)

        @when(tp + h < n_tp)
        def _():
            tp_copy(tp + h, c, tp).wait_recv()

            @when(tp > 0)
            def _():
                tp_copy(tp + h, c, tp - 1).start()

            share(h + n_tp - 1, c)

    def crossed(h, c):
        def take(tag):
            y_copy(tag, c).wait_recv()
            f_copy(tag, c).start()

        if h == 0 or c >= relayed:
            take(h)
            return

        @when(tp >= h)
        def _():
            take(h)

        @when(tp + h < n_tp)
        def _():
            take(h + n_tp - 1)

    def named(name, fn, *args):
        def run():
            with jax.named_scope(name):
                fn(*args)
        return run

    events = []
    for c in range(parts):
        events.append((8.0 + 5.6 / parts * c, 0, named(f"p{c}", project, c)))
        events.append((9.5 + 8.4 / parts * (c + 1), 0, named(f"a{c}", add, c)))
        t = 10.8 + 8.4 / parts * (c + 1)
        events.append((t, 1, named(f"f{c}", finish, c)))
        events.append((t + 2.8, 3, named(f"y{c}_0", crossed, 0, c)))
        for h in range(1, n_tp):
            if c < relayed:
                there = t + 3.6 * h
                events.append((there, 2, named(f"h{c}_{h}", hop, h, c)))
            else:
                there = t + 3.2 + 0.8 * h
                events.append((there, 2, named(f"d{c}_{h}", direct, h, c)))
            events.append((there + 2.8, 3, named(f"y{c}_{h}", crossed, h, c)))
    for _, _, event in sorted(events, key=lambda e: e[:2]):
        event()

    whole = y_buf.at[pl.ds(0, own)]
    with jax.named_scope("close"):
        all_of(whole, c_send, c_recv).wait()
        all_of(whole, f_send, f_recv).wait()
        all_of(whole, y_send, f_recv).wait_send()
        all_of(sq_buf, sq_send, ml_recv).wait_send()
        all_of(z_out.at[:, pl.ds(0, half + 1)], z_send, ml_recv).wait_send()
        straight = (parts - relayed) * (n_tp - 1)

        @when(middle)
        def _():
            blocks = y_buf.at[pl.ds(0, (straight + relayed * (n_tp + 1)) * step), pl.ds(0, cols)]
            all_of(blocks, g_send, ml_recv).wait_send()

        @when(jnp.logical_not(middle))
        def _():
            blocks = y_buf.at[pl.ds(0, (straight + relayed) * step), pl.ds(0, cols)]
            all_of(blocks, g_send, ml_recv).wait_send()

    chunk = 32
    for i in range(y_buf.shape[0] // chunk):
      with jax.named_scope(f'emit{i}'):
        out_ref[i * chunk:(i + 1) * chunk, :] = y_buf[i * chunk:(i + 1) * chunk, :].astype(BF16)


def meet(acc, x, wo, bo, n_sq, n_tp, parts=4, relayed=1):
    batch, width = x.shape
    own = batch // n_sq
    cols = width // n_tp
    step = own // parts
    heads = wo.shape[0] // acc.shape[1]
    dim = acc.shape[1]
    vmem = pl.BlockSpec(memory_space=pltpu.VMEM)
    dma = pltpu.SemaphoreType.DMA
    return pl.pallas_call(
        functools.partial(meet_kernel, parts, relayed),
        out_shape=jax.ShapeDtypeStruct((batch, width), BF16),
        in_specs=[vmem] * 4,
        out_specs=vmem,
        scratch_shapes=[
            pltpu.VMEM((own, cols), F32),
            pltpu.VMEM((parts, n_sq - 1, step * heads, dim), F32),
            pltpu.VMEM((n_sq - 1, 4 * heads, dim), F32),
            pltpu.VMEM((step * heads, dim), F32),
            pltpu.VMEM((parts, n_tp, step, cols), F32),
            pltpu.VMEM((parts, n_tp // 2, step, cols), F32),
            pltpu.VMEM((parts, 2, step, cols), F32),
            pltpu.VMEM((batch, width), F32),
            dma, dma, dma, dma((parts,)),
            dma, dma((parts,)), dma((parts,)), dma, dma((n_tp, parts)),
            dma, dma((n_tp, parts)), dma, dma, dma, dma,
        ],
        compiler_params=pltpu.CompilerParams(collective_id=0, has_side_effects=True, vmem_limit_bytes=32 * 1024 * 1024),
        cost_estimate=pl.CostEstimate(flops=2**28, bytes_accessed=8 * 2**20, transcendentals=0),
        name="meet",
    )(acc, x, wo, bo.reshape(1, width))


def solution(mesh):
    def local_step(hidden, cache_lens, k_cache, v_cache, ln_gain, ln_bias, w_query, b_query, w_kv, b_kv, w_out, b_out):
        key_new, val_new, acc = attend(
            cache_lens, hidden, ln_gain, ln_bias, w_query, b_query, w_kv, b_kv, k_cache, v_cache)
        out_hidden = meet(acc, hidden, w_out, b_out, mesh.shape["sq"], mesh.shape["tp"])
        return out_hidden, key_new, val_new

    cache_spec = P("dp", "sq", None)
    row_spec = P("dp", None)
    in_specs = (row_spec, P("dp"), cache_spec, cache_spec, P(None), P(None), P(None, "tp"), P("tp"), P(None, None), P(None), P("tp", None), P(None))
    out_specs = (row_spec, cache_spec, cache_spec)
    return jax.shard_map(local_step, mesh=mesh, in_specs=in_specs, out_specs=out_specs, check_vma=False)
```

```python
import functools

import jax
import jax.numpy as jnp
from jax import lax
from jax.experimental import pallas as pl
from jax.experimental.pallas import tpu as pltpu
from jax.sharding import PartitionSpec as P

F32 = jnp.float32
BF16 = jnp.bfloat16
NEG = -1e30


def attend_kernel(
    pairs, held, lens_ref, x_hbm, gain_ref, bias_ref, wq_hbm, bq_ref, wkv_hbm, bkv_ref, k_hbm, v_hbm,
    k_out, v_out, acc_out,
    x_buf, h_buf, wq_buf, wkv_buf, q_buf, kv_buf, s_buf, acc_ref, ml_ref, k_buf, v_buf,
    in_sem, k_sem, v_sem, ko_sem, vo_sem, acc_sem, ml_sem,
):
    batch, pos_local, dim = k_buf.shape
    heads = wq_buf.shape[1] // dim
    per = 2 * pairs
    chunks = batch // per
    rows = 2 * heads
    first_pos = lax.axis_index("sq") * pos_local
    scale = dim ** -0.5

    x_copy = pltpu.make_async_copy(x_hbm, x_buf, in_sem.at[0])
    kv_copy = pltpu.make_async_copy(wkv_hbm, wkv_buf, in_sem.at[1])
    q_copy = pltpu.make_async_copy(wq_hbm, wq_buf, in_sem.at[2])
    x_copy.start()
    kv_copy.start()
    q_copy.start()

    def span(ref, c):
        return ref.at[pl.ds(c * per, per)]

    def k_load(c):
        return pltpu.make_async_copy(span(k_hbm, c), span(k_buf, c), k_sem.at[c])

    def v_load(c):
        return pltpu.make_async_copy(span(v_hbm, c), span(v_buf, c), v_sem.at[c])

    def k_store(c):
        return pltpu.make_async_copy(span(k_buf, c), span(k_out, c), ko_sem.at[c])

    def v_store(c):
        return pltpu.make_async_copy(span(v_buf, c), span(v_out, c), vo_sem.at[c])

    @pl.loop(0, chunks)
    def _(c):
        k_load(c).start()
        v_load(c).start()

    x_copy.wait()
    block = 32

    @pl.loop(0, batch // block)
    def _(i):
        x = x_buf[pl.ds(i * block, block), :].astype(F32)
        mean = jnp.mean(x, axis=-1, keepdims=True)
        cen = x - mean
        var = jnp.mean(cen * cen, axis=-1, keepdims=True)
        h = cen * lax.rsqrt(var + 1e-5) * gain_ref[...] + bias_ref[...]
        h_buf[pl.ds(i * block, block), :] = h.astype(BF16)

    kv_copy.wait()
    kv = jnp.dot(h_buf[...], wkv_buf[...], preferred_element_type=F32) + bkv_ref[...]
    kv_buf[...] = kv.astype(BF16).astype(F32)
    q_copy.wait()
    for n0 in range(0, heads, 2):
        cols = slice(n0 * dim, (n0 + 2) * dim)
        q = jnp.dot(h_buf[...], wq_buf[:, cols], preferred_element_type=F32) + bq_ref[:, cols]
        q = q.astype(BF16).astype(F32)
        q_buf[pl.ds(n0, batch, stride=heads), :] = q[:, :dim]
        q_buf[pl.ds(n0 + 1, batch, stride=heads), :] = q[:, dim:]

    top = lax.broadcasted_iota(jnp.int32, (rows, dim), 0) < heads
    top2 = lax.broadcasted_iota(jnp.int32, (rows, pos_local), 0) < heads
    lane = lax.broadcasted_iota(jnp.int32, (rows, dim), 1)
    place = first_pos + lax.broadcasted_iota(jnp.int32, (rows, pos_local), 1)
    sub = lax.broadcasted_iota(jnp.int32, (16, dim), 0)

    def update_rows(c):
        fresh = kv_buf[pl.ds(pl.multiple_of(c * per, per), per), :]
        for j in range(per):
            b = c * per + j
            at = lens_ref[b] - first_pos
            base = pl.multiple_of(jnp.clip(at, 0, pos_local - 1) // 16 * 16, 16)
            hit = sub == at - base
            for buf, lo in ((k_buf, 0), (v_buf, dim)):
                new = jnp.broadcast_to(fresh[j:j + 1, lo:lo + dim], (16, dim))
                old = buf[b, pl.ds(base, 16), :].astype(F32)
                buf[b, pl.ds(base, 16), :] = jnp.where(hit, new, old).astype(BF16)

    def score(c):
        out = []
        for j in range(pairs):
            p = c * pairs + j
            q = q_buf[pl.ds(pl.multiple_of(p * rows, rows), rows), :]
            lhs = jnp.concatenate([jnp.where(top, q, 0.0), jnp.where(top, 0.0, q)], axis=1).astype(BF16)
            keys = jnp.concatenate([k_buf[2 * p], k_buf[2 * p + 1]], axis=1)
            s = lax.dot_general(lhs, keys, (((1,), (1,)), ((), ())), preferred_element_type=F32)
            out.append(s)
        return out

    def weigh(c, m_all, l_all):
        for j in range(pairs):
            p = c * pairs + j
            s = s_buf[j * rows:(j + 1) * rows, :] * scale
            last = jnp.where(top2, lens_ref[2 * p], lens_ref[2 * p + 1])
            valid = place <= last
            s = jnp.where(valid, s, NEG)
            m = jnp.max(s, axis=-1, keepdims=True)
            w = jnp.where(valid, jnp.exp(s - m), 0.0)
            total = jnp.sum(w, axis=-1, keepdims=True)
            vals = jnp.concatenate([v_buf[2 * p], v_buf[2 * p + 1]], axis=1)
            o = jnp.dot(w.astype(BF16), vals, preferred_element_type=F32)
            acc_ref[pl.ds(pl.multiple_of(p * rows, rows), rows), :] = jnp.where(top, o[:, :dim], o[:, dim:])
            m_all = jnp.where(lane == p, m, m_all)
            l_all = jnp.where(lane == p, total, l_all)
        return m_all, l_all

    def put_scores(out):
        for j, s in enumerate(out):
            s_buf[j * rows:(j + 1) * rows, :] = s

    def acc_store(c):
        part = pl.ds(pl.multiple_of(c * (pairs * rows), pairs * rows), pairs * rows)
        return pltpu.make_async_copy(acc_ref.at[part], acc_out.at[part], acc_sem.at[c])

    def loaded(c):
        k_load(c).wait()
        v_load(c).wait()

    def leave(c):
        k_store(c).start()
        v_store(c).start()

    loaded(0)
    update_rows(0)
    put_scores(score(0))
    zero = jnp.zeros((rows, dim), F32)

    def early(c, carry):
        loaded(c + 1)
        update_rows(c + 1)
        carry = weigh(c, *carry)
        put_scores(score(c + 1))
        acc_store(c).start()
        return carry

    carry = lax.fori_loop(0, held, early, (zero, zero))

    @pl.loop(held + 1, chunks)
    def _(c):
        loaded(c)

    @pl.loop(0, held + 1)
    def _(c):
        leave(c)

    def late(c, carry):
        update_rows(c + 1)
        carry = weigh(c, *carry)
        put_scores(score(c + 1))
        acc_store(c).start()
        leave(c + 1)
        return carry

    carry = lax.fori_loop(held, chunks - 1, late, carry)
    m_all, l_all = weigh(chunks - 1, *carry)
    ml_ref[:rows, :] = m_all
    ml_ref[rows:, :] = l_all
    acc_store(chunks - 1).start()

    @pl.loop(0, chunks - 1)
    def _(c):
        k_store(c).wait()
        v_store(c).wait()
        acc_store(c).wait()

    ml_store = pltpu.make_async_copy(ml_ref, acc_out.at[pl.ds(batch * heads, 2 * rows)], ml_sem)
    ml_store.start()
    k_store(chunks - 1).wait()
    v_store(chunks - 1).wait()
    acc_store(chunks - 1).wait()
    ml_store.wait()


def attend(lens, x, gain, bias, wq, bq, wkv, bkv, k, v, pairs=8, held=8):
    batch, pos_local, dim = k.shape
    width = x.shape[1]
    heads = wq.shape[1] // dim
    chunks = batch // (2 * pairs)
    hbm = pl.BlockSpec(memory_space=pltpu.HBM)
    vmem = pl.BlockSpec(memory_space=pltpu.VMEM)
    dma = pltpu.SemaphoreType.DMA
    return pl.pallas_call(
        functools.partial(attend_kernel, pairs, held),
        out_shape=(
            jax.ShapeDtypeStruct(k.shape, k.dtype),
            jax.ShapeDtypeStruct(v.shape, v.dtype),
            jax.ShapeDtypeStruct((batch * heads + 4 * heads, dim), F32),
        ),
        in_specs=[pl.BlockSpec(memory_space=pltpu.SMEM), hbm, vmem, vmem, hbm, vmem, hbm, vmem, hbm, hbm],
        out_specs=(hbm, hbm, hbm),
        scratch_shapes=[
            pltpu.VMEM(x.shape, BF16),
            pltpu.VMEM(x.shape, BF16),
            pltpu.VMEM(wq.shape, BF16),
            pltpu.VMEM(wkv.shape, BF16),
            pltpu.VMEM((batch * heads, dim), F32),
            pltpu.VMEM((batch, 2 * dim), F32),
            pltpu.VMEM((pairs * 2 * heads, pos_local), F32),
            pltpu.VMEM((batch * heads, dim), F32),
            pltpu.VMEM((4 * heads, dim), F32),
            pltpu.VMEM(k.shape, BF16),
            pltpu.VMEM(v.shape, BF16),
            dma((3,)), dma((chunks,)), dma((chunks,)), dma((chunks,)), dma((chunks,)), dma((chunks,)), dma,
        ],
        compiler_params=pltpu.CompilerParams(vmem_limit_bytes=60 * 1024 * 1024),
        cost_estimate=pl.CostEstimate(flops=2 * 2**30, bytes_accessed=72 * 2**20, transcendentals=0),
        name="attend",
    )(lens, x, gain.reshape(1, width), bias.reshape(1, width), wq, bq.reshape(1, -1), wkv, bkv.reshape(1, -1), k, v)


def meet_kernel(
    parts, relayed, acc_buf, x_ref, wo_ref, bo_ref, out_ref,
    base_buf, sq_buf, ml_buf, a_buf, z_out, far_in, in_buf, y_buf,
    ml_send, ml_recv, sq_send, sq_recv, z_send, m_recv, s_recv, g_send, g_recv, y_send, y_recv, c_send, c_recv, f_send, f_recv,
):
    n_sq, n_tp = sq_buf.shape[1] + 1, z_out.shape[1]
    width = y_buf.shape[1]
    dim = acc_buf.shape[1]
    sq, tp = lax.axis_index("sq"), lax.axis_index("tp")
    own = y_buf.shape[0] // n_sq
    step = own // parts
    cols = width // n_tp
    heads = wo_ref.shape[0] // dim
    rows = 2 * heads
    pairs = step // 2
    fold = step * heads
    mesh_id = pl.DeviceIdType.MESH

    def at_sq(d):
        return {"sq": lax.rem(sq + d, n_sq)}

    def at_tp(d):
        return {"tp": lax.rem(tp + d, n_tp)}

    core_sq = sq + 1 - 2 * lax.rem(sq, 2)
    across_sq = lax.rem(sq + 2, n_sq)
    core, across = {"sq": core_sq}, {"sq": across_sq}

    barrier = pltpu.get_barrier_semaphore()
    for d in range(1, n_sq):
        pl.semaphore_signal(barrier, inc=1, device_id=at_sq(d), device_id_type=mesh_id)
    for d in range(1, n_tp):
        pl.semaphore_signal(barrier, inc=1, device_id=at_tp(d), device_id_type=mesh_id)
    x_cols = pl.ds(pl.multiple_of(tp * cols, cols), cols)
    base_buf[...] = x_ref[pl.ds(pl.multiple_of(sq * own, own), own), x_cols].astype(F32) + bo_ref[:, x_cols]
    ml_own = acc_buf.at[pl.ds(own * n_sq * heads, 2 * rows)]
    with jax.named_scope('barrier'):
        pl.semaphore_wait(barrier, n_sq - 1 + n_tp - 1)

    def remote(src, dst, send, recv, to):
        return pltpu.make_async_remote_copy(src_ref=src, dst_ref=dst, send_sem=send, recv_sem=recv, device_id=to, device_id_type=mesh_id)

    def ml_copy(d):
        return remote(ml_own, ml_buf.at[d - 1], ml_send, ml_recv, at_sq(d))

    def sq_copy(d, c):
        start = pl.multiple_of(lax.rem(sq + d, n_sq) * (own * heads) + c * fold, fold)
        return remote(acc_buf.at[pl.ds(start, fold)], sq_buf.at[c, d - 1], sq_send, sq_recv.at[c], at_sq(d))

    half = n_tp // 2
    middle = lax.div(tp + 1, 2) == 1
    partner = tp + 1 - 2 * lax.rem(tp, 2)
    far = half - half * lax.div(tp, half)

    def m_copy(c):
        return remote(z_out.at[c, pl.ds(far, half)], far_in.at[c], z_send, m_recv.at[c], {"tp": partner})

    def n_copy(c):
        return remote(z_out.at[c, partner], in_buf.at[c, 0], z_send, s_recv.at[c], {"tp": partner})

    def s_copy(k, c):
        return remote(z_out.at[c, far + k], in_buf.at[c, 1], z_send, s_recv.at[c], {"tp": far + k})

    def block(s, t, c):
        return y_buf.at[pl.ds(pl.multiple_of(s * own + c * step, step), step), pl.ds(pl.multiple_of(t * cols, cols), cols)]

    def source(tag):
        return tp - tag if tag < n_tp else tp + (tag - n_tp + 1)

    def source_of(tag, c):
        return source(tag) if c < relayed else lax.rem(tp - tag + n_tp, n_tp)

    def tp_copy(t, c, to):
        b = block(sq, t, c)
        return remote(b, b, g_send, g_recv.at[t, c], {"tp": to})

    def y_copy(tag, c):
        t = source_of(tag, c)
        b = block(sq, t, c)
        return remote(b, b, y_send, y_recv.at[t, c], across)

    def c_copy(tag, c):
        b = block(sq, source_of(tag, c), c)
        return remote(b, b, c_send, c_recv, core)

    def f_copy(tag, c):
        b = block(across_sq, source_of(tag, c), c)
        return remote(b, b, f_send, f_recv, core)

    def all_of(ref, send, recv):
        return remote(ref, ref, send, recv, {"tp": tp})

    for d in range(1, n_sq):
        ml_copy(d).start()
    for c in range(parts):
        for d in range(1, n_sq):
            sq_copy(d, c).start()

    with jax.named_scope('mlwait'):
        all_of(ml_buf, ml_send, ml_recv).wait()
    maxima = [acc_buf[own * n_sq * heads:own * n_sq * heads + rows, :]] + [ml_buf[d, :rows, :] for d in range(n_sq - 1)]
    sums = [acc_buf[own * n_sq * heads + rows:, :]] + [ml_buf[d, rows:, :] for d in range(n_sq - 1)]
    top = functools.reduce(jnp.maximum, maxima)
    scales = [jnp.exp(m - top) for m in maxima]
    den = sum(e * s for e, s in zip(scales, sums))
    scales = [e / den for e in scales]
    lane = lax.broadcasted_iota(jnp.int32, (rows, dim), 1)

    def when(cond):
        return pl.when(cond)

    def project(c):
        all_of(sq_buf.at[c], sq_send, sq_recv.at[c]).wait_recv()
        for j in range(pairs):
            p = sq * (own // 2) + c * pairs + j
            pick = lane == p
            mine = pl.multiple_of(sq * (own * heads) + c * fold + j * rows, rows)
            terms = [acc_buf[pl.ds(mine, rows), :]]
            terms += [sq_buf[c, d, j * rows:(j + 1) * rows, :] for d in range(n_sq - 1)]
            total = sum(jnp.sum(jnp.where(pick, e, 0.0), axis=1, keepdims=True) * t for e, t in zip(scales, terms))
            a_buf[j * rows:(j + 1) * rows, :] = total
        lhs = jnp.concatenate([a_buf[pl.ds(n, step, stride=heads), :].astype(BF16) for n in range(heads)], axis=1)
        for t in range(n_tp):
            z_out[c, t] = jnp.dot(lhs, wo_ref[:, t * cols:(t + 1) * cols], preferred_element_type=F32)

        @when(jnp.logical_not(middle))
        def _():
            m_copy(c).start()

        n_copy(c).start()

    def add(c):
        @when(middle)
        def _():
            m_copy(c).wait_recv()
            for k in range(half):
                z_out[c, far + k] = z_out[c, far + k] + far_in[c, k]
            for k in range(half):
                s_copy(k, c).start()

    def share(tag, c):
        y_copy(tag, c).start()
        c_copy(tag, c).start()

    def finish(c):
        all_of(in_buf.at[c], z_send, s_recv.at[c]).wait_recv()
        total = z_out[c, tp] + in_buf[c, 0] + in_buf[c, 1]
        total = total + base_buf[c * step:(c + 1) * step, :]
        mine = block(sq, tp, c)
        mine[...] = total

        if c < relayed:
            @when(tp < n_tp - 1)
            def _():
                tp_copy(tp, c, tp + 1).start()

            @when(tp > 0)
            def _():
                tp_copy(tp, c, tp - 1).start()
        else:
            for d in range(1, n_tp):
                tp_copy(tp, c, lax.rem(tp + d, n_tp)).start()

        share(0, c)

    def direct(d, c):
        tp_copy(source_of(d, c), c, tp).wait_recv()
        share(d, c)

    def hop(h, c):
        @when(tp >= h)
        def _():
            tp_copy(tp - h, c, tp).wait_recv()

            @when(tp < n_tp - 1)
            def _():
                tp_copy(tp - h, c, tp + 1).start()

            share(h, c)

        @when(tp + h < n_tp)
        def _():
            tp_copy(tp + h, c, tp).wait_recv()

            @when(tp > 0)
            def _():
                tp_copy(tp + h, c, tp - 1).start()

            share(h + n_tp - 1, c)

    def crossed(h, c):
        def take(tag):
            y_copy(tag, c).wait_recv()
            f_copy(tag, c).start()

        if h == 0 or c >= relayed:
            take(h)
            return

        @when(tp >= h)
        def _():
            take(h)

        @when(tp + h < n_tp)
        def _():
            take(h + n_tp - 1)

    def named(name, fn, *args):
        def run():
            with jax.named_scope(name):
                fn(*args)
        return run

    events = []
    for c in range(parts):
        events.append((6.3 + 5.6 / parts * c, 0, named(f"p{c}", project, c)))
        events.append((8.1 + 8.4 / parts * (c + 1), 0, named(f"a{c}", add, c)))
        t = 11.7 + 8.4 / parts * (c + 1)
        events.append((t, 1, named(f"f{c}", finish, c)))
        events.append((t + 2.8, 3, named(f"y{c}_0", crossed, 0, c)))
        for h in range(1, n_tp):
            if c < relayed:
                there = t + 3.6 * h - 0.7
                events.append((there, 2, named(f"h{c}_{h}", hop, h, c)))
            else:
                there = t + 3.2 + 0.8 * h
                events.append((there, 2, named(f"d{c}_{h}", direct, h, c)))
            events.append((there + 2.8, 3, named(f"y{c}_{h}", crossed, h, c)))
    for _, _, event in sorted(events, key=lambda e: e[:2]):
        event()

    whole = y_buf.at[pl.ds(0, own)]
    with jax.named_scope("close"):
        all_of(whole, c_send, c_recv).wait()
        all_of(whole, f_send, f_recv).wait()
        all_of(whole, y_send, f_recv).wait_send()
        all_of(sq_buf, sq_send, ml_recv).wait_send()
        all_of(z_out.at[:, pl.ds(0, half + 1)], z_send, ml_recv).wait_send()
        straight = (parts - relayed) * (n_tp - 1)

        @when(middle)
        def _():
            blocks = y_buf.at[pl.ds(0, (straight + relayed * (n_tp + 1)) * step // n_tp)]
            all_of(blocks, g_send, ml_recv).wait_send()

        @when(jnp.logical_not(middle))
        def _():
            blocks = y_buf.at[pl.ds(0, (straight + relayed) * step // n_tp)]
            all_of(blocks, g_send, ml_recv).wait_send()

    chunk = 32
    for i in range(y_buf.shape[0] // chunk):
      with jax.named_scope(f'emit{i}'):
        out_ref[i * chunk:(i + 1) * chunk, :] = y_buf[i * chunk:(i + 1) * chunk, :].astype(BF16)


def meet(acc, x, wo, bo, n_sq, n_tp, parts=4, relayed=3):
    batch, width = x.shape
    own = batch // n_sq
    cols = width // n_tp
    step = own // parts
    heads = wo.shape[0] // acc.shape[1]
    dim = acc.shape[1]
    vmem = pl.BlockSpec(memory_space=pltpu.VMEM)
    dma = pltpu.SemaphoreType.DMA
    return pl.pallas_call(
        functools.partial(meet_kernel, parts, relayed),
        out_shape=jax.ShapeDtypeStruct((batch, width), BF16),
        in_specs=[vmem] * 4,
        out_specs=vmem,
        scratch_shapes=[
            pltpu.VMEM((own, cols), F32),
            pltpu.VMEM((parts, n_sq - 1, step * heads, dim), F32),
            pltpu.VMEM((n_sq - 1, 4 * heads, dim), F32),
            pltpu.VMEM((step * heads, dim), F32),
            pltpu.VMEM((parts, n_tp, step, cols), F32),
            pltpu.VMEM((parts, n_tp // 2, step, cols), F32),
            pltpu.VMEM((parts, 2, step, cols), F32),
            pltpu.VMEM((batch, width), F32),
            dma, dma, dma, dma((parts,)),
            dma, dma((parts,)), dma((parts,)), dma, dma((n_tp, parts)),
            dma, dma((n_tp, parts)), dma, dma, dma, dma,
        ],
        compiler_params=pltpu.CompilerParams(collective_id=0, has_side_effects=True, vmem_limit_bytes=32 * 1024 * 1024),
        cost_estimate=pl.CostEstimate(flops=2**28, bytes_accessed=8 * 2**20, transcendentals=0),
        name="meet",
    )(acc, x, wo, bo.reshape(1, width))


def solution(mesh):
    def local_step(hidden, cache_lens, k_cache, v_cache, ln_gain, ln_bias, w_query, b_query, w_kv, b_kv, w_out, b_out):
        key_new, val_new, acc = attend(
            cache_lens, hidden, ln_gain, ln_bias, w_query, b_query, w_kv, b_kv, k_cache, v_cache)
        out_hidden = meet(acc, hidden, w_out, b_out, mesh.shape["sq"], mesh.shape["tp"])
        return out_hidden, key_new, val_new

    cache_spec = P("dp", "sq", None)
    row_spec = P("dp", None)
    in_specs = (row_spec, P("dp"), cache_spec, cache_spec, P(None), P(None), P(None, "tp"), P("tp"), P(None, None), P(None), P("tp", None), P(None))
    out_specs = (row_spec, cache_spec, cache_spec)
    return jax.shard_map(local_step, mesh=mesh, in_specs=in_specs, out_specs=out_specs, check_vma=False)
```

```python
import functools

import jax
import jax.numpy as jnp
from jax import lax
from jax.experimental import pallas as pl
from jax.experimental.pallas import tpu as pltpu
from jax.sharding import PartitionSpec as P

F32 = jnp.float32
BF16 = jnp.bfloat16
NEG = -1e30


def attend_kernel(
    pairs, held, lens_ref, x_hbm, gain_ref, bias_ref, wq_hbm, bq_ref, wkv_hbm, bkv_ref, k_hbm, v_hbm,
    k_out, v_out, acc_out,
    x_buf, h_buf, wq_buf, wkv_buf, q_buf, kv_buf, s_buf, acc_ref, ml_ref, k_buf, v_buf,
    in_sem, k_sem, v_sem, ko_sem, vo_sem, acc_sem, ml_sem,
):
    batch, pos_local, dim = k_buf.shape
    heads = wq_buf.shape[1] // dim
    per = 2 * pairs
    chunks = batch // per
    rows = 2 * heads
    first_pos = lax.axis_index("sq") * pos_local
    scale = dim ** -0.5

    x_copy = pltpu.make_async_copy(x_hbm, x_buf, in_sem.at[0])
    kv_copy = pltpu.make_async_copy(wkv_hbm, wkv_buf, in_sem.at[1])
    q_copy = pltpu.make_async_copy(wq_hbm, wq_buf, in_sem.at[2])
    x_copy.start()
    kv_copy.start()
    q_copy.start()

    def span(ref, c):
        return ref.at[pl.ds(c * per, per)]

    def k_load(c):
        return pltpu.make_async_copy(span(k_hbm, c), span(k_buf, c), k_sem.at[c])

    def v_load(c):
        return pltpu.make_async_copy(span(v_hbm, c), span(v_buf, c), v_sem.at[c])

    def k_store(c):
        return pltpu.make_async_copy(span(k_buf, c), span(k_out, c), ko_sem.at[c])

    def v_store(c):
        return pltpu.make_async_copy(span(v_buf, c), span(v_out, c), vo_sem.at[c])

    @pl.loop(0, chunks)
    def _(c):
        k_load(c).start()
        v_load(c).start()

    x_copy.wait()
    block = 32

    @pl.loop(0, batch // block)
    def _(i):
        x = x_buf[pl.ds(i * block, block), :].astype(F32)
        mean = jnp.mean(x, axis=-1, keepdims=True)
        cen = x - mean
        var = jnp.mean(cen * cen, axis=-1, keepdims=True)
        h = cen * lax.rsqrt(var + 1e-5) * gain_ref[...] + bias_ref[...]
        h_buf[pl.ds(i * block, block), :] = h.astype(BF16)

    kv_copy.wait()
    kv = jnp.dot(h_buf[...], wkv_buf[...], preferred_element_type=F32) + bkv_ref[...]
    kv_buf[...] = kv.astype(BF16).astype(F32)
    q_copy.wait()
    for n0 in range(0, heads, 2):
        cols = slice(n0 * dim, (n0 + 2) * dim)
        q = jnp.dot(h_buf[...], wq_buf[:, cols], preferred_element_type=F32) + bq_ref[:, cols]
        q = q.astype(BF16).astype(F32)
        q_buf[pl.ds(n0, batch, stride=heads), :] = q[:, :dim]
        q_buf[pl.ds(n0 + 1, batch, stride=heads), :] = q[:, dim:]

    top = lax.broadcasted_iota(jnp.int32, (rows, dim), 0) < heads
    top2 = lax.broadcasted_iota(jnp.int32, (rows, pos_local), 0) < heads
    lane = lax.broadcasted_iota(jnp.int32, (rows, dim), 1)
    place = first_pos + lax.broadcasted_iota(jnp.int32, (rows, pos_local), 1)
    sub = lax.broadcasted_iota(jnp.int32, (16, dim), 0)

    def update_rows(c):
        fresh = kv_buf[pl.ds(pl.multiple_of(c * per, per), per), :]
        for j in range(per):
            b = c * per + j
            at = lens_ref[b] - first_pos
            base = pl.multiple_of(jnp.clip(at, 0, pos_local - 1) // 16 * 16, 16)
            hit = sub == at - base
            for buf, lo in ((k_buf, 0), (v_buf, dim)):
                new = jnp.broadcast_to(fresh[j:j + 1, lo:lo + dim], (16, dim))
                old = buf[b, pl.ds(base, 16), :].astype(F32)
                buf[b, pl.ds(base, 16), :] = jnp.where(hit, new, old).astype(BF16)

    def score(c):
        out = []
        for j in range(pairs):
            p = c * pairs + j
            q = q_buf[pl.ds(pl.multiple_of(p * rows, rows), rows), :]
            lhs = jnp.concatenate([jnp.where(top, q, 0.0), jnp.where(top, 0.0, q)], axis=1).astype(BF16)
            keys = jnp.concatenate([k_buf[2 * p], k_buf[2 * p + 1]], axis=1)
            s = lax.dot_general(lhs, keys, (((1,), (1,)), ((), ())), preferred_element_type=F32)
            out.append(s)
        return out

    def weigh(c, m_all, l_all):
        for j in range(pairs):
            p = c * pairs + j
            s = s_buf[j * rows:(j + 1) * rows, :] * scale
            last = jnp.where(top2, lens_ref[2 * p], lens_ref[2 * p + 1])
            valid = place <= last
            s = jnp.where(valid, s, NEG)
            m = jnp.max(s, axis=-1, keepdims=True)
            w = jnp.where(valid, jnp.exp(s - m), 0.0)
            total = jnp.sum(w, axis=-1, keepdims=True)
            vals = jnp.concatenate([v_buf[2 * p], v_buf[2 * p + 1]], axis=1)
            o = jnp.dot(w.astype(BF16), vals, preferred_element_type=F32)
            acc_ref[pl.ds(pl.multiple_of(p * rows, rows), rows), :] = jnp.where(top, o[:, :dim], o[:, dim:])
            m_all = jnp.where(lane == p, m, m_all)
            l_all = jnp.where(lane == p, total, l_all)
        return m_all, l_all

    def put_scores(out):
        for j, s in enumerate(out):
            s_buf[j * rows:(j + 1) * rows, :] = s

    def acc_store(c):
        part = pl.ds(pl.multiple_of(c * (pairs * rows), pairs * rows), pairs * rows)
        return pltpu.make_async_copy(acc_ref.at[part], acc_out.at[part], acc_sem.at[c])

    def loaded(c):
        k_load(c).wait()
        v_load(c).wait()

    def leave(c):
        k_store(c).start()
        v_store(c).start()

    loaded(0)
    update_rows(0)
    put_scores(score(0))
    zero = jnp.zeros((rows, dim), F32)

    def early(c, carry):
        loaded(c + 1)
        update_rows(c + 1)
        carry = weigh(c, *carry)
        put_scores(score(c + 1))
        acc_store(c).start()
        return carry

    carry = lax.fori_loop(0, held, early, (zero, zero))

    @pl.loop(held + 1, chunks)
    def _(c):
        loaded(c)

    @pl.loop(0, held + 1)
    def _(c):
        leave(c)

    def late(c, carry):
        update_rows(c + 1)
        carry = weigh(c, *carry)
        put_scores(score(c + 1))
        acc_store(c).start()
        leave(c + 1)
        return carry

    carry = lax.fori_loop(held, chunks - 1, late, carry)
    m_all, l_all = weigh(chunks - 1, *carry)
    ml_ref[:rows, :] = m_all
    ml_ref[rows:, :] = l_all
    acc_store(chunks - 1).start()

    @pl.loop(0, chunks - 1)
    def _(c):
        k_store(c).wait()
        v_store(c).wait()
        acc_store(c).wait()

    ml_store = pltpu.make_async_copy(ml_ref, acc_out.at[pl.ds(batch * heads, 2 * rows)], ml_sem)
    ml_store.start()
    k_store(chunks - 1).wait()
    v_store(chunks - 1).wait()
    acc_store(chunks - 1).wait()
    ml_store.wait()


def attend(lens, x, gain, bias, wq, bq, wkv, bkv, k, v, pairs=8, held=6):
    batch, pos_local, dim = k.shape
    width = x.shape[1]
    heads = wq.shape[1] // dim
    chunks = batch // (2 * pairs)
    hbm = pl.BlockSpec(memory_space=pltpu.HBM)
    vmem = pl.BlockSpec(memory_space=pltpu.VMEM)
    dma = pltpu.SemaphoreType.DMA
    return pl.pallas_call(
        functools.partial(attend_kernel, pairs, held),
        out_shape=(
            jax.ShapeDtypeStruct(k.shape, k.dtype),
            jax.ShapeDtypeStruct(v.shape, v.dtype),
            jax.ShapeDtypeStruct((batch * heads + 4 * heads, dim), F32),
        ),
        in_specs=[pl.BlockSpec(memory_space=pltpu.SMEM), hbm, vmem, vmem, hbm, vmem, hbm, vmem, hbm, hbm],
        out_specs=(hbm, hbm, hbm),
        scratch_shapes=[
            pltpu.VMEM(x.shape, BF16),
            pltpu.VMEM(x.shape, BF16),
            pltpu.VMEM(wq.shape, BF16),
            pltpu.VMEM(wkv.shape, BF16),
            pltpu.VMEM((batch * heads, dim), F32),
            pltpu.VMEM((batch, 2 * dim), F32),
            pltpu.VMEM((pairs * 2 * heads, pos_local), F32),
            pltpu.VMEM((batch * heads, dim), F32),
            pltpu.VMEM((4 * heads, dim), F32),
            pltpu.VMEM(k.shape, BF16),
            pltpu.VMEM(v.shape, BF16),
            dma((3,)), dma((chunks,)), dma((chunks,)), dma((chunks,)), dma((chunks,)), dma((chunks,)), dma,
        ],
        compiler_params=pltpu.CompilerParams(vmem_limit_bytes=60 * 1024 * 1024),
        cost_estimate=pl.CostEstimate(flops=2 * 2**30, bytes_accessed=72 * 2**20, transcendentals=0),
        name="attend",
    )(lens, x, gain.reshape(1, width), bias.reshape(1, width), wq, bq.reshape(1, -1), wkv, bkv.reshape(1, -1), k, v)


def meet_kernel(
    n_sq, parts, relayed, acc_hbm, x_ref, wo_ref, bo_ref, out_ref,
    acc_buf, base_buf, pair_buf, ml_pair, up_buf, ml_up, cross_buf, ml_cross, a_buf, z_out, far_in, in_buf, y_buf,
    in_sem, ml_send, ml_recv, mlu_send, mlu_recv, pair_send, pair_recv, up_send, up_recv, z_send, m_recv, s_recv, g_send, g_recv, y_send, y_recv, c_send, c_recv, f_send, f_recv,
):
    n_tp = z_out.shape[1]
    width = y_buf.shape[1]
    dim = acc_buf.shape[1]
    sq, tp = lax.axis_index("sq"), lax.axis_index("tp")
    own = y_buf.shape[0] // n_sq
    step = own // parts
    cols = width // n_tp
    heads = wo_ref.shape[0] // dim
    rows = 2 * heads
    pairs = step // 2
    fold = step * heads
    mesh_id = pl.DeviceIdType.MESH

    def at_tp(d):
        return {"tp": lax.rem(tp + d, n_tp)}

    core_sq = sq + 1 - 2 * lax.rem(sq, 2)
    across_sq = lax.rem(sq + 2, n_sq)
    core, across = {"sq": core_sq}, {"sq": across_sq}

    acc_in = pltpu.make_async_copy(acc_hbm, acc_buf, in_sem)
    acc_in.start()
    barrier = pltpu.get_barrier_semaphore()
    for to in (core, across):
        pl.semaphore_signal(barrier, inc=1, device_id=to, device_id_type=mesh_id)
    for d in range(1, n_tp):
        pl.semaphore_signal(barrier, inc=1, device_id=at_tp(d), device_id_type=mesh_id)
    x_cols = pl.ds(pl.multiple_of(tp * cols, cols), cols)
    base_buf[...] = x_ref[pl.ds(pl.multiple_of(sq * own, own), own), x_cols].astype(F32) + bo_ref[:, x_cols]
    ml_own = acc_buf.at[pl.ds(own * n_sq * heads, 2 * rows)]
    with jax.named_scope('barrier'):
        acc_in.wait()
        pl.semaphore_wait(barrier, 2 + n_tp - 1)

    def remote(src, dst, send, recv, to):
        return pltpu.make_async_remote_copy(src_ref=src, dst_ref=dst, send_sem=send, recv_sem=recv, device_id=to, device_id_type=mesh_id)

    def acc_rows(s, c):
        return pl.ds(pl.multiple_of(s * (own * heads) + c * fold, fold), fold)

    def pair_copy(k, c):
        rows_for = acc_rows(core_sq if k == 0 else lax.rem(core_sq + 2, n_sq), c)
        return remote(acc_buf.at[rows_for], pair_buf.at[k, c], pair_send, pair_recv.at[k, c], core)

    def up_copy(c):
        return remote(up_buf.at[c], cross_buf.at[c], up_send, up_recv.at[c], across)

    ml_copy = remote(ml_own, ml_pair, ml_send, ml_recv, core)
    mlu_copy = remote(ml_up, ml_cross, mlu_send, mlu_recv, across)

    half = n_tp // 2
    middle = lax.div(tp + 1, 2) == 1
    partner = tp + 1 - 2 * lax.rem(tp, 2)
    far = half - half * lax.div(tp, half)

    def m_copy(c):
        return remote(z_out.at[c, pl.ds(far, half)], far_in.at[c], z_send, m_recv.at[c], {"tp": partner})

    def n_copy(c):
        return remote(z_out.at[c, partner], in_buf.at[c, 0], z_send, s_recv.at[c], {"tp": partner})

    def s_copy(k, c):
        return remote(z_out.at[c, far + k], in_buf.at[c, 1], z_send, s_recv.at[c], {"tp": far + k})

    def block(s, t, c):
        return y_buf.at[pl.ds(pl.multiple_of(s * own + c * step, step), step), pl.ds(pl.multiple_of(t * cols, cols), cols)]

    def source(tag):
        return tp - tag if tag < n_tp else tp + (tag - n_tp + 1)

    def source_of(tag, c):
        return source(tag) if c < relayed else lax.rem(tp - tag + n_tp, n_tp)

    def tp_copy(t, c, to):
        b = block(sq, t, c)
        return remote(b, b, g_send, g_recv.at[t, c], {"tp": to})

    def y_copy(tag, c):
        t = source_of(tag, c)
        b = block(sq, t, c)
        return remote(b, b, y_send, y_recv.at[t, c], across)

    def c_copy(tag, c):
        b = block(sq, source_of(tag, c), c)
        return remote(b, b, c_send, c_recv, core)

    def f_copy(tag, c):
        b = block(across_sq, source_of(tag, c), c)
        return remote(b, b, f_send, f_recv, core)

    def all_of(ref, send, recv):
        return remote(ref, ref, send, recv, {"tp": tp})

    ml_copy.start()
    for k in (1, 0):
        for c in range(parts):
            pair_copy(k, c).start()

    lane = lax.broadcasted_iota(jnp.int32, (rows, dim), 1)

    def column(e, p):
        return jnp.sum(jnp.where(lane == p, e, 0.0), axis=1, keepdims=True)

    def part_of(j):
        return slice(j * rows, (j + 1) * rows)

    with jax.named_scope("pairwait"):
        ml_copy.wait_recv()
    ml_at = own * n_sq * heads
    m_own, l_own = acc_buf[ml_at:ml_at + rows, :], acc_buf[ml_at + rows:ml_at + 2 * rows, :]
    m_pair, l_pair = ml_pair[:rows, :], ml_pair[rows:, :]
    m_up = jnp.maximum(m_own, m_pair)
    e_own, e_pair = jnp.exp(m_own - m_up), jnp.exp(m_pair - m_up)
    ml_up[:rows, :] = m_up
    ml_up[rows:, :] = e_own * l_own + e_pair * l_pair
    for c in range(parts):
        pair_copy(1, c).wait_recv()
        for j in range(pairs):
            p = across_sq * (own // 2) + c * pairs + j
            mine = pl.multiple_of(across_sq * (own * heads) + c * fold + j * rows, rows)
            up_buf[c, part_of(j), :] = column(e_own, p) * acc_buf[pl.ds(mine, rows), :] + column(e_pair, p) * pair_buf[1, c, part_of(j), :]
        if c == 0:
            mlu_copy.start()
        up_copy(c).start()

    with jax.named_scope("mlwait"):
        mlu_copy.wait_recv()
    m_cross, l_cross = ml_cross[:rows, :], ml_cross[rows:, :]
    top = jnp.maximum(m_up, m_cross)
    scales = [jnp.exp(m - top) for m in (m_own, m_pair, m_cross)]
    den = scales[0] * l_own + scales[1] * l_pair + scales[2] * l_cross
    scales = [e / den for e in scales]

    def when(cond):
        return pl.when(cond)

    def project(c):
        pair_copy(0, c).wait_recv()
        up_copy(c).wait_recv()
        for j in range(pairs):
            p = sq * (own // 2) + c * pairs + j
            mine = pl.multiple_of(sq * (own * heads) + c * fold + j * rows, rows)
            terms = (acc_buf[pl.ds(mine, rows), :], pair_buf[0, c, part_of(j), :], cross_buf[c, part_of(j), :])
            total = sum(column(e, p) * t for e, t in zip(scales, terms))
            a_buf[j * rows:(j + 1) * rows, :] = total
        lhs = jnp.concatenate([a_buf[pl.ds(n, step, stride=heads), :].astype(BF16) for n in range(heads)], axis=1)
        for t in range(n_tp):
            z_out[c, t] = jnp.dot(lhs, wo_ref[:, t * cols:(t + 1) * cols], preferred_element_type=F32)

        @when(jnp.logical_not(middle))
        def _():
            m_copy(c).start()

        n_copy(c).start()

    def add(c):
        @when(middle)
        def _():
            m_copy(c).wait_recv()
            for k in range(half):
                z_out[c, far + k] = z_out[c, far + k] + far_in[c, k]
            for k in range(half):
                s_copy(k, c).start()

    def share(tag, c):
        y_copy(tag, c).start()
        c_copy(tag, c).start()

    def finish(c):
        all_of(in_buf.at[c], z_send, s_recv.at[c]).wait_recv()
        total = z_out[c, tp] + in_buf[c, 0] + in_buf[c, 1]
        total = total + base_buf[c * step:(c + 1) * step, :]
        mine = block(sq, tp, c)
        mine[...] = total

        if c < relayed:
            @when(tp < n_tp - 1)
            def _():
                tp_copy(tp, c, tp + 1).start()

            @when(tp > 0)
            def _():
                tp_copy(tp, c, tp - 1).start()
        else:
            for d in range(1, n_tp):
                tp_copy(tp, c, lax.rem(tp + d, n_tp)).start()

        share(0, c)

    def direct(d, c):
        tp_copy(source_of(d, c), c, tp).wait_recv()
        share(d, c)

    def hop(h, c):
        @when(tp >= h)
        def _():
            tp_copy(tp - h, c, tp).wait_recv()

            @when(tp < n_tp - 1)
            def _():
                tp_copy(tp - h, c, tp + 1).start()

            share(h, c)

        @when(tp + h < n_tp)
        def _():
            tp_copy(tp + h, c, tp).wait_recv()

            @when(tp > 0)
            def _():
                tp_copy(tp + h, c, tp - 1).start()

            share(h + n_tp - 1, c)

    def crossed(h, c):
        def take(tag):
            y_copy(tag, c).wait_recv()
            f_copy(tag, c).start()

        if h == 0 or c >= relayed:
            take(h)
            return

        @when(tp >= h)
        def _():
            take(h)

        @when(tp + h < n_tp)
        def _():
            take(h + n_tp - 1)

    def named(name, fn, *args):
        def run():
            with jax.named_scope(name):
                fn(*args)
        return run

    events = []
    for c in range(parts):
        events.append((6.3 + 3.0 / parts * c, 0, named(f"p{c}", project, c)))
        events.append((8.1 + 8.4 / parts * (c + 1), 0, named(f"a{c}", add, c)))
        t = 11.7 + 8.4 / parts * (c + 1)
        events.append((t, 1, named(f"f{c}", finish, c)))
        events.append((t + 2.8, 3, named(f"y{c}_0", crossed, 0, c)))
        for h in range(1, n_tp):
            if c < relayed:
                there = t + 3.6 * h - 0.7
                events.append((there, 2, named(f"h{c}_{h}", hop, h, c)))
            else:
                there = t + 3.2 + 0.8 * h
                events.append((there, 2, named(f"d{c}_{h}", direct, h, c)))
            events.append((there + 2.8, 3, named(f"y{c}_{h}", crossed, h, c)))
    for _, _, event in sorted(events, key=lambda e: e[:2]):
        event()

    whole = y_buf.at[pl.ds(0, own)]
    with jax.named_scope("close"):
        all_of(whole, c_send, c_recv).wait()
        all_of(whole, f_send, f_recv).wait()
        all_of(whole, y_send, f_recv).wait_send()
        ml_copy.wait_send()
        mlu_copy.wait_send()
        all_of(pair_buf, pair_send, ml_recv).wait_send()
        all_of(up_buf, up_send, ml_recv).wait_send()
        all_of(z_out.at[:, pl.ds(0, half + 1)], z_send, ml_recv).wait_send()
        straight = (parts - relayed) * (n_tp - 1)

        @when(middle)
        def _():
            blocks = y_buf.at[pl.ds(0, (straight + relayed * (n_tp + 1)) * step // n_tp)]
            all_of(blocks, g_send, ml_recv).wait_send()

        @when(jnp.logical_not(middle))
        def _():
            blocks = y_buf.at[pl.ds(0, (straight + relayed) * step // n_tp)]
            all_of(blocks, g_send, ml_recv).wait_send()

    chunk = 32
    for i in range(y_buf.shape[0] // chunk):
      with jax.named_scope(f'emit{i}'):
        out_ref[i * chunk:(i + 1) * chunk, :] = y_buf[i * chunk:(i + 1) * chunk, :].astype(BF16)


def meet(acc, x, wo, bo, n_sq, n_tp, parts=4, relayed=3):
    batch, width = x.shape
    own = batch // n_sq
    cols = width // n_tp
    step = own // parts
    heads = wo.shape[0] // acc.shape[1]
    dim = acc.shape[1]
    vmem = pl.BlockSpec(memory_space=pltpu.VMEM)
    hbm = pl.BlockSpec(memory_space=pltpu.HBM)
    dma = pltpu.SemaphoreType.DMA
    return pl.pallas_call(
        functools.partial(meet_kernel, n_sq, parts, relayed),
        out_shape=jax.ShapeDtypeStruct((batch, width), BF16),
        in_specs=[hbm, vmem, vmem, vmem],
        out_specs=vmem,
        scratch_shapes=[
            pltpu.VMEM(acc.shape, F32),
            pltpu.VMEM((own, cols), F32),
            pltpu.VMEM((2, parts, step * heads, dim), F32),
            pltpu.VMEM((4 * heads, dim), F32),
            pltpu.VMEM((parts, step * heads, dim), F32),
            pltpu.VMEM((4 * heads, dim), F32),
            pltpu.VMEM((parts, step * heads, dim), F32),
            pltpu.VMEM((4 * heads, dim), F32),
            pltpu.VMEM((step * heads, dim), F32),
            pltpu.VMEM((parts, n_tp, step, cols), F32),
            pltpu.VMEM((parts, n_tp // 2, step, cols), F32),
            pltpu.VMEM((parts, 2, step, cols), F32),
            pltpu.VMEM((batch, width), F32),
            dma, dma, dma, dma, dma, dma, dma((2, parts)), dma, dma((parts,)),
            dma, dma((parts,)), dma((parts,)), dma, dma((n_tp, parts)),
            dma, dma((n_tp, parts)), dma, dma, dma, dma,
        ],
        compiler_params=pltpu.CompilerParams(collective_id=0, has_side_effects=True, vmem_limit_bytes=32 * 1024 * 1024),
        cost_estimate=pl.CostEstimate(flops=2**28, bytes_accessed=8 * 2**20, transcendentals=0),
        name="meet",
    )(pltpu.with_memory_space_constraint(acc, pltpu.HBM), x, wo, bo.reshape(1, width))


def solution(mesh):
    def local_step(hidden, cache_lens, k_cache, v_cache, ln_gain, ln_bias, w_query, b_query, w_kv, b_kv, w_out, b_out):
        key_new, val_new, acc = attend(
            cache_lens, hidden, ln_gain, ln_bias, w_query, b_query, w_kv, b_kv, k_cache, v_cache)
        out_hidden = meet(acc, hidden, w_out, b_out, mesh.shape["sq"], mesh.shape["tp"])
        return out_hidden, key_new, val_new

    cache_spec = P("dp", "sq", None)
    row_spec = P("dp", None)
    in_specs = (row_spec, P("dp"), cache_spec, cache_spec, P(None), P(None), P(None, "tp"), P("tp"), P(None, None), P(None), P("tp", None), P(None))
    out_specs = (row_spec, cache_spec, cache_spec)
    return jax.shard_map(local_step, mesh=mesh, in_specs=in_specs, out_specs=out_specs, check_vma=False)
```

```python
import functools

import jax
import jax.numpy as jnp
from jax import lax
from jax.experimental import pallas as pl
from jax.experimental.pallas import tpu as pltpu
from jax.sharding import PartitionSpec as P

F32 = jnp.float32
BF16 = jnp.bfloat16
NEG = -1e30


def attend_kernel(
    pairs, held, lens_ref, x_hbm, gain_ref, bias_ref, wq_hbm, bq_ref, wkv_hbm, bkv_ref, k_hbm, v_hbm,
    k_out, v_out, acc_out,
    x_buf, h_buf, wq_buf, wkv_buf, q_buf, kv_buf, s_buf, acc_ref, ml_ref, k_buf, v_buf,
    in_sem, k_sem, v_sem, ko_sem, vo_sem, acc_sem, ml_sem,
):
    batch, pos_local, dim = k_buf.shape
    heads = wq_buf.shape[1] // dim
    per = 2 * pairs
    chunks = batch // per
    rows = 2 * heads
    first_pos = lax.axis_index("sq") * pos_local
    scale = dim ** -0.5

    x_copy = pltpu.make_async_copy(x_hbm, x_buf, in_sem.at[0])
    kv_copy = pltpu.make_async_copy(wkv_hbm, wkv_buf, in_sem.at[1])
    q_copy = pltpu.make_async_copy(wq_hbm, wq_buf, in_sem.at[2])
    x_copy.start()
    kv_copy.start()
    q_copy.start()

    def span(ref, c):
        return ref.at[pl.ds(c * per, per)]

    def k_load(c):
        return pltpu.make_async_copy(span(k_hbm, c), span(k_buf, c), k_sem.at[c])

    def v_load(c):
        return pltpu.make_async_copy(span(v_hbm, c), span(v_buf, c), v_sem.at[c])

    def k_store(c):
        return pltpu.make_async_copy(span(k_buf, c), span(k_out, c), ko_sem.at[c])

    def v_store(c):
        return pltpu.make_async_copy(span(v_buf, c), span(v_out, c), vo_sem.at[c])

    @pl.loop(0, chunks)
    def _(c):
        k_load(c).start()
        v_load(c).start(priority=1)

    x_copy.wait()
    block = 32

    @pl.loop(0, batch // block)
    def _(i):
        x = x_buf[pl.ds(i * block, block), :].astype(F32)
        mean = jnp.mean(x, axis=-1, keepdims=True)
        cen = x - mean
        var = jnp.mean(cen * cen, axis=-1, keepdims=True)
        h = cen * lax.rsqrt(var + 1e-5) * gain_ref[...] + bias_ref[...]
        h_buf[pl.ds(i * block, block), :] = h.astype(BF16)

    kv_copy.wait()
    kv = jnp.dot(h_buf[...], wkv_buf[...], preferred_element_type=F32) + bkv_ref[...]
    kv_buf[...] = kv.astype(BF16).astype(F32)
    q_copy.wait()
    for n0 in range(0, heads, 2):
        cols = slice(n0 * dim, (n0 + 2) * dim)
        q = jnp.dot(h_buf[...], wq_buf[:, cols], preferred_element_type=F32) + bq_ref[:, cols]
        q = q.astype(BF16).astype(F32)
        q_buf[pl.ds(n0, batch, stride=heads), :] = q[:, :dim]
        q_buf[pl.ds(n0 + 1, batch, stride=heads), :] = q[:, dim:]

    top = lax.broadcasted_iota(jnp.int32, (rows, dim), 0) < heads
    top2 = lax.broadcasted_iota(jnp.int32, (rows, pos_local), 0) < heads
    lane = lax.broadcasted_iota(jnp.int32, (rows, dim), 1)
    place = first_pos + lax.broadcasted_iota(jnp.int32, (rows, pos_local), 1)
    sub = lax.broadcasted_iota(jnp.int32, (16, dim), 0)

    def update_rows(c):
        fresh = kv_buf[pl.ds(pl.multiple_of(c * per, per), per), :]
        for j in range(per):
            b = c * per + j
            at = lens_ref[b] - first_pos
            base = pl.multiple_of(jnp.clip(at, 0, pos_local - 1) // 16 * 16, 16)
            hit = sub == at - base
            for buf, lo in ((k_buf, 0), (v_buf, dim)):
                new = jnp.broadcast_to(fresh[j:j + 1, lo:lo + dim], (16, dim))
                old = buf[b, pl.ds(base, 16), :].astype(F32)
                buf[b, pl.ds(base, 16), :] = jnp.where(hit, new, old).astype(BF16)

    def score(c):
        out = []
        for j in range(pairs):
            p = c * pairs + j
            q = q_buf[pl.ds(pl.multiple_of(p * rows, rows), rows), :]
            lhs = jnp.concatenate([jnp.where(top, q, 0.0), jnp.where(top, 0.0, q)], axis=1).astype(BF16)
            keys = jnp.concatenate([k_buf[2 * p], k_buf[2 * p + 1]], axis=1)
            s = lax.dot_general(lhs, keys, (((1,), (1,)), ((), ())), preferred_element_type=F32)
            out.append(s)
        return out

    def weigh(c, m_all, l_all):
        for j in range(pairs):
            p = c * pairs + j
            s = s_buf[j * rows:(j + 1) * rows, :] * scale
            last = jnp.where(top2, lens_ref[2 * p], lens_ref[2 * p + 1])
            valid = place <= last
            s = jnp.where(valid, s, NEG)
            m = jnp.max(s, axis=-1, keepdims=True)
            w = jnp.where(valid, jnp.exp(s - m), 0.0)
            total = jnp.sum(w, axis=-1, keepdims=True)
            vals = jnp.concatenate([v_buf[2 * p], v_buf[2 * p + 1]], axis=1)
            o = jnp.dot(w.astype(BF16), vals, preferred_element_type=F32)
            acc_ref[pl.ds(pl.multiple_of(p * rows, rows), rows), :] = jnp.where(top, o[:, :dim], o[:, dim:])
            m_all = jnp.where(lane == p, m, m_all)
            l_all = jnp.where(lane == p, total, l_all)
        return m_all, l_all

    def put_scores(out):
        for j, s in enumerate(out):
            s_buf[j * rows:(j + 1) * rows, :] = s

    def acc_store(c):
        part = pl.ds(pl.multiple_of(c * (pairs * rows), pairs * rows), pairs * rows)
        return pltpu.make_async_copy(acc_ref.at[part], acc_out.at[part], acc_sem.at[c])

    def loaded(c):
        k_load(c).wait()
        v_load(c).wait()

    def leave(c):
        k_store(c).start()
        v_store(c).start(priority=1)

    loaded(0)
    update_rows(0)
    put_scores(score(0))
    zero = jnp.zeros((rows, dim), F32)

    def early(c, carry):
        loaded(c + 1)
        update_rows(c + 1)
        carry = weigh(c, *carry)
        put_scores(score(c + 1))
        acc_store(c).start()
        return carry

    carry = lax.fori_loop(0, held, early, (zero, zero))

    @pl.loop(held + 1, chunks)
    def _(c):
        loaded(c)

    @pl.loop(0, held + 1)
    def _(c):
        leave(c)

    def late(c, carry):
        update_rows(c + 1)
        carry = weigh(c, *carry)
        put_scores(score(c + 1))
        acc_store(c).start()
        leave(c + 1)
        return carry

    carry = lax.fori_loop(held, chunks - 1, late, carry)
    m_all, l_all = weigh(chunks - 1, *carry)
    ml_ref[:rows, :] = m_all
    ml_ref[rows:, :] = l_all
    acc_store(chunks - 1).start()

    @pl.loop(0, chunks - 1)
    def _(c):
        k_store(c).wait()
        v_store(c).wait()
        acc_store(c).wait()

    ml_store = pltpu.make_async_copy(ml_ref, acc_out.at[pl.ds(batch * heads, 2 * rows)], ml_sem)
    ml_store.start()
    k_store(chunks - 1).wait()
    v_store(chunks - 1).wait()
    acc_store(chunks - 1).wait()
    ml_store.wait()


def attend(lens, x, gain, bias, wq, bq, wkv, bkv, k, v, pairs=8, held=6):
    batch, pos_local, dim = k.shape
    width = x.shape[1]
    heads = wq.shape[1] // dim
    chunks = batch // (2 * pairs)
    hbm = pl.BlockSpec(memory_space=pltpu.HBM)
    vmem = pl.BlockSpec(memory_space=pltpu.VMEM)
    dma = pltpu.SemaphoreType.DMA
    return pl.pallas_call(
        functools.partial(attend_kernel, pairs, held),
        out_shape=(
            jax.ShapeDtypeStruct(k.shape, k.dtype),
            jax.ShapeDtypeStruct(v.shape, v.dtype),
            jax.ShapeDtypeStruct((batch * heads + 4 * heads, dim), F32),
        ),
        in_specs=[pl.BlockSpec(memory_space=pltpu.SMEM), hbm, vmem, vmem, hbm, vmem, hbm, vmem, hbm, hbm],
        out_specs=(hbm, hbm, hbm),
        scratch_shapes=[
            pltpu.VMEM(x.shape, BF16),
            pltpu.VMEM(x.shape, BF16),
            pltpu.VMEM(wq.shape, BF16),
            pltpu.VMEM(wkv.shape, BF16),
            pltpu.VMEM((batch * heads, dim), F32),
            pltpu.VMEM((batch, 2 * dim), F32),
            pltpu.VMEM((pairs * 2 * heads, pos_local), F32),
            pltpu.VMEM((batch * heads, dim), F32),
            pltpu.VMEM((4 * heads, dim), F32),
            pltpu.VMEM(k.shape, BF16),
            pltpu.VMEM(v.shape, BF16),
            dma((3,)), dma((chunks,)), dma((chunks,)), dma((chunks,)), dma((chunks,)), dma((chunks,)), dma,
        ],
        compiler_params=pltpu.CompilerParams(vmem_limit_bytes=60 * 1024 * 1024),
        cost_estimate=pl.CostEstimate(flops=2 * 2**30, bytes_accessed=72 * 2**20, transcendentals=0),
        name="attend",
    )(lens, x, gain.reshape(1, width), bias.reshape(1, width), wq, bq.reshape(1, -1), wkv, bkv.reshape(1, -1), k, v)


def meet_kernel(
    n_sq, parts, relayed, acc_hbm, x_ref, wo_ref, bo_ref, out_ref,
    acc_buf, base_buf, pair_buf, ml_pair, up_buf, ml_up, cross_buf, ml_cross, a_buf, z_out, far_in, in_buf, y_buf,
    in_sem, ml_send, ml_recv, mlu_send, mlu_recv, pair_send, pair_recv, up_send, up_recv, z_send, m_recv, s_recv, g_send, g_recv, y_send, y_recv, c_send, c_recv, f_send, f_recv,
):
    n_tp = z_out.shape[1]
    width = y_buf.shape[1]
    dim = acc_buf.shape[1]
    sq, tp = lax.axis_index("sq"), lax.axis_index("tp")
    own = y_buf.shape[0] // n_sq
    step = own // parts
    cols = width // n_tp
    heads = wo_ref.shape[0] // dim
    rows = 2 * heads
    pairs = step // 2
    fold = step * heads
    mesh_id = pl.DeviceIdType.MESH

    def at_tp(d):
        return {"tp": lax.rem(tp + d, n_tp)}

    core_sq = sq + 1 - 2 * lax.rem(sq, 2)
    across_sq = lax.rem(sq + 2, n_sq)
    core, across = {"sq": core_sq}, {"sq": across_sq}

    acc_in = pltpu.make_async_copy(acc_hbm, acc_buf, in_sem)
    acc_in.start()
    barrier = pltpu.get_barrier_semaphore()
    for to in (core, across):
        pl.semaphore_signal(barrier, inc=1, device_id=to, device_id_type=mesh_id)
    for d in range(1, n_tp):
        pl.semaphore_signal(barrier, inc=1, device_id=at_tp(d), device_id_type=mesh_id)
    x_cols = pl.ds(pl.multiple_of(tp * cols, cols), cols)
    base_buf[...] = x_ref[pl.ds(pl.multiple_of(sq * own, own), own), x_cols].astype(F32) + bo_ref[:, x_cols]
    ml_own = acc_buf.at[pl.ds(own * n_sq * heads, 2 * rows)]
    with jax.named_scope('barrier'):
        acc_in.wait()
        pl.semaphore_wait(barrier, 2 + n_tp - 1)

    def remote(src, dst, send, recv, to):
        return pltpu.make_async_remote_copy(src_ref=src, dst_ref=dst, send_sem=send, recv_sem=recv, device_id=to, device_id_type=mesh_id)

    def acc_rows(s, c):
        return pl.ds(pl.multiple_of(s * (own * heads) + c * fold, fold), fold)

    def pair_copy(k, c):
        rows_for = acc_rows(core_sq if k == 0 else lax.rem(core_sq + 2, n_sq), c)
        return remote(acc_buf.at[rows_for], pair_buf.at[k, c], pair_send, pair_recv.at[k, c], core)

    def up_copy(c):
        return remote(up_buf.at[c], cross_buf.at[c], up_send, up_recv.at[c], across)

    ml_copy = remote(ml_own, ml_pair, ml_send, ml_recv, core)
    mlu_copy = remote(ml_up, ml_cross, mlu_send, mlu_recv, across)

    half = n_tp // 2
    middle = lax.div(tp + 1, 2) == 1
    partner = tp + 1 - 2 * lax.rem(tp, 2)
    far = half - half * lax.div(tp, half)

    def m_copy(c):
        return remote(z_out.at[c, pl.ds(far, half)], far_in.at[c], z_send, m_recv.at[c], {"tp": partner})

    def n_copy(c):
        return remote(z_out.at[c, partner], in_buf.at[c, 0], z_send, s_recv.at[c], {"tp": partner})

    def s_copy(k, c):
        return remote(z_out.at[c, far + k], in_buf.at[c, 1], z_send, s_recv.at[c], {"tp": far + k})

    def block(s, t, c):
        return y_buf.at[pl.ds(pl.multiple_of(s * own + c * step, step), step), pl.ds(pl.multiple_of(t * cols, cols), cols)]

    def source(tag):
        return tp - tag if tag < n_tp else tp + (tag - n_tp + 1)

    def source_of(tag, c):
        return source(tag) if c < relayed else lax.rem(tp - tag + n_tp, n_tp)

    def tp_copy(t, c, to):
        b = block(sq, t, c)
        return remote(b, b, g_send, g_recv.at[t, c], {"tp": to})

    def y_copy(tag, c):
        t = source_of(tag, c)
        b = block(sq, t, c)
        return remote(b, b, y_send, y_recv.at[t, c], across)

    def c_copy(tag, c):
        b = block(sq, source_of(tag, c), c)
        return remote(b, b, c_send, c_recv, core)

    def f_copy(tag, c):
        b = block(across_sq, source_of(tag, c), c)
        return remote(b, b, f_send, f_recv, core)

    def all_of(ref, send, recv):
        return remote(ref, ref, send, recv, {"tp": tp})

    ml_copy.start()
    for k in (1, 0):
        for c in range(parts):
            pair_copy(k, c).start()

    lane = lax.broadcasted_iota(jnp.int32, (rows, dim), 1)

    def column(e, p):
        return jnp.sum(jnp.where(lane == p, e, 0.0), axis=1, keepdims=True)

    def part_of(j):
        return slice(j * rows, (j + 1) * rows)

    with jax.named_scope("pairwait"):
        ml_copy.wait_recv()
    ml_at = own * n_sq * heads
    m_own, l_own = acc_buf[ml_at:ml_at + rows, :], acc_buf[ml_at + rows:ml_at + 2 * rows, :]
    m_pair, l_pair = ml_pair[:rows, :], ml_pair[rows:, :]
    m_up = jnp.maximum(m_own, m_pair)
    e_own, e_pair = jnp.exp(m_own - m_up), jnp.exp(m_pair - m_up)
    ml_up[:rows, :] = m_up
    ml_up[rows:, :] = e_own * l_own + e_pair * l_pair
    for c in range(parts):
        pair_copy(1, c).wait_recv()
        for j in range(pairs):
            p = across_sq * (own // 2) + c * pairs + j
            mine = pl.multiple_of(across_sq * (own * heads) + c * fold + j * rows, rows)
            up_buf[c, part_of(j), :] = column(e_own, p) * acc_buf[pl.ds(mine, rows), :] + column(e_pair, p) * pair_buf[1, c, part_of(j), :]
        if c == 0:
            mlu_copy.start()
        up_copy(c).start()

    with jax.named_scope("mlwait"):
        mlu_copy.wait_recv()
    m_cross, l_cross = ml_cross[:rows, :], ml_cross[rows:, :]
    top = jnp.maximum(m_up, m_cross)
    scales = [jnp.exp(m - top) for m in (m_own, m_pair, m_cross)]
    den = scales[0] * l_own + scales[1] * l_pair + scales[2] * l_cross
    scales = [e / den for e in scales]

    def when(cond):
        return pl.when(cond)

    def project(c):
        pair_copy(0, c).wait_recv()
        up_copy(c).wait_recv()
        for j in range(pairs):
            p = sq * (own // 2) + c * pairs + j
            mine = pl.multiple_of(sq * (own * heads) + c * fold + j * rows, rows)
            terms = (acc_buf[pl.ds(mine, rows), :], pair_buf[0, c, part_of(j), :], cross_buf[c, part_of(j), :])
            total = sum(column(e, p) * t for e, t in zip(scales, terms))
            a_buf[j * rows:(j + 1) * rows, :] = total
        lhs = jnp.concatenate([a_buf[pl.ds(n, step, stride=heads), :].astype(BF16) for n in range(heads)], axis=1)
        for t in range(n_tp):
            z_out[c, t] = jnp.dot(lhs, wo_ref[:, t * cols:(t + 1) * cols], preferred_element_type=F32)

        @when(jnp.logical_not(middle))
        def _():
            m_copy(c).start()

        if c:
            n_copy(c - 1).start()
        if c == parts - 1:
            n_copy(c).start()

    def add(c):
        @when(middle)
        def _():
            m_copy(c).wait_recv()
            for k in range(half):
                z_out[c, far + k] = z_out[c, far + k] + far_in[c, k]
            for k in range(half):
                s_copy(k, c).start()

    def share(tag, c):
        y_copy(tag, c).start()
        c_copy(tag, c).start()

    def finish(c):
        all_of(in_buf.at[c], z_send, s_recv.at[c]).wait_recv()
        total = z_out[c, tp] + in_buf[c, 0] + in_buf[c, 1]
        total = total + base_buf[c * step:(c + 1) * step, :]
        mine = block(sq, tp, c)
        mine[...] = total

        if c < relayed:
            @when(tp < n_tp - 1)
            def _():
                tp_copy(tp, c, tp + 1).start()

            @when(tp > 0)
            def _():
                tp_copy(tp, c, tp - 1).start()
        else:
            for d in range(1, n_tp):
                tp_copy(tp, c, lax.rem(tp + d, n_tp)).start()

        share(0, c)

    def direct(d, c):
        tp_copy(source_of(d, c), c, tp).wait_recv()
        share(d, c)

    def hop(h, c):
        @when(tp >= h)
        def _():
            tp_copy(tp - h, c, tp).wait_recv()

            @when(tp < n_tp - 1)
            def _():
                tp_copy(tp - h, c, tp + 1).start()

            share(h, c)

        @when(tp + h < n_tp)
        def _():
            tp_copy(tp + h, c, tp).wait_recv()

            @when(tp > 0)
            def _():
                tp_copy(tp + h, c, tp - 1).start()

            share(h + n_tp - 1, c)

    def crossed(h, c):
        def take(tag):
            y_copy(tag, c).wait_recv()
            f_copy(tag, c).start()

        if h == 0 or c >= relayed:
            take(h)
            return

        @when(tp >= h)
        def _():
            take(h)

        @when(tp + h < n_tp)
        def _():
            take(h + n_tp - 1)

    def named(name, fn, *args):
        def run():
            with jax.named_scope(name):
                fn(*args)
        return run

    events = []
    for c in range(parts):
        events.append((6.3 + 3.0 / parts * c, 0, named(f"p{c}", project, c)))
        events.append((8.1 + 8.4 / parts * (c + 1), 0, named(f"a{c}", add, c)))
        t = 11.7 + 8.4 / parts * (c + 1)
        events.append((t, 1, named(f"f{c}", finish, c)))
        events.append((t + 4.0, 3, named(f"y{c}_0", crossed, 0, c)))
        for h in range(1, n_tp):
            if c < relayed:
                there = t + 3.6 * h - 0.7
                events.append((there, 2, named(f"h{c}_{h}", hop, h, c)))
            else:
                there = t + 3.2 + 0.8 * h
                events.append((there, 2, named(f"d{c}_{h}", direct, h, c)))
            events.append((there + 5.0, 3, named(f"y{c}_{h}", crossed, h, c)))
    for _, _, event in sorted(events, key=lambda e: e[:2]):
        event()

    whole = y_buf.at[pl.ds(0, own)]
    with jax.named_scope("close"):
        all_of(whole, c_send, c_recv).wait()
        all_of(whole, f_send, f_recv).wait()
        all_of(whole, y_send, f_recv).wait_send()
        ml_copy.wait_send()
        mlu_copy.wait_send()
        all_of(pair_buf, pair_send, ml_recv).wait_send()
        all_of(up_buf, up_send, ml_recv).wait_send()
        all_of(z_out.at[:, pl.ds(0, half + 1)], z_send, ml_recv).wait_send()
        straight = (parts - relayed) * (n_tp - 1)

        @when(middle)
        def _():
            blocks = y_buf.at[pl.ds(0, (straight + relayed * (n_tp + 1)) * step // n_tp)]
            all_of(blocks, g_send, ml_recv).wait_send()

        @when(jnp.logical_not(middle))
        def _():
            blocks = y_buf.at[pl.ds(0, (straight + relayed) * step // n_tp)]
            all_of(blocks, g_send, ml_recv).wait_send()

    chunk = 32
    for i in range(y_buf.shape[0] // chunk):
      with jax.named_scope(f'emit{i}'):
        out_ref[i * chunk:(i + 1) * chunk, :] = y_buf[i * chunk:(i + 1) * chunk, :].astype(BF16)


def meet(acc, x, wo, bo, n_sq, n_tp, parts=4, relayed=2):
    batch, width = x.shape
    own = batch // n_sq
    cols = width // n_tp
    step = own // parts
    heads = wo.shape[0] // acc.shape[1]
    dim = acc.shape[1]
    vmem = pl.BlockSpec(memory_space=pltpu.VMEM)
    hbm = pl.BlockSpec(memory_space=pltpu.HBM)
    dma = pltpu.SemaphoreType.DMA
    return pl.pallas_call(
        functools.partial(meet_kernel, n_sq, parts, relayed),
        out_shape=jax.ShapeDtypeStruct((batch, width), BF16),
        in_specs=[hbm, vmem, vmem, vmem],
        out_specs=vmem,
        scratch_shapes=[
            pltpu.VMEM(acc.shape, F32),
            pltpu.VMEM((own, cols), F32),
            pltpu.VMEM((2, parts, step * heads, dim), F32),
            pltpu.VMEM((4 * heads, dim), F32),
            pltpu.VMEM((parts, step * heads, dim), F32),
            pltpu.VMEM((4 * heads, dim), F32),
            pltpu.VMEM((parts, step * heads, dim), F32),
            pltpu.VMEM((4 * heads, dim), F32),
            pltpu.VMEM((step * heads, dim), F32),
            pltpu.VMEM((parts, n_tp, step, cols), F32),
            pltpu.VMEM((parts, n_tp // 2, step, cols), F32),
            pltpu.VMEM((parts, 2, step, cols), F32),
            pltpu.VMEM((batch, width), F32),
            dma, dma, dma, dma, dma, dma, dma((2, parts)), dma, dma((parts,)),
            dma, dma((parts,)), dma((parts,)), dma, dma((n_tp, parts)),
            dma, dma((n_tp, parts)), dma, dma, dma, dma,
        ],
        compiler_params=pltpu.CompilerParams(collective_id=0, has_side_effects=True, vmem_limit_bytes=32 * 1024 * 1024),
        cost_estimate=pl.CostEstimate(flops=2**28, bytes_accessed=8 * 2**20, transcendentals=0),
        name="meet",
    )(pltpu.with_memory_space_constraint(acc, pltpu.HBM), x, wo, bo.reshape(1, width))


def solution(mesh):
    def local_step(hidden, cache_lens, k_cache, v_cache, ln_gain, ln_bias, w_query, b_query, w_kv, b_kv, w_out, b_out):
        key_new, val_new, acc = attend(
            cache_lens, hidden, ln_gain, ln_bias, w_query, b_query, w_kv, b_kv, k_cache, v_cache)
        out_hidden = meet(acc, hidden, w_out, b_out, mesh.shape["sq"], mesh.shape["tp"])
        return out_hidden, key_new, val_new

    cache_spec = P("dp", "sq", None)
    row_spec = P("dp", None)
    in_specs = (row_spec, P("dp"), cache_spec, cache_spec, P(None), P(None), P(None, "tp"), P("tp"), P(None, None), P(None), P("tp", None), P(None))
    out_specs = (row_spec, cache_spec, cache_spec)
    return jax.shard_map(local_step, mesh=mesh, in_specs=in_specs, out_specs=out_specs, check_vma=False)
```

```python
import functools

import jax
import jax.numpy as jnp
from jax import lax
from jax.experimental import pallas as pl
from jax.experimental.pallas import tpu as pltpu
from jax.sharding import PartitionSpec as P

F32 = jnp.float32
BF16 = jnp.bfloat16
NEG = -1e30


def attend_kernel(
    pairs, held, lens_ref, x_hbm, gain_ref, bias_ref, wq_hbm, bq_ref, wkv_hbm, bkv_ref, k_hbm, v_hbm,
    k_out, v_out, acc_out,
    x_buf, h_buf, wq_buf, wkv_buf, q_buf, kv_buf, s_buf, acc_ref, ml_ref, k_buf, v_buf,
    in_sem, k_sem, v_sem, ko_sem, vo_sem, acc_sem, ml_sem,
):
    batch, pos_local, dim = k_buf.shape
    heads = wq_buf.shape[1] // dim
    per = 2 * pairs
    chunks = batch // per
    rows = 2 * heads
    first_pos = lax.axis_index("sq") * pos_local
    scale = dim ** -0.5

    x_copy = pltpu.make_async_copy(x_hbm, x_buf, in_sem.at[0])
    kv_copy = pltpu.make_async_copy(wkv_hbm, wkv_buf, in_sem.at[1])
    q_copy = pltpu.make_async_copy(wq_hbm, wq_buf, in_sem.at[2])
    x_copy.start()
    kv_copy.start()
    q_copy.start()

    def span(ref, c):
        return ref.at[pl.ds(c * per, per)]

    def k_load(c):
        return pltpu.make_async_copy(span(k_hbm, c), span(k_buf, c), k_sem.at[c])

    def v_load(c):
        return pltpu.make_async_copy(span(v_hbm, c), span(v_buf, c), v_sem.at[c])

    def k_store(c):
        return pltpu.make_async_copy(span(k_buf, c), span(k_out, c), ko_sem.at[c])

    def v_store(c):
        return pltpu.make_async_copy(span(v_buf, c), span(v_out, c), vo_sem.at[c])

    @pl.loop(0, chunks)
    def _(c):
        k_load(c).start()
        v_load(c).start(priority=1)

    x_copy.wait()
    block = 32

    @pl.loop(0, batch // block)
    def _(i):
        x = x_buf[pl.ds(i * block, block), :].astype(F32)
        mean = jnp.mean(x, axis=-1, keepdims=True)
        cen = x - mean
        var = jnp.mean(cen * cen, axis=-1, keepdims=True)
        h = cen * lax.rsqrt(var + 1e-5) * gain_ref[...] + bias_ref[...]
        h_buf[pl.ds(i * block, block), :] = h.astype(BF16)

    kv_copy.wait()
    kv = jnp.dot(h_buf[...], wkv_buf[...], preferred_element_type=F32) + bkv_ref[...]
    kv_buf[...] = kv.astype(BF16).astype(F32)
    q_copy.wait()
    for n0 in range(0, heads, 2):
        cols = slice(n0 * dim, (n0 + 2) * dim)
        q = jnp.dot(h_buf[...], wq_buf[:, cols], preferred_element_type=F32) + bq_ref[:, cols]
        q = q.astype(BF16).astype(F32)
        q_buf[pl.ds(n0, batch, stride=heads), :] = q[:, :dim]
        q_buf[pl.ds(n0 + 1, batch, stride=heads), :] = q[:, dim:]

    top = lax.broadcasted_iota(jnp.int32, (rows, dim), 0) < heads
    top2 = lax.broadcasted_iota(jnp.int32, (rows, pos_local), 0) < heads
    lane = lax.broadcasted_iota(jnp.int32, (rows, dim), 1)
    place = first_pos + lax.broadcasted_iota(jnp.int32, (rows, pos_local), 1)
    sub = lax.broadcasted_iota(jnp.int32, (16, dim), 0)

    def update_rows(c):
        fresh = kv_buf[pl.ds(pl.multiple_of(c * per, per), per), :]
        for j in range(per):
            b = c * per + j
            at = lens_ref[b] - first_pos
            base = pl.multiple_of(jnp.clip(at, 0, pos_local - 1) // 16 * 16, 16)
            hit = sub == at - base
            for buf, lo in ((k_buf, 0), (v_buf, dim)):
                new = jnp.broadcast_to(fresh[j:j + 1, lo:lo + dim], (16, dim))
                old = buf[b, pl.ds(base, 16), :].astype(F32)
                buf[b, pl.ds(base, 16), :] = jnp.where(hit, new, old).astype(BF16)

    def score(c):
        out = []
        for j in range(pairs):
            p = c * pairs + j
            q = q_buf[pl.ds(pl.multiple_of(p * rows, rows), rows), :]
            lhs = jnp.concatenate([jnp.where(top, q, 0.0), jnp.where(top, 0.0, q)], axis=1).astype(BF16)
            keys = jnp.concatenate([k_buf[2 * p], k_buf[2 * p + 1]], axis=1)
            s = lax.dot_general(lhs, keys, (((1,), (1,)), ((), ())), preferred_element_type=F32)
            out.append(s)
        return out

    def weigh(c, m_all, l_all):
        for j in range(pairs):
            p = c * pairs + j
            s = s_buf[j * rows:(j + 1) * rows, :] * scale
            last = jnp.where(top2, lens_ref[2 * p], lens_ref[2 * p + 1])
            valid = place <= last
            s = jnp.where(valid, s, NEG)
            m = jnp.max(s, axis=-1, keepdims=True)
            w = jnp.where(valid, jnp.exp(s - m), 0.0)
            total = jnp.sum(w, axis=-1, keepdims=True)
            vals = jnp.concatenate([v_buf[2 * p], v_buf[2 * p + 1]], axis=1)
            o = jnp.dot(w.astype(BF16), vals, preferred_element_type=F32)
            acc_ref[pl.ds(pl.multiple_of(p * rows, rows), rows), :] = jnp.where(top, o[:, :dim], o[:, dim:])
            m_all = jnp.where(lane == p, m, m_all)
            l_all = jnp.where(lane == p, total, l_all)
        return m_all, l_all

    def put_scores(out):
        for j, s in enumerate(out):
            s_buf[j * rows:(j + 1) * rows, :] = s

    def acc_store(c):
        part = pl.ds(pl.multiple_of(c * (pairs * rows), pairs * rows), pairs * rows)
        return pltpu.make_async_copy(acc_ref.at[part], acc_out.at[part], acc_sem.at[c])

    def loaded(c):
        k_load(c).wait()
        v_load(c).wait()

    def leave(c):
        k_store(c).start()
        v_store(c).start(priority=1)

    loaded(0)
    update_rows(0)
    put_scores(score(0))
    zero = jnp.zeros((rows, dim), F32)

    def early(c, carry):
        loaded(c + 1)
        update_rows(c + 1)
        carry = weigh(c, *carry)
        put_scores(score(c + 1))
        acc_store(c).start()
        return carry

    carry = lax.fori_loop(0, held, early, (zero, zero))

    @pl.loop(held + 1, chunks)
    def _(c):
        loaded(c)

    @pl.loop(0, held + 1)
    def _(c):
        leave(c)

    def late(c, carry):
        update_rows(c + 1)
        carry = weigh(c, *carry)
        put_scores(score(c + 1))
        acc_store(c).start()
        leave(c + 1)
        return carry

    carry = lax.fori_loop(held, chunks - 1, late, carry)
    m_all, l_all = weigh(chunks - 1, *carry)
    ml_ref[:rows, :] = m_all
    ml_ref[rows:, :] = l_all
    acc_store(chunks - 1).start()

    @pl.loop(0, chunks - 1)
    def _(c):
        k_store(c).wait()
        v_store(c).wait()
        acc_store(c).wait()

    ml_store = pltpu.make_async_copy(ml_ref, acc_out.at[pl.ds(batch * heads, 2 * rows)], ml_sem)
    ml_store.start()
    k_store(chunks - 1).wait()
    v_store(chunks - 1).wait()
    acc_store(chunks - 1).wait()
    ml_store.wait()


def attend(lens, x, gain, bias, wq, bq, wkv, bkv, k, v, pairs=8, held=6):
    batch, pos_local, dim = k.shape
    width = x.shape[1]
    heads = wq.shape[1] // dim
    chunks = batch // (2 * pairs)
    hbm = pl.BlockSpec(memory_space=pltpu.HBM)
    vmem = pl.BlockSpec(memory_space=pltpu.VMEM)
    dma = pltpu.SemaphoreType.DMA
    return pl.pallas_call(
        functools.partial(attend_kernel, pairs, held),
        out_shape=(
            jax.ShapeDtypeStruct(k.shape, k.dtype),
            jax.ShapeDtypeStruct(v.shape, v.dtype),
            jax.ShapeDtypeStruct((batch * heads + 4 * heads, dim), F32),
        ),
        in_specs=[pl.BlockSpec(memory_space=pltpu.SMEM), hbm, vmem, vmem, hbm, vmem, hbm, vmem, hbm, hbm],
        out_specs=(hbm, hbm, hbm),
        scratch_shapes=[
            pltpu.VMEM(x.shape, BF16),
            pltpu.VMEM(x.shape, BF16),
            pltpu.VMEM(wq.shape, BF16),
            pltpu.VMEM(wkv.shape, BF16),
            pltpu.VMEM((batch * heads, dim), F32),
            pltpu.VMEM((batch, 2 * dim), F32),
            pltpu.VMEM((pairs * 2 * heads, pos_local), F32),
            pltpu.VMEM((batch * heads, dim), F32),
            pltpu.VMEM((4 * heads, dim), F32),
            pltpu.VMEM(k.shape, BF16),
            pltpu.VMEM(v.shape, BF16),
            dma((3,)), dma((chunks,)), dma((chunks,)), dma((chunks,)), dma((chunks,)), dma((chunks,)), dma,
        ],
        compiler_params=pltpu.CompilerParams(vmem_limit_bytes=60 * 1024 * 1024),
        cost_estimate=pl.CostEstimate(flops=2 * 2**30, bytes_accessed=72 * 2**20, transcendentals=0),
        name="attend",
    )(lens, x, gain.reshape(1, width), bias.reshape(1, width), wq, bq.reshape(1, -1), wkv, bkv.reshape(1, -1), k, v)


def meet_kernel(
    n_sq, parts, relayed, acc_hbm, x_hbm, wo_ref, bo_ref, out_ref,
    acc_buf, x_buf, base_buf, pair_buf, ml_pair, up_buf, ml_up, cross_buf, ml_cross, a_buf, z_out, far_in, in_buf, y_buf,
    in_sem, ml_send, ml_recv, mlu_send, mlu_recv, pair_send, pair_recv, up_send, up_recv, z_send, m_recv, s_recv, g_send, g_recv, y_send, y_recv, c_send, c_recv, f_send, f_recv,
):
    n_tp = z_out.shape[1]
    width = y_buf.shape[1]
    dim = acc_buf.shape[1]
    sq, tp = lax.axis_index("sq"), lax.axis_index("tp")
    own = y_buf.shape[0] // n_sq
    step = own // parts
    cols = width // n_tp
    heads = wo_ref.shape[0] // dim
    rows = 2 * heads
    pairs = step // 2
    fold = step * heads
    mesh_id = pl.DeviceIdType.MESH

    def at_tp(d):
        return {"tp": lax.rem(tp + d, n_tp)}

    core_sq = sq + 1 - 2 * lax.rem(sq, 2)
    across_sq = lax.rem(sq + 2, n_sq)
    core, across = {"sq": core_sq}, {"sq": across_sq}

    acc_in = pltpu.make_async_copy(acc_hbm, acc_buf, in_sem.at[0])
    acc_in.start()
    barrier = pltpu.get_barrier_semaphore()
    for to in (core, across):
        pl.semaphore_signal(barrier, inc=1, device_id=to, device_id_type=mesh_id)
    for d in range(1, n_tp):
        pl.semaphore_signal(barrier, inc=1, device_id=at_tp(d), device_id_type=mesh_id)
    x_cols = pl.ds(pl.multiple_of(tp * cols, cols), cols)
    x_in = pltpu.make_async_copy(x_hbm.at[pl.ds(pl.multiple_of(sq * own, own), own), x_cols], x_buf, in_sem.at[1])
    x_in.start()
    ml_own = acc_buf.at[pl.ds(own * n_sq * heads, 2 * rows)]
    with jax.named_scope('barrier'):
        acc_in.wait()
        pl.semaphore_wait(barrier, 2 + n_tp - 1)

    def remote(src, dst, send, recv, to):
        return pltpu.make_async_remote_copy(src_ref=src, dst_ref=dst, send_sem=send, recv_sem=recv, device_id=to, device_id_type=mesh_id)

    def acc_rows(s, c):
        return pl.ds(pl.multiple_of(s * (own * heads) + c * fold, fold), fold)

    def pair_copy(k, c):
        rows_for = acc_rows(core_sq if k == 0 else lax.rem(core_sq + 2, n_sq), c)
        return remote(acc_buf.at[rows_for], pair_buf.at[k, c], pair_send, pair_recv.at[k, c], core)

    def up_copy(c):
        return remote(up_buf.at[c], cross_buf.at[c], up_send, up_recv.at[c], across)

    ml_copy = remote(ml_own, ml_pair, ml_send, ml_recv, core)
    mlu_copy = remote(ml_up, ml_cross, mlu_send, mlu_recv, across)

    half = n_tp // 2
    middle = lax.div(tp + 1, 2) == 1
    partner = tp + 1 - 2 * lax.rem(tp, 2)
    far = half - half * lax.div(tp, half)

    def m_copy(c):
        return remote(z_out.at[c, pl.ds(far, half)], far_in.at[c], z_send, m_recv.at[c], {"tp": partner})

    def n_copy(c):
        return remote(z_out.at[c, partner], in_buf.at[c, 0], z_send, s_recv.at[c], {"tp": partner})

    def s_copy(k, c):
        return remote(z_out.at[c, far + k], in_buf.at[c, 1], z_send, s_recv.at[c], {"tp": far + k})

    def block(s, t, c):
        return y_buf.at[pl.ds(pl.multiple_of(s * own + c * step, step), step), pl.ds(pl.multiple_of(t * cols, cols), cols)]

    def source(tag):
        return tp - tag if tag < n_tp else tp + (tag - n_tp + 1)

    def source_of(tag, c):
        return source(tag) if c < relayed else lax.rem(tp - tag + n_tp, n_tp)

    def tp_copy(t, c, to):
        b = block(sq, t, c)
        return remote(b, b, g_send, g_recv.at[t, c], {"tp": to})

    def y_copy(tag, c):
        t = source_of(tag, c)
        b = block(sq, t, c)
        return remote(b, b, y_send, y_recv.at[t, c], across)

    def c_copy(tag, c):
        b = block(sq, source_of(tag, c), c)
        return remote(b, b, c_send, c_recv, core)

    def f_copy(tag, c):
        b = block(across_sq, source_of(tag, c), c)
        return remote(b, b, f_send, f_recv, core)

    def all_of(ref, send, recv):
        return remote(ref, ref, send, recv, {"tp": tp})

    ml_copy.start()
    for k in (1, 0):
        for c in range(parts):
            pair_copy(k, c).start()

    lane = lax.broadcasted_iota(jnp.int32, (rows, dim), 1)

    def column(e, p):
        return jnp.sum(jnp.where(lane == p, e, 0.0), axis=1, keepdims=True)

    def part_of(j):
        return slice(j * rows, (j + 1) * rows)

    with jax.named_scope("pairwait"):
        ml_copy.wait_recv()
    ml_at = own * n_sq * heads
    m_own, l_own = acc_buf[ml_at:ml_at + rows, :], acc_buf[ml_at + rows:ml_at + 2 * rows, :]
    m_pair, l_pair = ml_pair[:rows, :], ml_pair[rows:, :]
    m_up = jnp.maximum(m_own, m_pair)
    e_own, e_pair = jnp.exp(m_own - m_up), jnp.exp(m_pair - m_up)
    ml_up[:rows, :] = m_up
    ml_up[rows:, :] = e_own * l_own + e_pair * l_pair
    for c in range(parts):
        pair_copy(1, c).wait_recv()
        for j in range(pairs):
            p = across_sq * (own // 2) + c * pairs + j
            mine = pl.multiple_of(across_sq * (own * heads) + c * fold + j * rows, rows)
            up_buf[c, part_of(j), :] = column(e_own, p) * acc_buf[pl.ds(mine, rows), :] + column(e_pair, p) * pair_buf[1, c, part_of(j), :]
        if c == 0:
            mlu_copy.start()
        up_copy(c).start()

    x_in.wait()
    base_buf[...] = x_buf[...].astype(F32) + bo_ref[:, x_cols]
    with jax.named_scope("mlwait"):
        mlu_copy.wait_recv()
    m_cross, l_cross = ml_cross[:rows, :], ml_cross[rows:, :]
    top = jnp.maximum(m_up, m_cross)
    scales = [jnp.exp(m - top) for m in (m_own, m_pair, m_cross)]
    den = scales[0] * l_own + scales[1] * l_pair + scales[2] * l_cross
    scales = [e / den for e in scales]

    def when(cond):
        return pl.when(cond)

    def project(c):
        pair_copy(0, c).wait_recv()
        up_copy(c).wait_recv()
        for j in range(pairs):
            p = sq * (own // 2) + c * pairs + j
            mine = pl.multiple_of(sq * (own * heads) + c * fold + j * rows, rows)
            terms = (acc_buf[pl.ds(mine, rows), :], pair_buf[0, c, part_of(j), :], cross_buf[c, part_of(j), :])
            total = sum(column(e, p) * t for e, t in zip(scales, terms))
            a_buf[j * rows:(j + 1) * rows, :] = total
        lhs = jnp.concatenate([a_buf[pl.ds(n, step, stride=heads), :].astype(BF16) for n in range(heads)], axis=1)
        for t in range(n_tp):
            z_out[c, t] = jnp.dot(lhs, wo_ref[:, t * cols:(t + 1) * cols], preferred_element_type=F32)

        @when(jnp.logical_not(middle))
        def _():
            m_copy(c).start()

        if c:
            n_copy(c - 1).start()
        if c == parts - 1:
            n_copy(c).start()

    def add(c):
        @when(middle)
        def _():
            m_copy(c).wait_recv()
            for k in range(half):
                z_out[c, far + k] = z_out[c, far + k] + far_in[c, k]
            for k in range(half):
                s_copy(k, c).start()

    def share(tag, c):
        y_copy(tag, c).start()
        c_copy(tag, c).start()

    def finish(c):
        all_of(in_buf.at[c], z_send, s_recv.at[c]).wait_recv()
        total = z_out[c, tp] + in_buf[c, 0] + in_buf[c, 1]
        total = total + base_buf[c * step:(c + 1) * step, :]
        mine = block(sq, tp, c)
        mine[...] = total

        if c < relayed:
            @when(tp < n_tp - 1)
            def _():
                tp_copy(tp, c, tp + 1).start()

            @when(tp > 0)
            def _():
                tp_copy(tp, c, tp - 1).start()
        else:
            for d in range(1, n_tp):
                tp_copy(tp, c, lax.rem(tp + d, n_tp)).start()

        share(0, c)

    def direct(d, c):
        tp_copy(source_of(d, c), c, tp).wait_recv()
        share(d, c)

    def hop(h, c):
        @when(tp >= h)
        def _():
            tp_copy(tp - h, c, tp).wait_recv()

            @when(tp < n_tp - 1)
            def _():
                tp_copy(tp - h, c, tp + 1).start()

            share(h, c)

        @when(tp + h < n_tp)
        def _():
            tp_copy(tp + h, c, tp).wait_recv()

            @when(tp > 0)
            def _():
                tp_copy(tp + h, c, tp - 1).start()

            share(h + n_tp - 1, c)

    def crossed(h, c):
        def take(tag):
            y_copy(tag, c).wait_recv()
            f_copy(tag, c).start()

        if h == 0 or c >= relayed:
            take(h)
            return

        @when(tp >= h)
        def _():
            take(h)

        @when(tp + h < n_tp)
        def _():
            take(h + n_tp - 1)

    def named(name, fn, *args):
        def run():
            with jax.named_scope(name):
                fn(*args)
        return run

    events = []
    for c in range(parts):
        events.append((6.3 + 3.0 / parts * c, 0, named(f"p{c}", project, c)))
        events.append((8.1 + 8.4 / parts * (c + 1), 0, named(f"a{c}", add, c)))
        t = 11.7 + 8.4 / parts * (c + 1)
        events.append((t, 1, named(f"f{c}", finish, c)))
        events.append((t + 4.0, 3, named(f"y{c}_0", crossed, 0, c)))
        for h in range(1, n_tp):
            if c < relayed:
                there = t + 3.6 * h - 0.7
                events.append((there, 2, named(f"h{c}_{h}", hop, h, c)))
            else:
                there = t + 3.2 + 0.8 * h
                events.append((there, 2, named(f"d{c}_{h}", direct, h, c)))
            events.append((there + 5.0, 3, named(f"y{c}_{h}", crossed, h, c)))
    for _, _, event in sorted(events, key=lambda e: e[:2]):
        event()

    whole = y_buf.at[pl.ds(0, own)]
    with jax.named_scope("close"):
        all_of(whole, c_send, c_recv).wait()
        all_of(whole, f_send, f_recv).wait()
        all_of(whole, y_send, f_recv).wait_send()
        ml_copy.wait_send()
        mlu_copy.wait_send()
        all_of(pair_buf, pair_send, ml_recv).wait_send()
        all_of(up_buf, up_send, ml_recv).wait_send()
        all_of(z_out.at[:, pl.ds(0, half + 1)], z_send, ml_recv).wait_send()
        straight = (parts - relayed) * (n_tp - 1)

        @when(middle)
        def _():
            blocks = y_buf.at[pl.ds(0, (straight + relayed * (n_tp + 1)) * step // n_tp)]
            all_of(blocks, g_send, ml_recv).wait_send()

        @when(jnp.logical_not(middle))
        def _():
            blocks = y_buf.at[pl.ds(0, (straight + relayed) * step // n_tp)]
            all_of(blocks, g_send, ml_recv).wait_send()

    chunk = 32
    for i in range(y_buf.shape[0] // chunk):
      with jax.named_scope(f'emit{i}'):
        out_ref[i * chunk:(i + 1) * chunk, :] = y_buf[i * chunk:(i + 1) * chunk, :].astype(BF16)


def meet(acc, x, wo, bo, n_sq, n_tp, parts=4, relayed=0):
    batch, width = x.shape
    own = batch // n_sq
    cols = width // n_tp
    step = own // parts
    heads = wo.shape[0] // acc.shape[1]
    dim = acc.shape[1]
    vmem = pl.BlockSpec(memory_space=pltpu.VMEM)
    hbm = pl.BlockSpec(memory_space=pltpu.HBM)
    dma = pltpu.SemaphoreType.DMA
    return pl.pallas_call(
        functools.partial(meet_kernel, n_sq, parts, relayed),
        out_shape=jax.ShapeDtypeStruct((batch, width), BF16),
        in_specs=[hbm, hbm, vmem, vmem],
        out_specs=vmem,
        scratch_shapes=[
            pltpu.VMEM(acc.shape, F32),
            pltpu.VMEM((own, cols), BF16),
            pltpu.VMEM((own, cols), F32),
            pltpu.VMEM((2, parts, step * heads, dim), F32),
            pltpu.VMEM((4 * heads, dim), F32),
            pltpu.VMEM((parts, step * heads, dim), F32),
            pltpu.VMEM((4 * heads, dim), F32),
            pltpu.VMEM((parts, step * heads, dim), F32),
            pltpu.VMEM((4 * heads, dim), F32),
            pltpu.VMEM((step * heads, dim), F32),
            pltpu.VMEM((parts, n_tp, step, cols), F32),
            pltpu.VMEM((parts, n_tp // 2, step, cols), F32),
            pltpu.VMEM((parts, 2, step, cols), F32),
            pltpu.VMEM((batch, width), F32),
            dma((2,)), dma, dma, dma, dma, dma, dma((2, parts)), dma, dma((parts,)),
            dma, dma((parts,)), dma((parts,)), dma, dma((n_tp, parts)),
            dma, dma((n_tp, parts)), dma, dma, dma, dma,
        ],
        compiler_params=pltpu.CompilerParams(collective_id=0, has_side_effects=True, vmem_limit_bytes=32 * 1024 * 1024),
        cost_estimate=pl.CostEstimate(flops=2**28, bytes_accessed=8 * 2**20, transcendentals=0),
        name="meet",
    )(pltpu.with_memory_space_constraint(acc, pltpu.HBM), pltpu.with_memory_space_constraint(x, pltpu.HBM), wo, bo.reshape(1, width))


def solution(mesh):
    def local_step(hidden, cache_lens, k_cache, v_cache, ln_gain, ln_bias, w_query, b_query, w_kv, b_kv, w_out, b_out):
        key_new, val_new, acc = attend(
            cache_lens, hidden, ln_gain, ln_bias, w_query, b_query, w_kv, b_kv, k_cache, v_cache)
        out_hidden = meet(acc, hidden, w_out, b_out, mesh.shape["sq"], mesh.shape["tp"])
        return out_hidden, key_new, val_new

    cache_spec = P("dp", "sq", None)
    row_spec = P("dp", None)
    in_specs = (row_spec, P("dp"), cache_spec, cache_spec, P(None), P(None), P(None, "tp"), P("tp"), P(None, None), P(None), P("tp", None), P(None))
    out_specs = (row_spec, cache_spec, cache_spec)
    return jax.shard_map(local_step, mesh=mesh, in_specs=in_specs, out_specs=out_specs, check_vma=False)
```

```python
import functools

import jax
import jax.numpy as jnp
from jax import lax
from jax.experimental import pallas as pl
from jax.experimental.pallas import tpu as pltpu
from jax.sharding import PartitionSpec as P

F32 = jnp.float32
BF16 = jnp.bfloat16
NEG = -1e30


def attend_kernel(
    pairs, held, lens_ref, x_hbm, gain_ref, bias_ref, wq_hbm, bq_ref, wkv_hbm, bkv_ref, k_hbm, v_hbm,
    k_out, v_out, acc_out,
    x_buf, h_buf, wq_buf, wkv_buf, q_buf, kv_buf, s_buf, acc_ref, ml_ref, k_buf, v_buf,
    in_sem, k_sem, v_sem, ko_sem, vo_sem, acc_sem, ml_sem,
):
    batch, pos_local, dim = k_buf.shape
    heads = wq_buf.shape[1] // dim
    per = 2 * pairs
    chunks = batch // per
    rows = 2 * heads
    first_pos = lax.axis_index("sq") * pos_local
    scale = dim ** -0.5

    x_copy = pltpu.make_async_copy(x_hbm, x_buf, in_sem.at[0])
    kv_copy = pltpu.make_async_copy(wkv_hbm, wkv_buf, in_sem.at[1])
    q_copy = pltpu.make_async_copy(wq_hbm, wq_buf, in_sem.at[2])
    x_copy.start()
    kv_copy.start()
    q_copy.start()

    def span(ref, c):
        return ref.at[pl.ds(c * per, per)]

    def k_load(c):
        return pltpu.make_async_copy(span(k_hbm, c), span(k_buf, c), k_sem.at[c])

    def v_load(c):
        return pltpu.make_async_copy(span(v_hbm, c), span(v_buf, c), v_sem.at[c])

    def k_store(c):
        return pltpu.make_async_copy(span(k_buf, c), span(k_out, c), ko_sem.at[c])

    def v_store(c):
        return pltpu.make_async_copy(span(v_buf, c), span(v_out, c), vo_sem.at[c])

    @pl.loop(0, chunks)
    def _(c):
        k_load(c).start()
        v_load(c).start(priority=1)

    x_copy.wait()
    block = 32

    @pl.loop(0, batch // block)
    def _(i):
        x = x_buf[pl.ds(i * block, block), :].astype(F32)
        mean = jnp.mean(x, axis=-1, keepdims=True)
        cen = x - mean
        var = jnp.mean(cen * cen, axis=-1, keepdims=True)
        h = cen * lax.rsqrt(var + 1e-5) * gain_ref[...] + bias_ref[...]
        h_buf[pl.ds(i * block, block), :] = h.astype(BF16)

    kv_copy.wait()
    kv = jnp.dot(h_buf[...], wkv_buf[...], preferred_element_type=F32) + bkv_ref[...]
    kv_buf[...] = kv.astype(BF16).astype(F32)
    q_copy.wait()
    for n0 in range(0, heads, 2):
        cols = slice(n0 * dim, (n0 + 2) * dim)
        q = jnp.dot(h_buf[...], wq_buf[:, cols], preferred_element_type=F32) + bq_ref[:, cols]
        q = q.astype(BF16).astype(F32)
        q_buf[pl.ds(n0, batch, stride=heads), :] = q[:, :dim]
        q_buf[pl.ds(n0 + 1, batch, stride=heads), :] = q[:, dim:]

    top = lax.broadcasted_iota(jnp.int32, (rows, dim), 0) < heads
    top2 = lax.broadcasted_iota(jnp.int32, (rows, pos_local), 0) < heads
    lane = lax.broadcasted_iota(jnp.int32, (rows, dim), 1)
    place = first_pos + lax.broadcasted_iota(jnp.int32, (rows, pos_local), 1)
    sub = lax.broadcasted_iota(jnp.int32, (16, dim), 0)

    def update_rows(c):
        fresh = kv_buf[pl.ds(pl.multiple_of(c * per, per), per), :]
        for j in range(per):
            b = c * per + j
            at = lens_ref[b] - first_pos
            base = pl.multiple_of(jnp.clip(at, 0, pos_local - 1) // 16 * 16, 16)
            hit = sub == at - base
            for buf, lo in ((k_buf, 0), (v_buf, dim)):
                new = jnp.broadcast_to(fresh[j:j + 1, lo:lo + dim], (16, dim))
                old = buf[b, pl.ds(base, 16), :].astype(F32)
                buf[b, pl.ds(base, 16), :] = jnp.where(hit, new, old).astype(BF16)

    def score(c):
        out = []
        for j in range(pairs):
            p = c * pairs + j
            q = q_buf[pl.ds(pl.multiple_of(p * rows, rows), rows), :]
            lhs = jnp.concatenate([jnp.where(top, q, 0.0), jnp.where(top, 0.0, q)], axis=1).astype(BF16)
            keys = jnp.concatenate([k_buf[2 * p], k_buf[2 * p + 1]], axis=1)
            s = lax.dot_general(lhs, keys, (((1,), (1,)), ((), ())), preferred_element_type=F32)
            out.append(s)
        return out

    def weigh(c, m_all, l_all):
        for j in range(pairs):
            p = c * pairs + j
            s = s_buf[j * rows:(j + 1) * rows, :] * scale
            last = jnp.where(top2, lens_ref[2 * p], lens_ref[2 * p + 1])
            valid = place <= last
            s = jnp.where(valid, s, NEG)
            m = jnp.max(s, axis=-1, keepdims=True)
            w = jnp.where(valid, jnp.exp(s - m), 0.0)
            total = jnp.sum(w, axis=-1, keepdims=True)
            vals = jnp.concatenate([v_buf[2 * p], v_buf[2 * p + 1]], axis=1)
            o = jnp.dot(w.astype(BF16), vals, preferred_element_type=F32)
            acc_ref[pl.ds(pl.multiple_of(p * rows, rows), rows), :] = jnp.where(top, o[:, :dim], o[:, dim:])
            m_all = jnp.where(lane == p, m, m_all)
            l_all = jnp.where(lane == p, total, l_all)
        return m_all, l_all

    def put_scores(out):
        for j, s in enumerate(out):
            s_buf[j * rows:(j + 1) * rows, :] = s

    def acc_store(c):
        part = pl.ds(pl.multiple_of(c * (pairs * rows), pairs * rows), pairs * rows)
        return pltpu.make_async_copy(acc_ref.at[part], acc_out.at[part], acc_sem.at[c])

    def loaded(c):
        k_load(c).wait()
        v_load(c).wait()

    def leave(c):
        k_store(c).start()
        v_store(c).start(priority=1)

    loaded(0)
    update_rows(0)
    put_scores(score(0))
    zero = jnp.zeros((rows, dim), F32)

    def early(c, carry):
        loaded(c + 1)
        update_rows(c + 1)
        carry = weigh(c, *carry)
        put_scores(score(c + 1))
        acc_store(c).start()
        return carry

    carry = lax.fori_loop(0, held, early, (zero, zero))

    @pl.loop(held + 1, chunks)
    def _(c):
        loaded(c)

    @pl.loop(0, held + 1)
    def _(c):
        leave(c)

    def late(c, carry):
        update_rows(c + 1)
        carry = weigh(c, *carry)
        put_scores(score(c + 1))
        acc_store(c).start()
        leave(c + 1)
        return carry

    carry = lax.fori_loop(held, chunks - 1, late, carry)
    m_all, l_all = weigh(chunks - 1, *carry)
    ml_ref[:rows, :] = m_all
    ml_ref[rows:, :] = l_all
    acc_store(chunks - 1).start()

    @pl.loop(0, chunks - 1)
    def _(c):
        k_store(c).wait()
        v_store(c).wait()
        acc_store(c).wait()

    ml_store = pltpu.make_async_copy(ml_ref, acc_out.at[pl.ds(batch * heads, 2 * rows)], ml_sem)
    ml_store.start()
    k_store(chunks - 1).wait()
    v_store(chunks - 1).wait()
    acc_store(chunks - 1).wait()
    ml_store.wait()


def attend(lens, x, gain, bias, wq, bq, wkv, bkv, k, v, pairs=8, held=6):
    batch, pos_local, dim = k.shape
    width = x.shape[1]
    heads = wq.shape[1] // dim
    chunks = batch // (2 * pairs)
    hbm = pl.BlockSpec(memory_space=pltpu.HBM)
    vmem = pl.BlockSpec(memory_space=pltpu.VMEM)
    dma = pltpu.SemaphoreType.DMA
    return pl.pallas_call(
        functools.partial(attend_kernel, pairs, held),
        out_shape=(
            jax.ShapeDtypeStruct(k.shape, k.dtype),
            jax.ShapeDtypeStruct(v.shape, v.dtype),
            jax.ShapeDtypeStruct((batch * heads + 4 * heads, dim), F32),
        ),
        in_specs=[pl.BlockSpec(memory_space=pltpu.SMEM), hbm, vmem, vmem, hbm, vmem, hbm, vmem, hbm, hbm],
        out_specs=(hbm, hbm, hbm),
        scratch_shapes=[
            pltpu.VMEM(x.shape, BF16),
            pltpu.VMEM(x.shape, BF16),
            pltpu.VMEM(wq.shape, BF16),
            pltpu.VMEM(wkv.shape, BF16),
            pltpu.VMEM((batch * heads, dim), F32),
            pltpu.VMEM((batch, 2 * dim), F32),
            pltpu.VMEM((pairs * 2 * heads, pos_local), F32),
            pltpu.VMEM((batch * heads, dim), F32),
            pltpu.VMEM((4 * heads, dim), F32),
            pltpu.VMEM(k.shape, BF16),
            pltpu.VMEM(v.shape, BF16),
            dma((3,)), dma((chunks,)), dma((chunks,)), dma((chunks,)), dma((chunks,)), dma((chunks,)), dma,
        ],
        compiler_params=pltpu.CompilerParams(vmem_limit_bytes=60 * 1024 * 1024),
        cost_estimate=pl.CostEstimate(flops=2 * 2**30, bytes_accessed=72 * 2**20, transcendentals=0),
        name="attend",
    )(lens, x, gain.reshape(1, width), bias.reshape(1, width), wq, bq.reshape(1, -1), wkv, bkv.reshape(1, -1), k, v)


def meet_kernel(
    n_sq, parts, relayed, acc_hbm, x_hbm, wo_ref, bo_ref, out_ref,
    acc_buf, x_buf, base_buf, pair_buf, ml_pair, up_buf, ml_up, cross_buf, ml_cross, a_buf, z_out, far_in, in_buf, y_buf,
    in_sem, ml_send, ml_recv, mlu_send, mlu_recv, pair_send, pair_recv, up_send, up_recv, z_send, m_recv, s_recv, g_send, g_recv, y_send, y_recv, c_send, c_recv, f_send, f_recv,
):
    n_tp = z_out.shape[1]
    width = y_buf.shape[1]
    dim = acc_buf.shape[1]
    sq, tp = lax.axis_index("sq"), lax.axis_index("tp")
    own = y_buf.shape[0] // n_sq
    step = own // parts
    cols = width // n_tp
    heads = wo_ref.shape[0] // dim
    rows = 2 * heads
    pairs = step // 2
    fold = step * heads
    mesh_id = pl.DeviceIdType.MESH

    def at_tp(d):
        return {"tp": lax.rem(tp + d, n_tp)}

    core_sq = sq + 1 - 2 * lax.rem(sq, 2)
    across_sq = lax.rem(sq + 2, n_sq)
    core, across = {"sq": core_sq}, {"sq": across_sq}

    acc_in = pltpu.make_async_copy(acc_hbm, acc_buf, in_sem.at[0])
    acc_in.start()
    barrier = pltpu.get_barrier_semaphore()
    for to in (core, across):
        pl.semaphore_signal(barrier, inc=1, device_id=to, device_id_type=mesh_id)
    for d in range(1, n_tp):
        pl.semaphore_signal(barrier, inc=1, device_id=at_tp(d), device_id_type=mesh_id)
    x_cols = pl.ds(pl.multiple_of(tp * cols, cols), cols)
    x_in = pltpu.make_async_copy(x_hbm.at[pl.ds(pl.multiple_of(sq * own, own), own), x_cols], x_buf, in_sem.at[1])
    x_in.start()
    ml_own = acc_buf.at[pl.ds(own * n_sq * heads, 2 * rows)]
    with jax.named_scope('barrier'):
        acc_in.wait()
        pl.semaphore_wait(barrier, 2 + n_tp - 1)

    def remote(src, dst, send, recv, to):
        return pltpu.make_async_remote_copy(src_ref=src, dst_ref=dst, send_sem=send, recv_sem=recv, device_id=to, device_id_type=mesh_id)

    def acc_rows(s, c):
        return pl.ds(pl.multiple_of(s * (own * heads) + c * fold, fold), fold)

    def pair_copy(k, c):
        rows_for = acc_rows(core_sq if k == 0 else lax.rem(core_sq + 2, n_sq), c)
        return remote(acc_buf.at[rows_for], pair_buf.at[k, c], pair_send, pair_recv.at[k, c], core)

    def up_copy(c):
        return remote(up_buf.at[c], cross_buf.at[c], up_send, up_recv.at[c], across)

    ml_copy = remote(ml_own, ml_pair, ml_send, ml_recv, core)
    mlu_copy = remote(ml_up, ml_cross, mlu_send, mlu_recv, across)

    half = n_tp // 2
    middle = lax.div(tp + 1, 2) == 1
    partner = tp + 1 - 2 * lax.rem(tp, 2)
    far = half - half * lax.div(tp, half)

    def m_copy(c):
        return remote(z_out.at[c, pl.ds(far, half)], far_in.at[c], z_send, m_recv.at[c], {"tp": partner})

    def n_copy(c):
        return remote(z_out.at[c, partner], in_buf.at[c, 0], z_send, s_recv.at[c], {"tp": partner})

    def s_copy(k, c):
        return remote(z_out.at[c, far + k], in_buf.at[c, 1], z_send, s_recv.at[c], {"tp": far + k})

    def block(s, t, c):
        return y_buf.at[pl.ds(pl.multiple_of(s * own + c * step, step), step), pl.ds(pl.multiple_of(t * cols, cols), cols)]

    def source(tag):
        return tp - tag if tag < n_tp else tp + (tag - n_tp + 1)

    def source_of(tag, c):
        return source(tag) if c < relayed else lax.rem(tp - tag + n_tp, n_tp)

    def tp_copy(t, c, to):
        b = block(sq, t, c)
        return remote(b, b, g_send, g_recv.at[t, c], {"tp": to})

    def y_copy(tag, c):
        t = source_of(tag, c)
        b = block(sq, t, c)
        return remote(b, b, y_send, y_recv.at[t, c], across)

    def c_copy(tag, c):
        b = block(sq, source_of(tag, c), c)
        return remote(b, b, c_send, c_recv, core)

    def f_copy(tag, c):
        b = block(across_sq, source_of(tag, c), c)
        return remote(b, b, f_send, f_recv, core)

    def all_of(ref, send, recv):
        return remote(ref, ref, send, recv, {"tp": tp})

    ml_copy.start()
    for k in (1, 0):
        for c in range(parts):
            pair_copy(k, c).start()

    lane = lax.broadcasted_iota(jnp.int32, (rows, dim), 1)

    def column(e, p):
        return jnp.sum(jnp.where(lane == p, e, 0.0), axis=1, keepdims=True)

    def part_of(j):
        return slice(j * rows, (j + 1) * rows)

    with jax.named_scope("pairwait"):
        ml_copy.wait_recv()
    ml_at = own * n_sq * heads
    m_own, l_own = acc_buf[ml_at:ml_at + rows, :], acc_buf[ml_at + rows:ml_at + 2 * rows, :]
    m_pair, l_pair = ml_pair[:rows, :], ml_pair[rows:, :]
    m_up = jnp.maximum(m_own, m_pair)
    e_own, e_pair = jnp.exp(m_own - m_up), jnp.exp(m_pair - m_up)
    ml_up[:rows, :] = m_up
    ml_up[rows:, :] = e_own * l_own + e_pair * l_pair
    for c in range(parts):
        pair_copy(1, c).wait_recv()
        for j in range(pairs):
            p = across_sq * (own // 2) + c * pairs + j
            mine = pl.multiple_of(across_sq * (own * heads) + c * fold + j * rows, rows)
            up_buf[c, part_of(j), :] = column(e_own, p) * acc_buf[pl.ds(mine, rows), :] + column(e_pair, p) * pair_buf[1, c, part_of(j), :]
        if c == 0:
            mlu_copy.start()
        up_copy(c).start()

    x_in.wait()
    base_buf[...] = x_buf[...].astype(F32) + bo_ref[:, x_cols]
    with jax.named_scope("mlwait"):
        mlu_copy.wait_recv()
    m_cross, l_cross = ml_cross[:rows, :], ml_cross[rows:, :]
    top = jnp.maximum(m_up, m_cross)
    scales = [jnp.exp(m - top) for m in (m_own, m_pair, m_cross)]
    den = scales[0] * l_own + scales[1] * l_pair + scales[2] * l_cross
    scales = [e / den for e in scales]

    def when(cond):
        return pl.when(cond)

    def project(c):
        pair_copy(0, c).wait_recv()
        up_copy(c).wait_recv()
        for j in range(pairs):
            p = sq * (own // 2) + c * pairs + j
            mine = pl.multiple_of(sq * (own * heads) + c * fold + j * rows, rows)
            terms = (acc_buf[pl.ds(mine, rows), :], pair_buf[0, c, part_of(j), :], cross_buf[c, part_of(j), :])
            total = sum(column(e, p) * t for e, t in zip(scales, terms))
            a_buf[j * rows:(j + 1) * rows, :] = total
        lhs = jnp.concatenate([a_buf[pl.ds(n, step, stride=heads), :].astype(BF16) for n in range(heads)], axis=1)
        for t in range(n_tp):
            z_out[c, t] = jnp.dot(lhs, wo_ref[:, t * cols:(t + 1) * cols], preferred_element_type=F32)

        @when(jnp.logical_not(middle))
        def _():
            m_copy(c).start()

        if c:
            n_copy(c - 1).start()
        if c == parts - 1:
            n_copy(c).start()

    def add(c):
        @when(middle)
        def _():
            m_copy(c).wait_recv()
            for k in range(half):
                z_out[c, far + k] = z_out[c, far + k] + far_in[c, k]
            for k in range(half):
                s_copy(k, c).start()

    def share(tag, c):
        y_copy(tag, c).start()
        c_copy(tag, c).start()

    def finish(c):
        all_of(in_buf.at[c], z_send, s_recv.at[c]).wait_recv()
        total = z_out[c, tp] + in_buf[c, 0] + in_buf[c, 1]
        total = total + base_buf[c * step:(c + 1) * step, :]
        mine = block(sq, tp, c)
        mine[...] = total

        if c < relayed:
            @when(tp < n_tp - 1)
            def _():
                tp_copy(tp, c, tp + 1).start()

            @when(tp > 0)
            def _():
                tp_copy(tp, c, tp - 1).start()
        else:
            for d in range(1, n_tp):
                tp_copy(tp, c, lax.rem(tp + d, n_tp)).start()

        share(0, c)

    def direct(d, c):
        tp_copy(source_of(d, c), c, tp).wait_recv()
        share(d, c)

    stages = {
        "e1": (1, tp < half, tp >= half),
        "e2": (2, tp == 0, tp == n_tp - 1),
        "l1": (1, tp == half, tp == half - 1),
        "l2": (2, tp == half - 1, tp == half),
        "l3": (3, tp == 0, tp == n_tp - 1),
    }

    def hop(stage, c):
        h, on_right, on_left = stages[stage]

        @when(on_right)
        def _():
            tp_copy(tp + h, c, tp).wait_recv()

            @when(tp > 0)
            def _():
                tp_copy(tp + h, c, tp - 1).start()

            share(h + n_tp - 1, c)

        @when(on_left)
        def _():
            tp_copy(tp - h, c, tp).wait_recv()

            @when(tp < n_tp - 1)
            def _():
                tp_copy(tp - h, c, tp + 1).start()

            share(h, c)

    def take(tag, c):
        y_copy(tag, c).wait_recv()
        f_copy(tag, c).start()

    def crossed(stage, c):
        h, on_right, on_left = stages[stage]

        @when(on_right)
        def _():
            take(h + n_tp - 1, c)

        @when(on_left)
        def _():
            take(h, c)

    def named(name, fn, *args):
        def run():
            with jax.named_scope(name):
                fn(*args)
        return run

    events = []
    for c in range(parts):
        events.append((6.3 + 3.0 / parts * c, 0, named(f"p{c}", project, c)))
        events.append((8.1 + 8.4 / parts * (c + 1), 0, named(f"a{c}", add, c)))
        t = 11.7 + 8.4 / parts * (c + 1)
        events.append((t, 1, named(f"f{c}", finish, c)))
        events.append((t + 4.0, 3, named(f"y{c}_0", take, 0, c)))
        if c < relayed:
            first = max(t, 17.4) + 2.1 + 0.7 * c
            ways = {"e1": t + 2.6, "e2": t + 5.2, "l1": first, "l2": first + 2.6, "l3": first + 5.2}
            for stage, there in ways.items():
                events.append((there, 2, named(f"h{c}_{stage}", hop, stage, c)))
                events.append((there + 4.5, 3, named(f"y{c}_{stage}", crossed, stage, c)))
        else:
            for h in range(1, n_tp):
                there = t + 3.2 + 0.8 * h
                events.append((there, 2, named(f"d{c}_{h}", direct, h, c)))
                events.append((there + 4.5, 3, named(f"y{c}_{h}", take, h, c)))
    for _, _, event in sorted(events, key=lambda e: e[:2]):
        event()

    whole = y_buf.at[pl.ds(0, own)]
    with jax.named_scope("close"):
        all_of(whole, c_send, c_recv).wait()
        all_of(whole, f_send, f_recv).wait()
        all_of(whole, y_send, f_recv).wait_send()
        ml_copy.wait_send()
        mlu_copy.wait_send()
        all_of(pair_buf, pair_send, ml_recv).wait_send()
        all_of(up_buf, up_send, ml_recv).wait_send()
        all_of(z_out.at[:, pl.ds(0, half + 1)], z_send, ml_recv).wait_send()
        straight = (parts - relayed) * (n_tp - 1)

        @when(middle)
        def _():
            blocks = y_buf.at[pl.ds(0, (straight + relayed * (n_tp + 1)) * step // n_tp)]
            all_of(blocks, g_send, ml_recv).wait_send()

        @when(jnp.logical_not(middle))
        def _():
            blocks = y_buf.at[pl.ds(0, (straight + relayed) * step // n_tp)]
            all_of(blocks, g_send, ml_recv).wait_send()

    chunk = 32
    for i in range(y_buf.shape[0] // chunk):
      with jax.named_scope(f'emit{i}'):
        out_ref[i * chunk:(i + 1) * chunk, :] = y_buf[i * chunk:(i + 1) * chunk, :].astype(BF16)


def meet(acc, x, wo, bo, n_sq, n_tp, parts=4, relayed=2):
    batch, width = x.shape
    own = batch // n_sq
    cols = width // n_tp
    step = own // parts
    heads = wo.shape[0] // acc.shape[1]
    dim = acc.shape[1]
    vmem = pl.BlockSpec(memory_space=pltpu.VMEM)
    hbm = pl.BlockSpec(memory_space=pltpu.HBM)
    dma = pltpu.SemaphoreType.DMA
    return pl.pallas_call(
        functools.partial(meet_kernel, n_sq, parts, relayed),
        out_shape=jax.ShapeDtypeStruct((batch, width), BF16),
        in_specs=[hbm, hbm, vmem, vmem],
        out_specs=vmem,
        scratch_shapes=[
            pltpu.VMEM(acc.shape, F32),
            pltpu.VMEM((own, cols), BF16),
            pltpu.VMEM((own, cols), F32),
            pltpu.VMEM((2, parts, step * heads, dim), F32),
            pltpu.VMEM((4 * heads, dim), F32),
            pltpu.VMEM((parts, step * heads, dim), F32),
            pltpu.VMEM((4 * heads, dim), F32),
            pltpu.VMEM((parts, step * heads, dim), F32),
            pltpu.VMEM((4 * heads, dim), F32),
            pltpu.VMEM((step * heads, dim), F32),
            pltpu.VMEM((parts, n_tp, step, cols), F32),
            pltpu.VMEM((parts, n_tp // 2, step, cols), F32),
            pltpu.VMEM((parts, 2, step, cols), F32),
            pltpu.VMEM((batch, width), F32),
            dma((2,)), dma, dma, dma, dma, dma, dma((2, parts)), dma, dma((parts,)),
            dma, dma((parts,)), dma((parts,)), dma, dma((n_tp, parts)),
            dma, dma((n_tp, parts)), dma, dma, dma, dma,
        ],
        compiler_params=pltpu.CompilerParams(collective_id=0, has_side_effects=True, vmem_limit_bytes=32 * 1024 * 1024),
        cost_estimate=pl.CostEstimate(flops=2**28, bytes_accessed=8 * 2**20, transcendentals=0),
        name="meet",
    )(pltpu.with_memory_space_constraint(acc, pltpu.HBM), pltpu.with_memory_space_constraint(x, pltpu.HBM), wo, bo.reshape(1, width))


def solution(mesh):
    def local_step(hidden, cache_lens, k_cache, v_cache, ln_gain, ln_bias, w_query, b_query, w_kv, b_kv, w_out, b_out):
        key_new, val_new, acc = attend(
            cache_lens, hidden, ln_gain, ln_bias, w_query, b_query, w_kv, b_kv, k_cache, v_cache)
        out_hidden = meet(acc, hidden, w_out, b_out, mesh.shape["sq"], mesh.shape["tp"])
        return out_hidden, key_new, val_new

    cache_spec = P("dp", "sq", None)
    row_spec = P("dp", None)
    in_specs = (row_spec, P("dp"), cache_spec, cache_spec, P(None), P(None), P(None, "tp"), P("tp"), P(None, None), P(None), P("tp", None), P(None))
    out_specs = (row_spec, cache_spec, cache_spec)
    return jax.shard_map(local_step, mesh=mesh, in_specs=in_specs, out_specs=out_specs, check_vma=False)
```

```python
import functools

import jax
import jax.numpy as jnp
from jax import lax
from jax.experimental import pallas as pl
from jax.experimental.pallas import tpu as pltpu
from jax.sharding import PartitionSpec as P

F32 = jnp.float32
BF16 = jnp.bfloat16
NEG = -1e30


def attend_kernel(
    pairs, held, lens_ref, x_hbm, gain_ref, bias_ref, wq_hbm, bq_ref, wkv_hbm, bkv_ref, k_hbm, v_hbm,
    k_out, v_out, acc_out,
    x_buf, h_buf, wq_buf, wkv_buf, q_buf, kv_buf, s_buf, acc_ref, ml_ref, k_buf, v_buf,
    in_sem, k_sem, v_sem, ko_sem, vo_sem, acc_sem, ml_sem,
):
    batch, pos_local, dim = k_buf.shape
    heads = wq_buf.shape[1] // dim
    per = 2 * pairs
    chunks = batch // per
    rows = 2 * heads
    first_pos = lax.axis_index("sq") * pos_local
    scale = dim ** -0.5

    x_copy = pltpu.make_async_copy(x_hbm, x_buf, in_sem.at[0])
    kv_copy = pltpu.make_async_copy(wkv_hbm, wkv_buf, in_sem.at[1])
    q_copy = pltpu.make_async_copy(wq_hbm, wq_buf, in_sem.at[2])
    x_copy.start()
    kv_copy.start()
    q_copy.start()

    def span(ref, c):
        return ref.at[pl.ds(c * per, per)]

    def k_load(c):
        return pltpu.make_async_copy(span(k_hbm, c), span(k_buf, c), k_sem.at[c])

    def v_load(c):
        return pltpu.make_async_copy(span(v_hbm, c), span(v_buf, c), v_sem.at[c])

    def k_store(c):
        return pltpu.make_async_copy(span(k_buf, c), span(k_out, c), ko_sem.at[c])

    def v_store(c):
        return pltpu.make_async_copy(span(v_buf, c), span(v_out, c), vo_sem.at[c])

    @pl.loop(0, chunks)
    def _(c):
        k_load(c).start()
        v_load(c).start(priority=1)

    x_copy.wait()
    block = 32

    @pl.loop(0, batch // block)
    def _(i):
        x = x_buf[pl.ds(i * block, block), :].astype(F32)
        mean = jnp.mean(x, axis=-1, keepdims=True)
        cen = x - mean
        var = jnp.mean(cen * cen, axis=-1, keepdims=True)
        h = cen * lax.rsqrt(var + 1e-5) * gain_ref[...] + bias_ref[...]
        h_buf[pl.ds(i * block, block), :] = h.astype(BF16)

    kv_copy.wait()
    kv = jnp.dot(h_buf[...], wkv_buf[...], preferred_element_type=F32) + bkv_ref[...]
    kv_buf[...] = kv.astype(BF16).astype(F32)
    q_copy.wait()
    for n0 in range(0, heads, 2):
        cols = slice(n0 * dim, (n0 + 2) * dim)
        q = jnp.dot(h_buf[...], wq_buf[:, cols], preferred_element_type=F32) + bq_ref[:, cols]
        q = q.astype(BF16).astype(F32)
        q_buf[pl.ds(n0, batch, stride=heads), :] = q[:, :dim]
        q_buf[pl.ds(n0 + 1, batch, stride=heads), :] = q[:, dim:]

    top = lax.broadcasted_iota(jnp.int32, (rows, dim), 0) < heads
    top2 = lax.broadcasted_iota(jnp.int32, (rows, pos_local), 0) < heads
    lane = lax.broadcasted_iota(jnp.int32, (rows, dim), 1)
    place = first_pos + lax.broadcasted_iota(jnp.int32, (rows, pos_local), 1)
    sub = lax.broadcasted_iota(jnp.int32, (16, dim), 0)

    def update_rows(c):
        fresh = kv_buf[pl.ds(pl.multiple_of(c * per, per), per), :]
        for j in range(per):
            b = c * per + j
            at = lens_ref[b] - first_pos
            base = pl.multiple_of(jnp.clip(at, 0, pos_local - 1) // 16 * 16, 16)
            hit = sub == at - base
            for buf, lo in ((k_buf, 0), (v_buf, dim)):
                new = jnp.broadcast_to(fresh[j:j + 1, lo:lo + dim], (16, dim))
                old = buf[b, pl.ds(base, 16), :].astype(F32)
                buf[b, pl.ds(base, 16), :] = jnp.where(hit, new, old).astype(BF16)

    def score(c):
        out = []
        for j in range(pairs):
            p = c * pairs + j
            q = q_buf[pl.ds(pl.multiple_of(p * rows, rows), rows), :]
            lhs = jnp.concatenate([jnp.where(top, q, 0.0), jnp.where(top, 0.0, q)], axis=1).astype(BF16)
            keys = jnp.concatenate([k_buf[2 * p], k_buf[2 * p + 1]], axis=1)
            s = lax.dot_general(lhs, keys, (((1,), (1,)), ((), ())), preferred_element_type=F32)
            out.append(s)
        return out

    def weigh(c, m_all, l_all):
        for j in range(pairs):
            p = c * pairs + j
            s = s_buf[j * rows:(j + 1) * rows, :] * scale
            last = jnp.where(top2, lens_ref[2 * p], lens_ref[2 * p + 1])
            valid = place <= last
            s = jnp.where(valid, s, NEG)
            m = jnp.max(s, axis=-1, keepdims=True)
            w = jnp.where(valid, jnp.exp(s - m), 0.0)
            total = jnp.sum(w, axis=-1, keepdims=True)
            vals = jnp.concatenate([v_buf[2 * p], v_buf[2 * p + 1]], axis=1)
            o = jnp.dot(w.astype(BF16), vals, preferred_element_type=F32)
            acc_ref[pl.ds(pl.multiple_of(p * rows, rows), rows), :] = jnp.where(top, o[:, :dim], o[:, dim:])
            m_all = jnp.where(lane == p, m, m_all)
            l_all = jnp.where(lane == p, total, l_all)
        return m_all, l_all

    def put_scores(out):
        for j, s in enumerate(out):
            s_buf[j * rows:(j + 1) * rows, :] = s

    def acc_store(c):
        part = pl.ds(pl.multiple_of(c * (pairs * rows), pairs * rows), pairs * rows)
        return pltpu.make_async_copy(acc_ref.at[part], acc_out.at[part], acc_sem.at[c])

    def loaded(c):
        k_load(c).wait()
        v_load(c).wait()

    def leave(c):
        k_store(c).start()
        v_store(c).start(priority=1)

    loaded(0)
    update_rows(0)
    put_scores(score(0))
    zero = jnp.zeros((rows, dim), F32)

    def early(c, carry):
        loaded(c + 1)
        update_rows(c + 1)
        carry = weigh(c, *carry)
        put_scores(score(c + 1))
        acc_store(c).start()
        return carry

    carry = lax.fori_loop(0, held, early, (zero, zero))

    @pl.loop(held + 1, chunks)
    def _(c):
        loaded(c)

    @pl.loop(0, held + 1)
    def _(c):
        leave(c)

    def late(c, carry):
        update_rows(c + 1)
        carry = weigh(c, *carry)
        put_scores(score(c + 1))
        acc_store(c).start()
        leave(c + 1)
        return carry

    carry = lax.fori_loop(held, chunks - 1, late, carry)
    m_all, l_all = weigh(chunks - 1, *carry)
    ml_ref[:rows, :] = m_all
    ml_ref[rows:, :] = l_all
    acc_store(chunks - 1).start()

    @pl.loop(0, chunks - 1)
    def _(c):
        k_store(c).wait()
        v_store(c).wait()
        acc_store(c).wait()

    ml_store = pltpu.make_async_copy(ml_ref, acc_out.at[pl.ds(batch * heads, 2 * rows)], ml_sem)
    ml_store.start()
    k_store(chunks - 1).wait()
    v_store(chunks - 1).wait()
    acc_store(chunks - 1).wait()
    ml_store.wait()


def attend(lens, x, gain, bias, wq, bq, wkv, bkv, k, v, pairs=8, held=6):
    batch, pos_local, dim = k.shape
    width = x.shape[1]
    heads = wq.shape[1] // dim
    chunks = batch // (2 * pairs)
    hbm = pl.BlockSpec(memory_space=pltpu.HBM)
    vmem = pl.BlockSpec(memory_space=pltpu.VMEM)
    dma = pltpu.SemaphoreType.DMA
    return pl.pallas_call(
        functools.partial(attend_kernel, pairs, held),
        out_shape=(
            jax.ShapeDtypeStruct(k.shape, k.dtype),
            jax.ShapeDtypeStruct(v.shape, v.dtype),
            jax.ShapeDtypeStruct((batch * heads + 4 * heads, dim), F32),
        ),
        in_specs=[pl.BlockSpec(memory_space=pltpu.SMEM), hbm, vmem, vmem, hbm, vmem, hbm, vmem, hbm, hbm],
        out_specs=(hbm, hbm, hbm),
        scratch_shapes=[
            pltpu.VMEM(x.shape, BF16),
            pltpu.VMEM(x.shape, BF16),
            pltpu.VMEM(wq.shape, BF16),
            pltpu.VMEM(wkv.shape, BF16),
            pltpu.VMEM((batch * heads, dim), F32),
            pltpu.VMEM((batch, 2 * dim), F32),
            pltpu.VMEM((pairs * 2 * heads, pos_local), F32),
            pltpu.VMEM((batch * heads, dim), F32),
            pltpu.VMEM((4 * heads, dim), F32),
            pltpu.VMEM(k.shape, BF16),
            pltpu.VMEM(v.shape, BF16),
            dma((3,)), dma((chunks,)), dma((chunks,)), dma((chunks,)), dma((chunks,)), dma((chunks,)), dma,
        ],
        compiler_params=pltpu.CompilerParams(vmem_limit_bytes=60 * 1024 * 1024),
        cost_estimate=pl.CostEstimate(flops=2 * 2**30, bytes_accessed=72 * 2**20, transcendentals=0),
        name="attend",
    )(lens, x, gain.reshape(1, width), bias.reshape(1, width), wq, bq.reshape(1, -1), wkv, bkv.reshape(1, -1), k, v)


def meet_kernel(
    n_sq, parts, relayed, acc_hbm, x_hbm, wo_ref, bo_ref, out_ref,
    acc_buf, x_buf, base_buf, pair_buf, ml_pair, up_buf, ml_up, cross_buf, ml_cross, a_buf, z_out, far_in, in_buf, y_buf,
    in_sem, ml_send, ml_recv, mlu_send, mlu_recv, pair_send, pair_recv, up_send, up_recv, z_send, m_recv, s_recv, g_send, g_recv, y_send, y_recv, c_send, c_recv, f_send, f_recv,
):
    n_tp = z_out.shape[1]
    width = y_buf.shape[1]
    dim = acc_buf.shape[1]
    sq, tp = lax.axis_index("sq"), lax.axis_index("tp")
    own = y_buf.shape[0] // n_sq
    step = own // parts
    cols = width // n_tp
    heads = wo_ref.shape[0] // dim
    rows = 2 * heads
    pairs = step // 2
    fold = step * heads
    mesh_id = pl.DeviceIdType.MESH

    def at_tp(d):
        return {"tp": lax.rem(tp + d, n_tp)}

    core_sq = sq + 1 - 2 * lax.rem(sq, 2)
    across_sq = lax.rem(sq + 2, n_sq)
    core, across = {"sq": core_sq}, {"sq": across_sq}

    acc_in = pltpu.make_async_copy(acc_hbm, acc_buf, in_sem.at[0])
    acc_in.start()
    barrier = pltpu.get_barrier_semaphore()
    for to in (core, across):
        pl.semaphore_signal(barrier, inc=1, device_id=to, device_id_type=mesh_id)
    for d in range(1, n_tp):
        pl.semaphore_signal(barrier, inc=1, device_id=at_tp(d), device_id_type=mesh_id)
    x_cols = pl.ds(pl.multiple_of(tp * cols, cols), cols)
    x_in = pltpu.make_async_copy(x_hbm.at[pl.ds(pl.multiple_of(sq * own, own), own), x_cols], x_buf, in_sem.at[1])
    x_in.start()
    ml_own = acc_buf.at[pl.ds(own * n_sq * heads, 2 * rows)]
    with jax.named_scope('barrier'):
        acc_in.wait()
        pl.semaphore_wait(barrier, 2 + n_tp - 1)

    def remote(src, dst, send, recv, to):
        return pltpu.make_async_remote_copy(src_ref=src, dst_ref=dst, send_sem=send, recv_sem=recv, device_id=to, device_id_type=mesh_id)

    def acc_rows(s, c):
        return pl.ds(pl.multiple_of(s * (own * heads) + c * fold, fold), fold)

    def pair_copy(k, c):
        rows_for = acc_rows(core_sq if k == 0 else lax.rem(core_sq + 2, n_sq), c)
        return remote(acc_buf.at[rows_for], pair_buf.at[k, c], pair_send, pair_recv.at[k, c], core)

    def up_copy(c):
        return remote(up_buf.at[c], cross_buf.at[c], up_send, up_recv.at[c], across)

    ml_copy = remote(ml_own, ml_pair, ml_send, ml_recv, core)
    mlu_copy = remote(ml_up, ml_cross, mlu_send, mlu_recv, across)

    half = n_tp // 2
    middle = lax.div(tp + 1, 2) == 1
    partner = tp + 1 - 2 * lax.rem(tp, 2)
    far = half - half * lax.div(tp, half)

    def m_copy(c):
        return remote(z_out.at[c, pl.ds(far, half)], far_in.at[c], z_send, m_recv.at[c], {"tp": partner})

    def n_copy(c):
        return remote(z_out.at[c, partner], in_buf.at[c, 0], z_send, s_recv.at[c], {"tp": partner})

    def s_copy(k, c):
        return remote(z_out.at[c, far + k], in_buf.at[c, 1], z_send, s_recv.at[c], {"tp": far + k})

    def block(s, t, c):
        return y_buf.at[pl.ds(pl.multiple_of(s * own + c * step, step), step), pl.ds(pl.multiple_of(t * cols, cols), cols)]

    def source(tag):
        return tp - tag if tag < n_tp else tp + (tag - n_tp + 1)

    def source_of(tag, c):
        return source(tag) if c < relayed else lax.rem(tp - tag + n_tp, n_tp)

    def tp_copy(t, c, to):
        b = block(sq, t, c)
        return remote(b, b, g_send, g_recv.at[t, c], {"tp": to})

    def y_copy(tag, c):
        t = source_of(tag, c)
        b = block(sq, t, c)
        return remote(b, b, y_send, y_recv.at[t, c], across)

    def c_copy(tag, c):
        b = block(sq, source_of(tag, c), c)
        return remote(b, b, c_send, c_recv, core)

    def f_copy(tag, c):
        b = block(across_sq, source_of(tag, c), c)
        return remote(b, b, f_send, f_recv, core)

    def all_of(ref, send, recv):
        return remote(ref, ref, send, recv, {"tp": tp})

    ml_copy.start()
    for k in (1, 0):
        for c in range(parts):
            pair_copy(k, c).start()

    lane = lax.broadcasted_iota(jnp.int32, (rows, dim), 1)

    def column(e, p):
        return jnp.sum(jnp.where(lane == p, e, 0.0), axis=1, keepdims=True)

    def part_of(j):
        return slice(j * rows, (j + 1) * rows)

    with jax.named_scope("pairwait"):
        ml_copy.wait_recv()
    ml_at = own * n_sq * heads
    m_own, l_own = acc_buf[ml_at:ml_at + rows, :], acc_buf[ml_at + rows:ml_at + 2 * rows, :]
    m_pair, l_pair = ml_pair[:rows, :], ml_pair[rows:, :]
    m_up = jnp.maximum(m_own, m_pair)
    e_own, e_pair = jnp.exp(m_own - m_up), jnp.exp(m_pair - m_up)
    ml_up[:rows, :] = m_up
    ml_up[rows:, :] = e_own * l_own + e_pair * l_pair
    for c in range(parts):
        pair_copy(1, c).wait_recv()
        for j in range(pairs):
            p = across_sq * (own // 2) + c * pairs + j
            mine = pl.multiple_of(across_sq * (own * heads) + c * fold + j * rows, rows)
            up_buf[c, part_of(j), :] = column(e_own, p) * acc_buf[pl.ds(mine, rows), :] + column(e_pair, p) * pair_buf[1, c, part_of(j), :]
        if c == 0:
            mlu_copy.start()
        up_copy(c).start()

    x_in.wait()
    base_buf[...] = x_buf[...].astype(F32) + bo_ref[:, x_cols]
    with jax.named_scope("mlwait"):
        mlu_copy.wait_recv()
    m_cross, l_cross = ml_cross[:rows, :], ml_cross[rows:, :]
    top = jnp.maximum(m_up, m_cross)
    scales = [jnp.exp(m - top) for m in (m_own, m_pair, m_cross)]
    den = scales[0] * l_own + scales[1] * l_pair + scales[2] * l_cross
    scales = [e / den for e in scales]

    def when(cond):
        return pl.when(cond)

    def project(c):
        pair_copy(0, c).wait_recv()
        up_copy(c).wait_recv()
        for j in range(pairs):
            p = sq * (own // 2) + c * pairs + j
            mine = pl.multiple_of(sq * (own * heads) + c * fold + j * rows, rows)
            terms = (acc_buf[pl.ds(mine, rows), :], pair_buf[0, c, part_of(j), :], cross_buf[c, part_of(j), :])
            total = sum(column(e, p) * t for e, t in zip(scales, terms))
            a_buf[j * rows:(j + 1) * rows, :] = total
        lhs = jnp.concatenate([a_buf[pl.ds(n, step, stride=heads), :].astype(BF16) for n in range(heads)], axis=1)
        def term(t):
            w = wo_ref[:, pl.ds(pl.multiple_of(t * cols, cols), cols)]
            z_out[c, t] = jnp.dot(lhs, w, preferred_element_type=F32)

        for k in range(half):
            term(far + k)

        @when(jnp.logical_not(middle))
        def _():
            m_copy(c).start()

        term(partner)
        term(tp)

        if c:
            n_copy(c - 1).start()
        if c == parts - 1:
            n_copy(c).start()

    def add(c):
        @when(middle)
        def _():
            m_copy(c).wait_recv()
            for k in range(half):
                z_out[c, far + k] = z_out[c, far + k] + far_in[c, k]
            for k in range(half):
                s_copy(k, c).start()

    def share(tag, c):
        y_copy(tag, c).start()
        c_copy(tag, c).start()

    def finish(c):
        all_of(in_buf.at[c], z_send, s_recv.at[c]).wait_recv()
        total = z_out[c, tp] + in_buf[c, 0] + in_buf[c, 1]
        total = total + base_buf[c * step:(c + 1) * step, :]
        mine = block(sq, tp, c)
        mine[...] = total

        if c < relayed:
            @when(tp < n_tp - 1)
            def _():
                tp_copy(tp, c, tp + 1).start()

            @when(tp > 0)
            def _():
                tp_copy(tp, c, tp - 1).start()
        else:
            for d in range(1, n_tp):
                tp_copy(tp, c, lax.rem(tp + d, n_tp)).start()

        share(0, c)

    def direct(d, c):
        tp_copy(source_of(d, c), c, tp).wait_recv()
        share(d, c)

    def hop(h, c):
        @when(tp >= h)
        def _():
            tp_copy(tp - h, c, tp).wait_recv()

            @when(tp < n_tp - 1)
            def _():
                tp_copy(tp - h, c, tp + 1).start()

            share(h, c)

        @when(tp + h < n_tp)
        def _():
            tp_copy(tp + h, c, tp).wait_recv()

            @when(tp > 0)
            def _():
                tp_copy(tp + h, c, tp - 1).start()

            share(h + n_tp - 1, c)

    def crossed(h, c):
        def take(tag):
            y_copy(tag, c).wait_recv()
            f_copy(tag, c).start()

        if h == 0 or c >= relayed:
            take(h)
            return

        @when(tp >= h)
        def _():
            take(h)

        @when(tp + h < n_tp)
        def _():
            take(h + n_tp - 1)

    def named(name, fn, *args):
        def run():
            with jax.named_scope(name):
                fn(*args)
        return run

    events = []
    for c in range(parts):
        events.append((6.3 + 3.0 / parts * c, 0, named(f"p{c}", project, c)))
        events.append((8.1 + 8.4 / parts * (c + 1), 0, named(f"a{c}", add, c)))
        t = 11.7 + 8.4 / parts * (c + 1)
        events.append((t, 1, named(f"f{c}", finish, c)))
        events.append((t + 4.0, 3, named(f"y{c}_0", crossed, 0, c)))
        for h in range(1, n_tp):
            if c < relayed:
                there = t + 3.6 * h - 0.7
                events.append((there, 2, named(f"h{c}_{h}", hop, h, c)))
            else:
                there = t + 3.2 + 0.8 * h
                events.append((there, 2, named(f"d{c}_{h}", direct, h, c)))
            events.append((there + 5.0, 3, named(f"y{c}_{h}", crossed, h, c)))
    for _, _, event in sorted(events, key=lambda e: e[:2]):
        event()

    whole = y_buf.at[pl.ds(0, own)]
    with jax.named_scope("close"):
        all_of(whole, c_send, c_recv).wait()
        all_of(whole, f_send, f_recv).wait()
        all_of(whole, y_send, f_recv).wait_send()
        ml_copy.wait_send()
        mlu_copy.wait_send()
        all_of(pair_buf, pair_send, ml_recv).wait_send()
        all_of(up_buf, up_send, ml_recv).wait_send()
        all_of(z_out.at[:, pl.ds(0, half + 1)], z_send, ml_recv).wait_send()
        straight = (parts - relayed) * (n_tp - 1)

        @when(middle)
        def _():
            blocks = y_buf.at[pl.ds(0, (straight + relayed * (n_tp + 1)) * step // n_tp)]
            all_of(blocks, g_send, ml_recv).wait_send()

        @when(jnp.logical_not(middle))
        def _():
            blocks = y_buf.at[pl.ds(0, (straight + relayed) * step // n_tp)]
            all_of(blocks, g_send, ml_recv).wait_send()

    chunk = 32
    for i in range(y_buf.shape[0] // chunk):
      with jax.named_scope(f'emit{i}'):
        out_ref[i * chunk:(i + 1) * chunk, :] = y_buf[i * chunk:(i + 1) * chunk, :].astype(BF16)


def meet(acc, x, wo, bo, n_sq, n_tp, parts=4, relayed=2):
    batch, width = x.shape
    own = batch // n_sq
    cols = width // n_tp
    step = own // parts
    heads = wo.shape[0] // acc.shape[1]
    dim = acc.shape[1]
    vmem = pl.BlockSpec(memory_space=pltpu.VMEM)
    hbm = pl.BlockSpec(memory_space=pltpu.HBM)
    dma = pltpu.SemaphoreType.DMA
    return pl.pallas_call(
        functools.partial(meet_kernel, n_sq, parts, relayed),
        out_shape=jax.ShapeDtypeStruct((batch, width), BF16),
        in_specs=[hbm, hbm, vmem, vmem],
        out_specs=vmem,
        scratch_shapes=[
            pltpu.VMEM(acc.shape, F32),
            pltpu.VMEM((own, cols), BF16),
            pltpu.VMEM((own, cols), F32),
            pltpu.VMEM((2, parts, step * heads, dim), F32),
            pltpu.VMEM((4 * heads, dim), F32),
            pltpu.VMEM((parts, step * heads, dim), F32),
            pltpu.VMEM((4 * heads, dim), F32),
            pltpu.VMEM((parts, step * heads, dim), F32),
            pltpu.VMEM((4 * heads, dim), F32),
            pltpu.VMEM((step * heads, dim), F32),
            pltpu.VMEM((parts, n_tp, step, cols), F32),
            pltpu.VMEM((parts, n_tp // 2, step, cols), F32),
            pltpu.VMEM((parts, 2, step, cols), F32),
            pltpu.VMEM((batch, width), F32),
            dma((2,)), dma, dma, dma, dma, dma, dma((2, parts)), dma, dma((parts,)),
            dma, dma((parts,)), dma((parts,)), dma, dma((n_tp, parts)),
            dma, dma((n_tp, parts)), dma, dma, dma, dma,
        ],
        compiler_params=pltpu.CompilerParams(collective_id=0, has_side_effects=True, vmem_limit_bytes=32 * 1024 * 1024),
        cost_estimate=pl.CostEstimate(flops=2**28, bytes_accessed=8 * 2**20, transcendentals=0),
        name="meet",
    )(pltpu.with_memory_space_constraint(acc, pltpu.HBM), pltpu.with_memory_space_constraint(x, pltpu.HBM), wo, bo.reshape(1, width))


def solution(mesh):
    def local_step(hidden, cache_lens, k_cache, v_cache, ln_gain, ln_bias, w_query, b_query, w_kv, b_kv, w_out, b_out):
        key_new, val_new, acc = attend(
            cache_lens, hidden, ln_gain, ln_bias, w_query, b_query, w_kv, b_kv, k_cache, v_cache)
        out_hidden = meet(acc, hidden, w_out, b_out, mesh.shape["sq"], mesh.shape["tp"])
        return out_hidden, key_new, val_new

    cache_spec = P("dp", "sq", None)
    row_spec = P("dp", None)
    in_specs = (row_spec, P("dp"), cache_spec, cache_spec, P(None), P(None), P(None, "tp"), P("tp"), P(None, None), P(None), P("tp", None), P(None))
    out_specs = (row_spec, cache_spec, cache_spec)
    return jax.shard_map(local_step, mesh=mesh, in_specs=in_specs, out_specs=out_specs, check_vma=False)
```

```python
import functools

import jax
import jax.numpy as jnp
from jax import lax
from jax.experimental import pallas as pl
from jax.experimental.pallas import tpu as pltpu
from jax.sharding import PartitionSpec as P

F32 = jnp.float32
BF16 = jnp.bfloat16
NEG = -1e30


def attend_kernel(
    pairs, held, lens_ref, x_hbm, gain_ref, bias_ref, wq_hbm, bq_ref, wkv_hbm, bkv_ref, k_hbm, v_hbm,
    k_out, v_out, acc_out,
    x_buf, h_buf, wq_buf, wkv_buf, q_buf, kv_buf, s_buf, acc_ref, ml_ref, k_buf, v_buf,
    in_sem, k_sem, v_sem, ko_sem, vo_sem, acc_sem, ml_sem,
):
    batch, pos_local, dim = k_buf.shape
    heads = wq_buf.shape[1] // dim
    per = 2 * pairs
    chunks = batch // per
    rows = 2 * heads
    first_pos = lax.axis_index("sq") * pos_local
    scale = dim ** -0.5

    x_copy = pltpu.make_async_copy(x_hbm, x_buf, in_sem.at[0])
    kv_copy = pltpu.make_async_copy(wkv_hbm, wkv_buf, in_sem.at[1])
    q_copy = pltpu.make_async_copy(wq_hbm, wq_buf, in_sem.at[2])
    x_copy.start()
    kv_copy.start()
    q_copy.start()

    def span(ref, c):
        return ref.at[pl.ds(c * per, per)]

    def k_load(c):
        return pltpu.make_async_copy(span(k_hbm, c), span(k_buf, c), k_sem.at[c])

    def v_load(c):
        return pltpu.make_async_copy(span(v_hbm, c), span(v_buf, c), v_sem.at[c])

    def k_store(c):
        return pltpu.make_async_copy(span(k_buf, c), span(k_out, c), ko_sem.at[c])

    def v_store(c):
        return pltpu.make_async_copy(span(v_buf, c), span(v_out, c), vo_sem.at[c])

    @pl.loop(0, chunks)
    def _(c):
        k_load(c).start()
        v_load(c).start(priority=1)

    x_copy.wait()
    block = 32

    @pl.loop(0, batch // block)
    def _(i):
        x = x_buf[pl.ds(i * block, block), :].astype(F32)
        mean = jnp.mean(x, axis=-1, keepdims=True)
        cen = x - mean
        var = jnp.mean(cen * cen, axis=-1, keepdims=True)
        h = cen * lax.rsqrt(var + 1e-5) * gain_ref[...] + bias_ref[...]
        h_buf[pl.ds(i * block, block), :] = h.astype(BF16)

    kv_copy.wait()
    kv = jnp.dot(h_buf[...], wkv_buf[...], preferred_element_type=F32) + bkv_ref[...]
    kv_buf[...] = kv.astype(BF16).astype(F32)
    q_copy.wait()
    for n0 in range(0, heads, 2):
        cols = slice(n0 * dim, (n0 + 2) * dim)
        q = jnp.dot(h_buf[...], wq_buf[:, cols], preferred_element_type=F32) + bq_ref[:, cols]
        q = q.astype(BF16).astype(F32)
        q_buf[pl.ds(n0, batch, stride=heads), :] = q[:, :dim]
        q_buf[pl.ds(n0 + 1, batch, stride=heads), :] = q[:, dim:]

    top = lax.broadcasted_iota(jnp.int32, (rows, dim), 0) < heads
    top2 = lax.broadcasted_iota(jnp.int32, (rows, pos_local), 0) < heads
    lane = lax.broadcasted_iota(jnp.int32, (rows, dim), 1)
    place = first_pos + lax.broadcasted_iota(jnp.int32, (rows, pos_local), 1)
    sub = lax.broadcasted_iota(jnp.int32, (16, dim), 0)

    def update_rows(c):
        fresh = kv_buf[pl.ds(pl.multiple_of(c * per, per), per), :]
        for j in range(per):
            b = c * per + j
            at = lens_ref[b] - first_pos
            base = pl.multiple_of(jnp.clip(at, 0, pos_local - 1) // 16 * 16, 16)
            hit = sub == at - base
            for buf, lo in ((k_buf, 0), (v_buf, dim)):
                new = jnp.broadcast_to(fresh[j:j + 1, lo:lo + dim], (16, dim))
                old = buf[b, pl.ds(base, 16), :].astype(F32)
                buf[b, pl.ds(base, 16), :] = jnp.where(hit, new, old).astype(BF16)

    def score(c):
        out = []
        for j in range(pairs):
            p = c * pairs + j
            q = q_buf[pl.ds(pl.multiple_of(p * rows, rows), rows), :]
            lhs = jnp.concatenate([jnp.where(top, q, 0.0), jnp.where(top, 0.0, q)], axis=1).astype(BF16)
            keys = jnp.concatenate([k_buf[2 * p], k_buf[2 * p + 1]], axis=1)
            s = lax.dot_general(lhs, keys, (((1,), (1,)), ((), ())), preferred_element_type=F32)
            out.append(s)
        return out

    def weigh(c, m_all, l_all):
        for j in range(pairs):
            p = c * pairs + j
            s = s_buf[j * rows:(j + 1) * rows, :] * scale
            last = jnp.where(top2, lens_ref[2 * p], lens_ref[2 * p + 1])
            valid = place <= last
            s = jnp.where(valid, s, NEG)
            m = jnp.max(s, axis=-1, keepdims=True)
            w = jnp.where(valid, jnp.exp(s - m), 0.0)
            total = jnp.sum(w, axis=-1, keepdims=True)
            vals = jnp.concatenate([v_buf[2 * p], v_buf[2 * p + 1]], axis=1)
            o = jnp.dot(w.astype(BF16), vals, preferred_element_type=F32)
            acc_ref[pl.ds(pl.multiple_of(p * rows, rows), rows), :] = jnp.where(top, o[:, :dim], o[:, dim:])
            m_all = jnp.where(lane == p, m, m_all)
            l_all = jnp.where(lane == p, total, l_all)
        return m_all, l_all

    def put_scores(out):
        for j, s in enumerate(out):
            s_buf[j * rows:(j + 1) * rows, :] = s

    def acc_store(c):
        part = pl.ds(pl.multiple_of(c * (pairs * rows), pairs * rows), pairs * rows)
        return pltpu.make_async_copy(acc_ref.at[part], acc_out.at[part], acc_sem.at[c])

    def loaded(c):
        k_load(c).wait()
        v_load(c).wait()

    def leave(c):
        k_store(c).start()
        v_store(c).start(priority=1)

    loaded(0)
    update_rows(0)
    put_scores(score(0))
    zero = jnp.zeros((rows, dim), F32)

    def early(c, carry):
        loaded(c + 1)
        update_rows(c + 1)
        carry = weigh(c, *carry)
        put_scores(score(c + 1))
        acc_store(c).start()
        return carry

    carry = lax.fori_loop(0, held, early, (zero, zero))

    @pl.loop(held + 1, chunks)
    def _(c):
        loaded(c)

    @pl.loop(0, held + 1)
    def _(c):
        leave(c)

    def late(c, carry):
        update_rows(c + 1)
        carry = weigh(c, *carry)
        put_scores(score(c + 1))
        acc_store(c).start()
        leave(c + 1)
        return carry

    carry = lax.fori_loop(held, chunks - 1, late, carry)
    m_all, l_all = weigh(chunks - 1, *carry)
    ml_ref[:rows, :] = m_all
    ml_ref[rows:, :] = l_all
    acc_store(chunks - 1).start()

    @pl.loop(0, chunks - 1)
    def _(c):
        k_store(c).wait()
        v_store(c).wait()
        acc_store(c).wait()

    ml_store = pltpu.make_async_copy(ml_ref, acc_out.at[pl.ds(batch * heads, 2 * rows)], ml_sem)
    ml_store.start()
    k_store(chunks - 1).wait()
    v_store(chunks - 1).wait()
    acc_store(chunks - 1).wait()
    ml_store.wait()


def attend(lens, x, gain, bias, wq, bq, wkv, bkv, k, v, pairs=8, held=6):
    batch, pos_local, dim = k.shape
    width = x.shape[1]
    heads = wq.shape[1] // dim
    chunks = batch // (2 * pairs)
    hbm = pl.BlockSpec(memory_space=pltpu.HBM)
    vmem = pl.BlockSpec(memory_space=pltpu.VMEM)
    dma = pltpu.SemaphoreType.DMA
    return pl.pallas_call(
        functools.partial(attend_kernel, pairs, held),
        out_shape=(
            jax.ShapeDtypeStruct(k.shape, k.dtype),
            jax.ShapeDtypeStruct(v.shape, v.dtype),
            jax.ShapeDtypeStruct((batch * heads + 4 * heads, dim), F32),
        ),
        in_specs=[pl.BlockSpec(memory_space=pltpu.SMEM), hbm, vmem, vmem, hbm, vmem, hbm, vmem, hbm, hbm],
        out_specs=(hbm, hbm, hbm),
        scratch_shapes=[
            pltpu.VMEM(x.shape, BF16),
            pltpu.VMEM(x.shape, BF16),
            pltpu.VMEM(wq.shape, BF16),
            pltpu.VMEM(wkv.shape, BF16),
            pltpu.VMEM((batch * heads, dim), F32),
            pltpu.VMEM((batch, 2 * dim), F32),
            pltpu.VMEM((pairs * 2 * heads, pos_local), F32),
            pltpu.VMEM((batch * heads, dim), F32),
            pltpu.VMEM((4 * heads, dim), F32),
            pltpu.VMEM(k.shape, BF16),
            pltpu.VMEM(v.shape, BF16),
            dma((3,)), dma((chunks,)), dma((chunks,)), dma((chunks,)), dma((chunks,)), dma((chunks,)), dma,
        ],
        compiler_params=pltpu.CompilerParams(vmem_limit_bytes=60 * 1024 * 1024),
        cost_estimate=pl.CostEstimate(flops=2 * 2**30, bytes_accessed=72 * 2**20, transcendentals=0),
        name="attend",
    )(lens, x, gain.reshape(1, width), bias.reshape(1, width), wq, bq.reshape(1, -1), wkv, bkv.reshape(1, -1), k, v)


def meet_kernel(
    n_sq, parts, relayed, acc_hbm, x_hbm, wo_ref, bo_ref, out_ref,
    acc_buf, x_buf, base_buf, pair_buf, ml_pair, up_buf, ml_up, cross_buf, ml_cross, a_buf, z_out, far_in, in_buf, y_buf,
    in_sem, ml_send, ml_recv, mlu_send, mlu_recv, pair_send, pair_recv, up_send, up_recv, z_send, m_recv, s_recv, g_send, g_recv, y_send, y_recv, c_send, c_recv, f_send, f_recv,
):
    n_tp = z_out.shape[1]
    width = y_buf.shape[1]
    dim = acc_buf.shape[1]
    sq, tp = lax.axis_index("sq"), lax.axis_index("tp")
    own = y_buf.shape[0] // n_sq
    step = own // parts
    cols = width // n_tp
    heads = wo_ref.shape[0] // dim
    rows = 2 * heads
    pairs = step // 2
    fold = step * heads
    mesh_id = pl.DeviceIdType.MESH

    def at_tp(d):
        return {"tp": lax.rem(tp + d, n_tp)}

    core_sq = sq + 1 - 2 * lax.rem(sq, 2)
    across_sq = lax.rem(sq + 2, n_sq)
    core, across = {"sq": core_sq}, {"sq": across_sq}

    acc_in = pltpu.make_async_copy(acc_hbm, acc_buf, in_sem.at[0])
    acc_in.start()
    barrier = pltpu.get_barrier_semaphore()
    for to in (core, across):
        pl.semaphore_signal(barrier, inc=1, device_id=to, device_id_type=mesh_id)
    for d in range(1, n_tp):
        pl.semaphore_signal(barrier, inc=1, device_id=at_tp(d), device_id_type=mesh_id)
    x_cols = pl.ds(pl.multiple_of(tp * cols, cols), cols)
    x_in = pltpu.make_async_copy(x_hbm.at[pl.ds(pl.multiple_of(sq * own, own), own), x_cols], x_buf, in_sem.at[1])
    x_in.start()
    ml_own = acc_buf.at[pl.ds(own * n_sq * heads, 2 * rows)]
    with jax.named_scope('barrier'):
        acc_in.wait()
        pl.semaphore_wait(barrier, 2 + n_tp - 1)

    def remote(src, dst, send, recv, to):
        return pltpu.make_async_remote_copy(src_ref=src, dst_ref=dst, send_sem=send, recv_sem=recv, device_id=to, device_id_type=mesh_id)

    def acc_rows(s, c):
        return pl.ds(pl.multiple_of(s * (own * heads) + c * fold, fold), fold)

    def pair_copy(k, c):
        rows_for = acc_rows(core_sq if k == 0 else lax.rem(core_sq + 2, n_sq), c)
        return remote(acc_buf.at[rows_for], pair_buf.at[k, c], pair_send, pair_recv.at[k, c], core)

    def up_copy(c):
        return remote(up_buf.at[c], cross_buf.at[c], up_send, up_recv.at[c], across)

    ml_copy = remote(ml_own, ml_pair, ml_send, ml_recv, core)
    mlu_copy = remote(ml_up, ml_cross, mlu_send, mlu_recv, across)

    half = n_tp // 2
    middle = lax.div(tp + 1, 2) == 1
    partner = tp + 1 - 2 * lax.rem(tp, 2)
    far = half - half * lax.div(tp, half)

    def m_copy(c):
        return remote(z_out.at[c, pl.ds(far, half)], far_in.at[c], z_send, m_recv.at[c], {"tp": partner})

    def n_copy(c):
        return remote(z_out.at[c, partner], in_buf.at[c, 0], z_send, s_recv.at[c], {"tp": partner})

    def s_copy(k, c):
        return remote(z_out.at[c, far + k], in_buf.at[c, 1], z_send, s_recv.at[c], {"tp": far + k})

    def block(s, t, c):
        return y_buf.at[pl.ds(pl.multiple_of(s * own + c * step, step), step), pl.ds(pl.multiple_of(t * cols, cols), cols)]

    def source(tag):
        return tp - tag if tag < n_tp else tp + (tag - n_tp + 1)

    def source_of(tag, c):
        return source(tag) if c < relayed else lax.rem(tp - tag + n_tp, n_tp)

    def tp_copy(t, c, to):
        b = block(sq, t, c)
        return remote(b, b, g_send, g_recv.at[t, c], {"tp": to})

    def y_copy(tag, c):
        t = source_of(tag, c)
        b = block(sq, t, c)
        return remote(b, b, y_send, y_recv.at[t, c], across)

    def c_copy(tag, c):
        b = block(sq, source_of(tag, c), c)
        return remote(b, b, c_send, c_recv, core)

    def f_copy(tag, c):
        b = block(across_sq, source_of(tag, c), c)
        return remote(b, b, f_send, f_recv, core)

    def all_of(ref, send, recv):
        return remote(ref, ref, send, recv, {"tp": tp})

    ml_copy.start()
    for k in (1, 0):
        for c in range(parts):
            pair_copy(k, c).start()

    lane = lax.broadcasted_iota(jnp.int32, (rows, dim), 1)

    def column(e, p):
        return jnp.sum(jnp.where(lane == p, e, 0.0), axis=1, keepdims=True)

    def part_of(j):
        return slice(j * rows, (j + 1) * rows)

    with jax.named_scope("pairwait"):
        ml_copy.wait_recv()
    ml_at = own * n_sq * heads
    m_own, l_own = acc_buf[ml_at:ml_at + rows, :], acc_buf[ml_at + rows:ml_at + 2 * rows, :]
    m_pair, l_pair = ml_pair[:rows, :], ml_pair[rows:, :]
    m_up = jnp.maximum(m_own, m_pair)
    e_own, e_pair = jnp.exp(m_own - m_up), jnp.exp(m_pair - m_up)
    ml_up[:rows, :] = m_up
    ml_up[rows:, :] = e_own * l_own + e_pair * l_pair
    for c in range(parts):
        pair_copy(1, c).wait_recv()
        for j in range(pairs):
            p = across_sq * (own // 2) + c * pairs + j
            mine = pl.multiple_of(across_sq * (own * heads) + c * fold + j * rows, rows)
            up_buf[c, part_of(j), :] = column(e_own, p) * acc_buf[pl.ds(mine, rows), :] + column(e_pair, p) * pair_buf[1, c, part_of(j), :]
        if c == 0:
            mlu_copy.start()
        up_copy(c).start()

    x_in.wait()
    base_buf[...] = x_buf[...].astype(F32) + bo_ref[:, x_cols]
    with jax.named_scope("mlwait"):
        mlu_copy.wait_recv()
    m_cross, l_cross = ml_cross[:rows, :], ml_cross[rows:, :]
    top = jnp.maximum(m_up, m_cross)
    scales = [jnp.exp(m - top) for m in (m_own, m_pair, m_cross)]
    den = scales[0] * l_own + scales[1] * l_pair + scales[2] * l_cross
    scales = [e / den for e in scales]

    def when(cond):
        return pl.when(cond)

    def project(c):
        pair_copy(0, c).wait_recv()
        up_copy(c).wait_recv()
        for j in range(pairs):
            p = sq * (own // 2) + c * pairs + j
            mine = pl.multiple_of(sq * (own * heads) + c * fold + j * rows, rows)
            terms = (acc_buf[pl.ds(mine, rows), :], pair_buf[0, c, part_of(j), :], cross_buf[c, part_of(j), :])
            total = sum(column(e, p) * t for e, t in zip(scales, terms))
            a_buf[j * rows:(j + 1) * rows, :] = total
        lhs = jnp.concatenate([a_buf[pl.ds(n, step, stride=heads), :].astype(BF16) for n in range(heads)], axis=1)
        def term(t):
            w = wo_ref[:, pl.ds(pl.multiple_of(t * cols, cols), cols)]
            z_out[c, t] = jnp.dot(lhs, w, preferred_element_type=F32)

        for k in range(half):
            term(far + k)

        @when(jnp.logical_not(middle))
        def _():
            m_copy(c).start()

        term(partner)
        term(tp)

        if c:
            n_copy(c - 1).start()
        if c == parts - 1:
            n_copy(c).start()

    def add(c):
        @when(middle)
        def _():
            m_copy(c).wait_recv()
            for k in range(half):
                z_out[c, far + k] = z_out[c, far + k] + far_in[c, k]
            for k in range(half):
                s_copy(k, c).start()

    def share(tag, c):
        y_copy(tag, c).start()
        c_copy(tag, c).start()

    def finish(c):
        all_of(in_buf.at[c], z_send, s_recv.at[c]).wait_recv()
        total = z_out[c, tp] + in_buf[c, 0] + in_buf[c, 1]
        total = total + base_buf[c * step:(c + 1) * step, :]
        mine = block(sq, tp, c)
        mine[...] = total

        if c < relayed:
            @when(tp < n_tp - 1)
            def _():
                tp_copy(tp, c, tp + 1).start()

            @when(tp > 0)
            def _():
                tp_copy(tp, c, tp - 1).start()
        else:
            for d in range(1, n_tp):
                tp_copy(tp, c, lax.rem(tp + d, n_tp)).start()

        share(0, c)

    def direct(d, c):
        tp_copy(source_of(d, c), c, tp).wait_recv()
        share(d, c)

    def hop(h, c):
        @when(tp >= h)
        def _():
            tp_copy(tp - h, c, tp).wait_recv()

            @when(tp < n_tp - 1)
            def _():
                tp_copy(tp - h, c, tp + 1).start()

            share(h, c)

        @when(tp + h < n_tp)
        def _():
            tp_copy(tp + h, c, tp).wait_recv()

            @when(tp > 0)
            def _():
                tp_copy(tp + h, c, tp - 1).start()

            share(h + n_tp - 1, c)

    def crossed(h, c):
        def take(tag):
            y_copy(tag, c).wait_recv()
            f_copy(tag, c).start()

        if h == 0 or c >= relayed:
            take(h)
            return

        @when(tp >= h)
        def _():
            take(h)

        @when(tp + h < n_tp)
        def _():
            take(h + n_tp - 1)

    def named(name, fn, *args):
        def run():
            with jax.named_scope(name):
                fn(*args)
        return run

    events = []
    for c in range(parts):
        events.append((6.3 + 3.0 / parts * c, 0, named(f"p{c}", project, c)))
        events.append((8.1 + 8.4 / parts * (c + 1), 0, named(f"a{c}", add, c)))
        t = 11.7 + 8.4 / parts * (c + 1)
        events.append((t, 1, named(f"f{c}", finish, c)))
        events.append((t + 4.0, 3, named(f"y{c}_0", crossed, 0, c)))
        for h in range(1, n_tp):
            if c < relayed:
                there = t + 3.6 * h - 0.7
                events.append((there, 2, named(f"h{c}_{h}", hop, h, c)))
            else:
                there = max(t, 17.4) + 3.2 + 0.8 * h
                events.append((there, 2, named(f"d{c}_{h}", direct, h, c)))
            events.append((there + 5.0, 3, named(f"y{c}_{h}", crossed, h, c)))
    for _, _, event in sorted(events, key=lambda e: e[:2]):
        event()

    whole = y_buf.at[pl.ds(0, own)]
    with jax.named_scope("close"):
        all_of(whole, c_send, c_recv).wait()
        all_of(whole, f_send, f_recv).wait()
        all_of(whole, y_send, f_recv).wait_send()
        ml_copy.wait_send()
        mlu_copy.wait_send()
        all_of(pair_buf, pair_send, ml_recv).wait_send()
        all_of(up_buf, up_send, ml_recv).wait_send()
        all_of(z_out.at[:, pl.ds(0, half + 1)], z_send, ml_recv).wait_send()
        straight = (parts - relayed) * (n_tp - 1)

        @when(middle)
        def _():
            blocks = y_buf.at[pl.ds(0, (straight + relayed * (n_tp + 1)) * step // n_tp)]
            all_of(blocks, g_send, ml_recv).wait_send()

        @when(jnp.logical_not(middle))
        def _():
            blocks = y_buf.at[pl.ds(0, (straight + relayed) * step // n_tp)]
            all_of(blocks, g_send, ml_recv).wait_send()

    chunk = 32
    for i in range(y_buf.shape[0] // chunk):
      with jax.named_scope(f'emit{i}'):
        out_ref[i * chunk:(i + 1) * chunk, :] = y_buf[i * chunk:(i + 1) * chunk, :].astype(BF16)


def meet(acc, x, wo, bo, n_sq, n_tp, parts=4, relayed=1):
    batch, width = x.shape
    own = batch // n_sq
    cols = width // n_tp
    step = own // parts
    heads = wo.shape[0] // acc.shape[1]
    dim = acc.shape[1]
    vmem = pl.BlockSpec(memory_space=pltpu.VMEM)
    hbm = pl.BlockSpec(memory_space=pltpu.HBM)
    dma = pltpu.SemaphoreType.DMA
    return pl.pallas_call(
        functools.partial(meet_kernel, n_sq, parts, relayed),
        out_shape=jax.ShapeDtypeStruct((batch, width), BF16),
        in_specs=[hbm, hbm, vmem, vmem],
        out_specs=vmem,
        scratch_shapes=[
            pltpu.VMEM(acc.shape, F32),
            pltpu.VMEM((own, cols), BF16),
            pltpu.VMEM((own, cols), F32),
            pltpu.VMEM((2, parts, step * heads, dim), F32),
            pltpu.VMEM((4 * heads, dim), F32),
            pltpu.VMEM((parts, step * heads, dim), F32),
            pltpu.VMEM((4 * heads, dim), F32),
            pltpu.VMEM((parts, step * heads, dim), F32),
            pltpu.VMEM((4 * heads, dim), F32),
            pltpu.VMEM((step * heads, dim), F32),
            pltpu.VMEM((parts, n_tp, step, cols), F32),
            pltpu.VMEM((parts, n_tp // 2, step, cols), F32),
            pltpu.VMEM((parts, 2, step, cols), F32),
            pltpu.VMEM((batch, width), F32),
            dma((2,)), dma, dma, dma, dma, dma, dma((2, parts)), dma, dma((parts,)),
            dma, dma((parts,)), dma((parts,)), dma, dma((n_tp, parts)),
            dma, dma((n_tp, parts)), dma, dma, dma, dma,
        ],
        compiler_params=pltpu.CompilerParams(collective_id=0, has_side_effects=True, vmem_limit_bytes=32 * 1024 * 1024),
        cost_estimate=pl.CostEstimate(flops=2**28, bytes_accessed=8 * 2**20, transcendentals=0),
        name="meet",
    )(pltpu.with_memory_space_constraint(acc, pltpu.HBM), pltpu.with_memory_space_constraint(x, pltpu.HBM), wo, bo.reshape(1, width))


def solution(mesh):
    def local_step(hidden, cache_lens, k_cache, v_cache, ln_gain, ln_bias, w_query, b_query, w_kv, b_kv, w_out, b_out):
        key_new, val_new, acc = attend(
            cache_lens, hidden, ln_gain, ln_bias, w_query, b_query, w_kv, b_kv, k_cache, v_cache)
        out_hidden = meet(acc, hidden, w_out, b_out, mesh.shape["sq"], mesh.shape["tp"])
        return out_hidden, key_new, val_new

    cache_spec = P("dp", "sq", None)
    row_spec = P("dp", None)
    in_specs = (row_spec, P("dp"), cache_spec, cache_spec, P(None), P(None), P(None, "tp"), P("tp"), P(None, None), P(None), P("tp", None), P(None))
    out_specs = (row_spec, cache_spec, cache_spec)
    return jax.shard_map(local_step, mesh=mesh, in_specs=in_specs, out_specs=out_specs, check_vma=False)
```

```python
import functools

import jax
import jax.numpy as jnp
from jax import lax
from jax.experimental import pallas as pl
from jax.experimental.pallas import tpu as pltpu
from jax.sharding import PartitionSpec as P

F32 = jnp.float32
BF16 = jnp.bfloat16
NEG = -1e30


def attend_kernel(
    pairs, held, lens_ref, x_hbm, gain_ref, bias_ref, wq_hbm, bq_ref, wkv_hbm, bkv_ref, k_hbm, v_hbm,
    k_out, v_out, acc_out,
    x_buf, h_buf, wq_buf, wkv_buf, q_buf, kv_buf, s_buf, acc_ref, ml_ref, k_buf, v_buf,
    in_sem, k_sem, v_sem, ko_sem, vo_sem, acc_sem, ml_sem,
):
    batch, pos_local, dim = k_buf.shape
    heads = wq_buf.shape[1] // dim
    per = 2 * pairs
    chunks = batch // per
    rows = 2 * heads
    first_pos = lax.axis_index("sq") * pos_local
    scale = dim ** -0.5

    x_copy = pltpu.make_async_copy(x_hbm, x_buf, in_sem.at[0])
    kv_copy = pltpu.make_async_copy(wkv_hbm, wkv_buf, in_sem.at[1])
    q_copy = pltpu.make_async_copy(wq_hbm, wq_buf, in_sem.at[2])
    x_copy.start()
    kv_copy.start()
    q_copy.start()

    def span(ref, c):
        return ref.at[pl.ds(c * per, per)]

    def k_load(c):
        return pltpu.make_async_copy(span(k_hbm, c), span(k_buf, c), k_sem.at[c])

    def v_load(c):
        return pltpu.make_async_copy(span(v_hbm, c), span(v_buf, c), v_sem.at[c])

    def k_store(c):
        return pltpu.make_async_copy(span(k_buf, c), span(k_out, c), ko_sem.at[c])

    def v_store(c):
        return pltpu.make_async_copy(span(v_buf, c), span(v_out, c), vo_sem.at[c])

    @pl.loop(0, chunks)
    def _(c):
        k_load(c).start()
        v_load(c).start(priority=1)

    x_copy.wait()
    block = 32

    @pl.loop(0, batch // block)
    def _(i):
        x = x_buf[pl.ds(i * block, block), :].astype(F32)
        mean = jnp.mean(x, axis=-1, keepdims=True)
        cen = x - mean
        var = jnp.mean(cen * cen, axis=-1, keepdims=True)
        h = cen * lax.rsqrt(var + 1e-5) * gain_ref[...] + bias_ref[...]
        h_buf[pl.ds(i * block, block), :] = h.astype(BF16)

    kv_copy.wait()
    kv = jnp.dot(h_buf[...], wkv_buf[...], preferred_element_type=F32) + bkv_ref[...]
    kv_buf[...] = kv.astype(BF16).astype(F32)
    q_copy.wait()
    for n0 in range(0, heads, 2):
        cols = slice(n0 * dim, (n0 + 2) * dim)
        q = jnp.dot(h_buf[...], wq_buf[:, cols], preferred_element_type=F32) + bq_ref[:, cols]
        q = q.astype(BF16).astype(F32)
        q_buf[pl.ds(n0, batch, stride=heads), :] = q[:, :dim]
        q_buf[pl.ds(n0 + 1, batch, stride=heads), :] = q[:, dim:]

    top = lax.broadcasted_iota(jnp.int32, (rows, dim), 0) < heads
    top2 = lax.broadcasted_iota(jnp.int32, (rows, pos_local), 0) < heads
    lane = lax.broadcasted_iota(jnp.int32, (rows, dim), 1)
    place = first_pos + lax.broadcasted_iota(jnp.int32, (rows, pos_local), 1)
    sub = lax.broadcasted_iota(jnp.int32, (16, dim), 0)

    def update_rows(c):
        fresh = kv_buf[pl.ds(pl.multiple_of(c * per, per), per), :]
        for j in range(per):
            b = c * per + j
            at = lens_ref[b] - first_pos
            base = pl.multiple_of(jnp.clip(at, 0, pos_local - 1) // 16 * 16, 16)
            hit = sub == at - base
            for buf, lo in ((k_buf, 0), (v_buf, dim)):
                new = jnp.broadcast_to(fresh[j:j + 1, lo:lo + dim], (16, dim))
                old = buf[b, pl.ds(base, 16), :].astype(F32)
                buf[b, pl.ds(base, 16), :] = jnp.where(hit, new, old).astype(BF16)

    def score(c):
        out = []
        for j in range(pairs):
            p = c * pairs + j
            q = q_buf[pl.ds(pl.multiple_of(p * rows, rows), rows), :]
            lhs = jnp.concatenate([jnp.where(top, q, 0.0), jnp.where(top, 0.0, q)], axis=1).astype(BF16)
            keys = jnp.concatenate([k_buf[2 * p], k_buf[2 * p + 1]], axis=1)
            s = lax.dot_general(lhs, keys, (((1,), (1,)), ((), ())), preferred_element_type=F32)
            out.append(s)
        return out

    def weigh(c, m_all, l_all):
        for j in range(pairs):
            p = c * pairs + j
            s = s_buf[j * rows:(j + 1) * rows, :] * scale
            last = jnp.where(top2, lens_ref[2 * p], lens_ref[2 * p + 1])
            valid = place <= last
            s = jnp.where(valid, s, NEG)
            m = jnp.max(s, axis=-1, keepdims=True)
            w = jnp.where(valid, jnp.exp(s - m), 0.0)
            total = jnp.sum(w, axis=-1, keepdims=True)
            vals = jnp.concatenate([v_buf[2 * p], v_buf[2 * p + 1]], axis=1)
            o = jnp.dot(w.astype(BF16), vals, preferred_element_type=F32)
            acc_ref[pl.ds(pl.multiple_of(p * rows, rows), rows), :] = jnp.where(top, o[:, :dim], o[:, dim:])
            m_all = jnp.where(lane == p, m, m_all)
            l_all = jnp.where(lane == p, total, l_all)
        return m_all, l_all

    def put_scores(out):
        for j, s in enumerate(out):
            s_buf[j * rows:(j + 1) * rows, :] = s

    def acc_store(c):
        part = pl.ds(pl.multiple_of(c * (pairs * rows), pairs * rows), pairs * rows)
        return pltpu.make_async_copy(acc_ref.at[part], acc_out.at[part], acc_sem.at[c])

    def loaded(c):
        k_load(c).wait()
        v_load(c).wait()

    def leave(c):
        k_store(c).start()
        v_store(c).start(priority=1)

    loaded(0)
    update_rows(0)
    put_scores(score(0))
    zero = jnp.zeros((rows, dim), F32)

    def early(c, carry):
        loaded(c + 1)
        update_rows(c + 1)
        carry = weigh(c, *carry)
        put_scores(score(c + 1))
        acc_store(c).start()
        return carry

    carry = lax.fori_loop(0, held, early, (zero, zero))

    @pl.loop(held + 1, chunks)
    def _(c):
        loaded(c)

    @pl.loop(0, held + 1)
    def _(c):
        leave(c)

    def late(c, carry):
        update_rows(c + 1)
        carry = weigh(c, *carry)
        put_scores(score(c + 1))
        acc_store(c).start()
        leave(c + 1)
        return carry

    carry = lax.fori_loop(held, chunks - 1, late, carry)
    m_all, l_all = weigh(chunks - 1, *carry)
    ml_ref[:rows, :] = m_all
    ml_ref[rows:, :] = l_all
    acc_store(chunks - 1).start()

    @pl.loop(0, chunks - 1)
    def _(c):
        k_store(c).wait()
        v_store(c).wait()
        acc_store(c).wait()

    ml_store = pltpu.make_async_copy(ml_ref, acc_out.at[pl.ds(batch * heads, 2 * rows)], ml_sem)
    ml_store.start()
    k_store(chunks - 1).wait()
    v_store(chunks - 1).wait()
    acc_store(chunks - 1).wait()
    ml_store.wait()


def attend(lens, x, gain, bias, wq, bq, wkv, bkv, k, v, pairs=8, held=6):
    batch, pos_local, dim = k.shape
    width = x.shape[1]
    heads = wq.shape[1] // dim
    chunks = batch // (2 * pairs)
    hbm = pl.BlockSpec(memory_space=pltpu.HBM)
    vmem = pl.BlockSpec(memory_space=pltpu.VMEM)
    dma = pltpu.SemaphoreType.DMA
    return pl.pallas_call(
        functools.partial(attend_kernel, pairs, held),
        out_shape=(
            jax.ShapeDtypeStruct(k.shape, k.dtype),
            jax.ShapeDtypeStruct(v.shape, v.dtype),
            jax.ShapeDtypeStruct((batch * heads + 4 * heads, dim), F32),
        ),
        in_specs=[pl.BlockSpec(memory_space=pltpu.SMEM), hbm, vmem, vmem, hbm, vmem, hbm, vmem, hbm, hbm],
        out_specs=(hbm, hbm, hbm),
        scratch_shapes=[
            pltpu.VMEM(x.shape, BF16),
            pltpu.VMEM(x.shape, BF16),
            pltpu.VMEM(wq.shape, BF16),
            pltpu.VMEM(wkv.shape, BF16),
            pltpu.VMEM((batch * heads, dim), F32),
            pltpu.VMEM((batch, 2 * dim), F32),
            pltpu.VMEM((pairs * 2 * heads, pos_local), F32),
            pltpu.VMEM((batch * heads, dim), F32),
            pltpu.VMEM((4 * heads, dim), F32),
            pltpu.VMEM(k.shape, BF16),
            pltpu.VMEM(v.shape, BF16),
            dma((3,)), dma((chunks,)), dma((chunks,)), dma((chunks,)), dma((chunks,)), dma((chunks,)), dma,
        ],
        compiler_params=pltpu.CompilerParams(vmem_limit_bytes=60 * 1024 * 1024),
        cost_estimate=pl.CostEstimate(flops=2 * 2**30, bytes_accessed=72 * 2**20, transcendentals=0),
        name="attend",
    )(lens, x, gain.reshape(1, width), bias.reshape(1, width), wq, bq.reshape(1, -1), wkv, bkv.reshape(1, -1), k, v)


def meet_kernel(
    n_sq, parts, relayed, acc_hbm, x_hbm, wo_ref, bo_ref, out_ref,
    acc_buf, x_buf, base_buf, pair_buf, ml_pair, up_buf, ml_up, cross_buf, ml_cross, a_buf, z_out, far_in, in_buf, y_buf,
    in_sem, ml_send, ml_recv, mlu_send, mlu_recv, pair_send, pair_recv, up_send, up_recv, z_send, m_recv, s_recv, g_send, g_recv, y_send, y_recv, c_send, c_recv, f_send, f_recv,
):
    n_tp = z_out.shape[1]
    width = y_buf.shape[1]
    dim = acc_buf.shape[1]
    sq, tp = lax.axis_index("sq"), lax.axis_index("tp")
    own = y_buf.shape[0] // n_sq
    step = own // parts
    cols = width // n_tp
    heads = wo_ref.shape[0] // dim
    rows = 2 * heads
    pairs = step // 2
    fold = step * heads
    mesh_id = pl.DeviceIdType.MESH

    def at_tp(d):
        return {"tp": lax.rem(tp + d, n_tp)}

    core_sq = sq + 1 - 2 * lax.rem(sq, 2)
    across_sq = lax.rem(sq + 2, n_sq)
    core, across = {"sq": core_sq}, {"sq": across_sq}

    acc_in = pltpu.make_async_copy(acc_hbm, acc_buf, in_sem.at[0])
    acc_in.start()
    barrier = pltpu.get_barrier_semaphore()
    for to in (core, across):
        pl.semaphore_signal(barrier, inc=1, device_id=to, device_id_type=mesh_id)
    for d in range(1, n_tp):
        pl.semaphore_signal(barrier, inc=1, device_id=at_tp(d), device_id_type=mesh_id)
    x_cols = pl.ds(pl.multiple_of(tp * cols, cols), cols)
    x_in = pltpu.make_async_copy(x_hbm.at[pl.ds(pl.multiple_of(sq * own, own), own), x_cols], x_buf, in_sem.at[1])
    x_in.start()
    ml_own = acc_buf.at[pl.ds(own * n_sq * heads, 2 * rows)]
    with jax.named_scope('barrier'):
        acc_in.wait()
        pl.semaphore_wait(barrier, 2 + n_tp - 1)

    def remote(src, dst, send, recv, to):
        return pltpu.make_async_remote_copy(src_ref=src, dst_ref=dst, send_sem=send, recv_sem=recv, device_id=to, device_id_type=mesh_id)

    def acc_rows(s, c):
        return pl.ds(pl.multiple_of(s * (own * heads) + c * fold, fold), fold)

    def pair_copy(k, c):
        rows_for = acc_rows(core_sq if k == 0 else lax.rem(core_sq + 2, n_sq), c)
        return remote(acc_buf.at[rows_for], pair_buf.at[k, c], pair_send, pair_recv.at[k, c], core)

    def up_copy(c):
        return remote(up_buf.at[c], cross_buf.at[c], up_send, up_recv.at[c], across)

    ml_copy = remote(ml_own, ml_pair, ml_send, ml_recv, core)
    mlu_copy = remote(ml_up, ml_cross, mlu_send, mlu_recv, across)

    half = n_tp // 2
    middle = lax.div(tp + 1, 2) == 1
    partner = tp + 1 - 2 * lax.rem(tp, 2)
    far = half - half * lax.div(tp, half)

    def m_copy(c):
        return remote(z_out.at[c, pl.ds(far, half)], far_in.at[c], z_send, m_recv.at[c], {"tp": partner})

    def n_copy(c):
        return remote(z_out.at[c, partner], in_buf.at[c, 0], z_send, s_recv.at[c], {"tp": partner})

    def s_copy(k, c):
        return remote(z_out.at[c, far + k], in_buf.at[c, 1], z_send, s_recv.at[c], {"tp": far + k})

    def block(s, t, c):
        return y_buf.at[pl.ds(pl.multiple_of(s * own + c * step, step), step), pl.ds(pl.multiple_of(t * cols, cols), cols)]

    def source(tag):
        return tp - tag if tag < n_tp else tp + (tag - n_tp + 1)

    def source_of(tag, c):
        return source(tag) if c < relayed else lax.rem(tp - tag + n_tp, n_tp)

    def tp_copy(t, c, to):
        b = block(sq, t, c)
        return remote(b, b, g_send, g_recv.at[t, c], {"tp": to})

    def y_copy(tag, c):
        t = source_of(tag, c)
        b = block(sq, t, c)
        return remote(b, b, y_send, y_recv.at[t, c], across)

    def c_copy(tag, c):
        b = block(sq, source_of(tag, c), c)
        return remote(b, b, c_send, c_recv, core)

    def f_copy(tag, c):
        b = block(across_sq, source_of(tag, c), c)
        return remote(b, b, f_send, f_recv, core)

    def all_of(ref, send, recv):
        return remote(ref, ref, send, recv, {"tp": tp})

    ml_copy.start()
    for k in (1, 0):
        for c in range(parts):
            pair_copy(k, c).start()

    lane = lax.broadcasted_iota(jnp.int32, (rows, dim), 1)

    def column(e, p):
        return jnp.sum(jnp.where(lane == p, e, 0.0), axis=1, keepdims=True)

    def part_of(j):
        return slice(j * rows, (j + 1) * rows)

    with jax.named_scope("pairwait"):
        ml_copy.wait_recv()
    ml_at = own * n_sq * heads
    m_own, l_own = acc_buf[ml_at:ml_at + rows, :], acc_buf[ml_at + rows:ml_at + 2 * rows, :]
    m_pair, l_pair = ml_pair[:rows, :], ml_pair[rows:, :]
    m_up = jnp.maximum(m_own, m_pair)
    e_own, e_pair = jnp.exp(m_own - m_up), jnp.exp(m_pair - m_up)
    ml_up[:rows, :] = m_up
    ml_up[rows:, :] = e_own * l_own + e_pair * l_pair
    for c in range(parts):
        pair_copy(1, c).wait_recv()
        for j in range(pairs):
            p = across_sq * (own // 2) + c * pairs + j
            mine = pl.multiple_of(across_sq * (own * heads) + c * fold + j * rows, rows)
            up_buf[c, part_of(j), :] = column(e_own, p) * acc_buf[pl.ds(mine, rows), :] + column(e_pair, p) * pair_buf[1, c, part_of(j), :]
        if c == 0:
            mlu_copy.start()
        up_copy(c).start()

    x_in.wait()
    base_buf[...] = x_buf[...].astype(F32) + bo_ref[:, x_cols]
    with jax.named_scope("mlwait"):
        mlu_copy.wait_recv()
    m_cross, l_cross = ml_cross[:rows, :], ml_cross[rows:, :]
    top = jnp.maximum(m_up, m_cross)
    scales = [jnp.exp(m - top) for m in (m_own, m_pair, m_cross)]
    den = scales[0] * l_own + scales[1] * l_pair + scales[2] * l_cross
    scales = [e / den for e in scales]

    def when(cond):
        return pl.when(cond)

    def project(c):
        pair_copy(0, c).wait_recv()
        up_copy(c).wait_recv()
        for j in range(pairs):
            p = sq * (own // 2) + c * pairs + j
            mine = pl.multiple_of(sq * (own * heads) + c * fold + j * rows, rows)
            terms = (acc_buf[pl.ds(mine, rows), :], pair_buf[0, c, part_of(j), :], cross_buf[c, part_of(j), :])
            total = sum(column(e, p) * t for e, t in zip(scales, terms))
            a_buf[j * rows:(j + 1) * rows, :] = total
        lhs = jnp.concatenate([a_buf[pl.ds(n, step, stride=heads), :].astype(BF16) for n in range(heads)], axis=1)
        def term(t):
            w = wo_ref[:, pl.ds(pl.multiple_of(t * cols, cols), cols)]
            z_out[c, t] = jnp.dot(lhs, w, preferred_element_type=F32)

        for k in range(half):
            term(far + k)

        @when(jnp.logical_not(middle))
        def _():
            m_copy(c).start()

        term(partner)
        term(tp)

        if c:
            n_copy(c - 1).start()
        if c == parts - 1:
            n_copy(c).start()

    def add(c):
        @when(middle)
        def _():
            m_copy(c).wait_recv()
            for k in range(half):
                z_out[c, far + k] = z_out[c, far + k] + far_in[c, k]
            for k in range(half):
                s_copy(k, c).start()

    def share(tag, c):
        y_copy(tag, c).start()
        c_copy(tag, c).start()

    def finish(c):
        all_of(in_buf.at[c], z_send, s_recv.at[c]).wait_recv()
        total = z_out[c, tp] + in_buf[c, 0] + in_buf[c, 1]
        total = total + base_buf[c * step:(c + 1) * step, :]
        mine = block(sq, tp, c)
        mine[...] = total

        if c < relayed:
            @when(tp < n_tp - 1)
            def _():
                tp_copy(tp, c, tp + 1).start()

            @when(tp > 0)
            def _():
                tp_copy(tp, c, tp - 1).start()
        else:
            for d in range(1, n_tp):
                tp_copy(tp, c, lax.rem(tp + d, n_tp)).start()

        share(0, c)

    def direct(d, c):
        tp_copy(source_of(d, c), c, tp).wait_recv()
        share(d, c)

    def hop(h, c):
        @when(tp >= h)
        def _():
            tp_copy(tp - h, c, tp).wait_recv()

            @when(tp < n_tp - 1)
            def _():
                tp_copy(tp - h, c, tp + 1).start()

            share(h, c)

        @when(tp + h < n_tp)
        def _():
            tp_copy(tp + h, c, tp).wait_recv()

            @when(tp > 0)
            def _():
                tp_copy(tp + h, c, tp - 1).start()

            share(h + n_tp - 1, c)

    def crossed(h, c):
        def take(tag):
            y_copy(tag, c).wait_recv()
            f_copy(tag, c).start()

        if h == 0 or c >= relayed:
            take(h)
            return

        @when(tp >= h)
        def _():
            take(h)

        @when(tp + h < n_tp)
        def _():
            take(h + n_tp - 1)

    def named(name, fn, *args):
        def run():
            with jax.named_scope(name):
                fn(*args)
        return run

    events = []
    for c in range(parts):
        events.append((6.3 + 3.0 / parts * c, 0, named(f"p{c}", project, c)))
        events.append((8.1 + 8.4 / parts * (c + 1), 0, named(f"a{c}", add, c)))
        t = 11.7 + 8.4 / parts * (c + 1)
        events.append((t, 1, named(f"f{c}", finish, c)))
        events.append((t + 4.0, 3, named(f"y{c}_0", crossed, 0, c)))
        for h in range(1, n_tp):
            if c < relayed:
                there = t + 3.6 * h - 0.7
                events.append((there, 2, named(f"h{c}_{h}", hop, h, c)))
            else:
                there = t + 3.2 + 0.8 * h
                events.append((there, 2, named(f"d{c}_{h}", direct, h, c)))
            events.append((there + 5.0, 3, named(f"y{c}_{h}", crossed, h, c)))
    for _, _, event in sorted(events, key=lambda e: e[:2]):
        event()

    whole = y_buf.at[pl.ds(0, own)]
    with jax.named_scope("close"):
        all_of(whole, c_send, c_recv).wait()
        all_of(whole, f_send, f_recv).wait()
        all_of(whole, y_send, f_recv).wait_send()
        ml_copy.wait_send()
        mlu_copy.wait_send()
        all_of(pair_buf, pair_send, ml_recv).wait_send()
        all_of(up_buf, up_send, ml_recv).wait_send()
        all_of(z_out.at[:, pl.ds(0, half + 1)], z_send, ml_recv).wait_send()
        straight = (parts - relayed) * (n_tp - 1)

        @when(middle)
        def _():
            blocks = y_buf.at[pl.ds(0, (straight + relayed * (n_tp + 1)) * step // n_tp)]
            all_of(blocks, g_send, ml_recv).wait_send()

        @when(jnp.logical_not(middle))
        def _():
            blocks = y_buf.at[pl.ds(0, (straight + relayed) * step // n_tp)]
            all_of(blocks, g_send, ml_recv).wait_send()

    chunk = 32
    for i in range(y_buf.shape[0] // chunk):
      with jax.named_scope(f'emit{i}'):
        out_ref[i * chunk:(i + 1) * chunk, :] = y_buf[i * chunk:(i + 1) * chunk, :].astype(BF16)


def meet(acc, x, wo, bo, n_sq, n_tp, parts=4, relayed=3):
    batch, width = x.shape
    own = batch // n_sq
    cols = width // n_tp
    step = own // parts
    heads = wo.shape[0] // acc.shape[1]
    dim = acc.shape[1]
    vmem = pl.BlockSpec(memory_space=pltpu.VMEM)
    hbm = pl.BlockSpec(memory_space=pltpu.HBM)
    dma = pltpu.SemaphoreType.DMA
    return pl.pallas_call(
        functools.partial(meet_kernel, n_sq, parts, relayed),
        out_shape=jax.ShapeDtypeStruct((batch, width), BF16),
        in_specs=[hbm, hbm, vmem, vmem],
        out_specs=vmem,
        scratch_shapes=[
            pltpu.VMEM(acc.shape, F32),
            pltpu.VMEM((own, cols), BF16),
            pltpu.VMEM((own, cols), F32),
            pltpu.VMEM((2, parts, step * heads, dim), F32),
            pltpu.VMEM((4 * heads, dim), F32),
            pltpu.VMEM((parts, step * heads, dim), F32),
            pltpu.VMEM((4 * heads, dim), F32),
            pltpu.VMEM((parts, step * heads, dim), F32),
            pltpu.VMEM((4 * heads, dim), F32),
            pltpu.VMEM((step * heads, dim), F32),
            pltpu.VMEM((parts, n_tp, step, cols), F32),
            pltpu.VMEM((parts, n_tp // 2, step, cols), F32),
            pltpu.VMEM((parts, 2, step, cols), F32),
            pltpu.VMEM((batch, width), F32),
            dma((2,)), dma, dma, dma, dma, dma, dma((2, parts)), dma, dma((parts,)),
            dma, dma((parts,)), dma((parts,)), dma, dma((n_tp, parts)),
            dma, dma((n_tp, parts)), dma, dma, dma, dma,
        ],
        compiler_params=pltpu.CompilerParams(collective_id=0, has_side_effects=True, vmem_limit_bytes=32 * 1024 * 1024),
        cost_estimate=pl.CostEstimate(flops=2**28, bytes_accessed=8 * 2**20, transcendentals=0),
        name="meet",
    )(pltpu.with_memory_space_constraint(acc, pltpu.HBM), pltpu.with_memory_space_constraint(x, pltpu.HBM), wo, bo.reshape(1, width))


def solution(mesh):
    def local_step(hidden, cache_lens, k_cache, v_cache, ln_gain, ln_bias, w_query, b_query, w_kv, b_kv, w_out, b_out):
        key_new, val_new, acc = attend(
            cache_lens, hidden, ln_gain, ln_bias, w_query, b_query, w_kv, b_kv, k_cache, v_cache)
        out_hidden = meet(acc, hidden, w_out, b_out, mesh.shape["sq"], mesh.shape["tp"])
        return out_hidden, key_new, val_new

    cache_spec = P("dp", "sq", None)
    row_spec = P("dp", None)
    in_specs = (row_spec, P("dp"), cache_spec, cache_spec, P(None), P(None), P(None, "tp"), P("tp"), P(None, None), P(None), P("tp", None), P(None))
    out_specs = (row_spec, cache_spec, cache_spec)
    return jax.shard_map(local_step, mesh=mesh, in_specs=in_specs, out_specs=out_specs, check_vma=False)
```
